32 devices in a mesh: dp: 2 (over x), seq: 8 (over z, y), tensor: 2 (over core).
Axes of the slice: x: 2, y: 2, z: 4, core: 2. Of those that a mesh axis runs over, the one named last changes fastest.
Arguments:
- tokens: bfloat16 [2, 8192, 1024], P('dp', 'seq'), may hold values from -6 to 6
- norm1_gain: float32 [1024], replicated, may hold values from 0.1 to 1.9
- in_weight: bfloat16 [3, 1024, 1024], P(None, None, 'tensor'), may hold values from -0.1875 to 0.1875
- conv_weight: float32 [3, 1024], P(None, 'tensor'), may hold values from -3.5 to 3.5
- out_weight: bfloat16 [1024, 1024], P('tensor'), may hold values from -0.1875 to 0.1875
- norm2_gain: float32 [1024], replicated, may hold values from 0.1 to 1.9
- gate_weight: bfloat16 [1024, 4608], P(None, 'tensor'), may hold values from -0.1875 to 0.1875
- up_weight: bfloat16 [1024, 4608], P(None, 'tensor'), may hold values from -0.1875 to 0.1875
- down_weight: bfloat16 [4608, 1024], P('tensor'), may hold values from -0.09375 to 0.09375
- out_cotangent: bfloat16 [2, 8192, 1024], P('dp', 'seq', 'tensor'), may hold values from -6 to 6
Outputs:
- block_out: bfloat16 [2, 8192, 1024], P('dp', 'seq', 'tensor')
- tokens_grad: float32 [2, 8192, 1024], P('dp', 'seq', 'tensor')
- norm1_grad: float32 [1024], P('tensor')
- in_grad: float32 [3, 1024, 1024], P(None, ('dp', 'seq'), 'tensor')
- conv_grad: float32 [3, 1024], P(None, 'tensor')
- out_grad: float32 [1024, 1024], P('tensor', ('dp', 'seq'))
- norm2_grad: float32 [1024], P('tensor')
- gate_grad: float32 [1024, 4608], P(('dp', 'seq'), 'tensor')
- up_grad: float32 [1024, 4608], P(('dp', 'seq'), 'tensor')
- down_grad: float32 [4608, 1024], P('tensor', ('dp', 'seq'))
The draws below stay inside these ranges and needn't reach their ends.
All inputs are finite; a program needn't handle non-finite values.
Results may differ from the reference program's by a relative error of at most 0.014.
Values may be sent and summed in bfloat16 or wider, within the bound.
A program may use at most 256 MiB of HBM per device.

```python
import jax
import jax.numpy as jnp
from jax import lax

D = 1024
FF = 4608
NSEQ = 2
LENGTH = 8192


def levels(stream_key, shape, split, smallest, largest):
    def one(axis_at, parts):
        steps = jax.random.uniform(jax.random.fold_in(jax.random.fold_in(stream_key, 6), axis_at), (parts,), jnp.float32, smallest / len(split), largest / len(split))
        return jnp.repeat(jnp.exp(steps), shape[axis_at] // parts).reshape((-1,) + (1,) * (len(shape) - axis_at - 1))

    gain = one(*split[0])
    for cut in split[1:]:
        gain = gain * one(*cut)
    return gain


def centred(rng, dims, spread, limit, split=(), kind=jnp.bfloat16):
    result = spread * jax.random.normal(rng, dims, jnp.float32)
    if split:
        result = result * levels(rng, dims, split, -0.22, 0.18)
    return jnp.clip(result, -limit, limit).astype(kind)


def setup_inputs(seed: int = 0) -> dict:
    key_list = jax.random.split(jax.random.key(seed), 11)
    tokens = centred(key_list[0], (NSEQ, LENGTH, D), 1.0, 6.0, ((0, 2), (1, 8)))
    norm1_gain = jnp.clip(1.0 + 0.18 * jax.random.normal(key_list[1], (D,), jnp.float32), 0.1, 1.9)
    in_weight = centred(key_list[2], (3, D, D), D ** -0.5, 0.1875, ((2, 2),))
    conv_weight = centred(key_list[3], (3, D), 3 ** -0.5, 3.5, ((1, 2),), jnp.float32)
    out_weight = centred(key_list[4], (D, D), D ** -0.5, 0.1875, ((0, 2),))
    norm2_gain = jnp.clip(1.0 + 0.18 * jax.random.normal(key_list[5], (D,), jnp.float32), 0.1, 1.9)
    gate_weight = centred(key_list[6], (D, FF), D ** -0.5, 0.1875, ((1, 2),))
    up_weight = centred(key_list[7], (D, FF), D ** -0.5, 0.1875, ((1, 2),))
    down_weight = centred(key_list[8], (FF, D), FF ** -0.5, 0.09375, ((0, 2),))
    out_cotangent = centred(key_list[9], (NSEQ, LENGTH, D), 1.0, 6.0, ((0, 2), (1, 8), (2, 2)))
    return {"tokens": tokens, "norm1_gain": norm1_gain, "in_weight": in_weight, "conv_weight": conv_weight, "out_weight": out_weight, "norm2_gain": norm2_gain, "gate_weight": gate_weight, "up_weight": up_weight, "down_weight": down_weight, "out_cotangent": out_cotangent}


EPSILON = 1e-05

def inverse_rms(values):
    return lax.rsqrt(lax.optimization_barrier(jnp.mean(values * values, axis=-1, keepdims=True)) + EPSILON)

def product(left, right):
    return jnp.dot(left, right, preferred_element_type=jnp.float32)

def reference(tokens, norm1_gain, in_weight, conv_weight, out_weight, norm2_gain, gate_weight, up_weight, down_weight, out_cotangent):
    total_rows = NSEQ * LENGTH
    block_rows = 4096 if LENGTH % 4096 == 0 else LENGTH
    blocks = total_rows // block_rows
    token_blocks = tokens.reshape(blocks, block_rows, D)
    cot_blocks = out_cotangent.reshape(blocks, block_rows, D)

    def project(block):
        token_float = block.astype(jnp.float32)
        scale_one = inverse_rms(token_float)
        unit_one = token_float * scale_one
        normed = (unit_one * norm1_gain).astype(jnp.bfloat16)
        return (scale_one, unit_one, normed, product(normed, in_weight[0]), product(normed, in_weight[1]), product(normed, in_weight[2]))

    def gated_input(block):
        pieces = project(block)
        return pieces[3] * pieces[5]
    gated = lax.map(gated_input, token_blocks).reshape(NSEQ, LENGTH, D)
    padded = jnp.pad(gated, ((0, 0), (2, 0), (0, 0)))
    conv_all = conv_weight[0] * padded[:, 0:LENGTH] + conv_weight[1] * padded[:, 1:LENGTH + 1] + conv_weight[2] * padded[:, 2:LENGTH + 2]
    conv_blocks = conv_all.reshape(blocks, block_rows, D)

    def forward_back(carry, inputs):
        block, cot_block, conv_block = inputs
        scale_one, unit_one, normed, b_signal, c_signal, x_signal = project(block)
        mixed_in = (c_signal * conv_block).astype(jnp.bfloat16)
        resid = block.astype(jnp.float32) + product(mixed_in, out_weight)
        scale_two = inverse_rms(resid)
        unit_two = resid * scale_two
        normed_two = (unit_two * norm2_gain).astype(jnp.bfloat16)
        gate_pre = product(normed_two, gate_weight)
        up_pre = product(normed_two, up_weight)
        sigma = jax.nn.sigmoid(gate_pre)
        active = gate_pre * sigma
        hidden = (active * up_pre).astype(jnp.bfloat16)
        final = (resid + product(hidden, down_weight)).astype(jnp.bfloat16)
        grad_hidden = product(cot_block, down_weight.T)
        grad_gate = (grad_hidden * up_pre * (sigma * (1.0 + gate_pre * (1.0 - sigma)))).astype(jnp.bfloat16)
        grad_up = (grad_hidden * active).astype(jnp.bfloat16)
        grad_norm_two = product(grad_gate, gate_weight.T) + product(grad_up, up_weight.T)
        grad_unit = grad_norm_two * norm2_gain
        grad_resid = cot_block.astype(jnp.float32) + scale_two * (grad_unit - unit_two * lax.optimization_barrier(jnp.mean(grad_unit * unit_two, axis=-1, keepdims=True)))
        resid_bf = grad_resid.astype(jnp.bfloat16)
        grad_mixed = product(resid_bf, out_weight.T)
        grad_c = (grad_mixed * conv_block).astype(jnp.bfloat16)
        grad_conv = grad_mixed * c_signal
        acc_gain, acc_out, acc_gate, acc_up, acc_down = carry
        carry = (acc_gain + lax.optimization_barrier(jnp.sum(grad_norm_two * unit_two, axis=0)), acc_out + product(mixed_in.T, resid_bf), acc_gate + product(normed_two.T, grad_gate), acc_up + product(normed_two.T, grad_up), acc_down + product(hidden.T, cot_block))
        return (carry, (final, grad_resid, grad_c, grad_conv))
    first_init = (jnp.zeros((D,), jnp.float32), jnp.zeros((D, D), jnp.float32), jnp.zeros((D, FF), jnp.float32), jnp.zeros((D, FF), jnp.float32), jnp.zeros((FF, D), jnp.float32))
    first_sums, outputs = lax.scan(forward_back, first_init, (token_blocks, cot_blocks, conv_blocks))
    final_blocks, resid_blocks, grad_c_blocks, grad_conv_blocks = outputs
    norm2_grad, out_grad, gate_grad, up_grad, down_grad = first_sums
    grad_conv_all = grad_conv_blocks.reshape(NSEQ, LENGTH, D)
    after = jnp.pad(grad_conv_all, ((0, 0), (0, 2), (0, 0)))
    grad_gated = conv_weight[0] * after[:, 2:LENGTH + 2] + conv_weight[1] * after[:, 1:LENGTH + 1] + conv_weight[2] * after[:, 0:LENGTH]
    conv_grad = jnp.stack([lax.optimization_barrier(jnp.sum(grad_conv_all * padded[:, index:index + LENGTH], axis=(0, 1))) for index in range(3)])

    def input_back(carry, inputs):
        block, gated_block, grad_c, grad_resid = inputs
        scale_one, unit_one, normed, b_signal, c_signal, x_signal = project(block)
        grad_b = (gated_block * x_signal).astype(jnp.bfloat16)
        grad_x = (gated_block * b_signal).astype(jnp.bfloat16)
        grad_normed = product(grad_b, in_weight[0].T) + product(grad_c, in_weight[1].T) + product(grad_x, in_weight[2].T)
        grad_unit = grad_normed * norm1_gain
        grad_token = grad_resid + scale_one * (grad_unit - unit_one * lax.optimization_barrier(jnp.mean(grad_unit * unit_one, axis=-1, keepdims=True)))
        acc_gain, acc_in = carry
        carry = (acc_gain + lax.optimization_barrier(jnp.sum(grad_normed * unit_one, axis=0)), acc_in + jnp.stack([product(normed.T, grad_b), product(normed.T, grad_c), product(normed.T, grad_x)]))
        return (carry, grad_token)
    second_init = (jnp.zeros((D,), jnp.float32), jnp.zeros((3, D, D), jnp.float32))
    second_sums, token_grad_blocks = lax.scan(input_back, second_init, (token_blocks, grad_gated.reshape(blocks, block_rows, D), grad_c_blocks, resid_blocks))
    norm1_grad, in_grad = second_sums
    block_out = final_blocks.reshape(NSEQ, LENGTH, D)
    tokens_grad = token_grad_blocks.reshape(NSEQ, LENGTH, D)
    return (block_out, tokens_grad, norm1_grad, in_grad, conv_grad, out_grad, norm2_grad, gate_grad, up_grad, down_grad)
```

```python
import functools

import jax
import jax.numpy as jnp
from jax import lax
from jax.experimental import pallas as pl
from jax.experimental.pallas import tpu as pltpu
from jax.sharding import PartitionSpec as P

EPSILON = 1e-05
MESH = pl.DeviceIdType.MESH
UNIT = 256
VMEM_BYTES = 63 * 1024 * 1024
F32 = jnp.float32
BF16 = jnp.bfloat16


def shifted(value, axis, steps):
    count = lax.axis_size(axis)
    first, last = (max(0, -steps), min(count, count - steps))
    return lax.ppermute(value, axis, [(source, source + steps) for source in range(first, last)])


def inverse_rms(values):
    return lax.rsqrt(jnp.mean(values * values, axis=-1, keepdims=True) + EPSILON)


def product(left, right):
    return jnp.dot(left, right, preferred_element_type=F32)


def product_t(left, right):
    return lax.dot_general(left, right, (((1,), (1,)), ((), ())), preferred_element_type=F32)


def own_columns(values, start, count):
    return lax.dynamic_slice_in_dim(values, start, count, 1)


class Halving:
    def __init__(self, seq_size, shards, rows):
        self.seq_size = seq_size
        self.bits = shards.bit_length() - 1
        self.shards = shards
        self.rows = rows

    def stage_rows(self, stage):
        return self.rows << (self.bits - 1 - stage)

    def enter(self):
        self.me = lax.axis_index("dp") * self.seq_size + lax.axis_index("seq")
        self.core = lax.axis_index("tensor")

    def place(self, flat):
        return (flat // self.seq_size, flat % self.seq_size, self.core)

    def flipped(self, weight):
        return self.me + (1 - 2 * ((self.me // weight) % 2)) * weight

    def other_core(self):
        return (self.me // self.seq_size, self.me % self.seq_size, 1 - self.core)

    def greet(self):
        barrier = pltpu.get_barrier_semaphore()
        partners = [self.place(self.flipped(1 << bit)) for bit in range(self.bits)]
        partners.append(self.other_core())
        for partner in partners:
            pl.semaphore_signal(barrier, inc=1, device_id=partner, device_id_type=MESH)
        pl.semaphore_wait(barrier, len(partners))

    def order(self, parity):
        top = self.shards // 2
        high = (self.me // top) % 2
        low = self.me % 2
        first = (top + parity * (1 - top), high + parity * (low - high))
        third = (1 + parity * (top - 1), low + parity * (high - low))
        middle = [(2, (self.me // 2) % 2)]
        rest = [(1 << bit, (self.me // (1 << bit)) % 2) for bit in range(2, self.bits - 1)]
        return [first] + middle + [third] + rest

    def chunks(self, order, keep):
        weight, bit = order[0]
        base = (bit if keep else 1 - bit) * weight
        found = []
        for code in range(self.shards // 2):
            chunk = base
            for place in range(1, self.bits):
                if (code >> (self.bits - 1 - place)) & 1:
                    chunk = chunk + order[place][0]
            found.append(chunk)
        return found

    def offset(self, order, source, stage):
        total = 0
        for place in range(source + 1, min(stage, self.bits - 1) + 1):
            bit = order[place][1]
            if place == stage:
                bit = 1 - bit
            total = total + bit * (1 << (self.bits - 1 - place))
        return total * self.rows

    def scratch(self, units):
        half = self.stage_rows(0)
        return (
            [pltpu.VMEM((units, half, UNIT), BF16), pltpu.VMEM((units, half, UNIT), BF16)]
            + [pltpu.VMEM((units, self.stage_rows(s), UNIT), BF16) for s in range(self.bits)]
            + [
                pltpu.SemaphoreType.DMA((self.bits, units)),
                pltpu.SemaphoreType.DMA((self.bits, units)),
            ]
        )

    def bind(self, refs):
        self.first, self.keep = refs[0], refs[1]
        self.recv = refs[2 : 2 + self.bits]
        self.send_sem, self.recv_sem = refs[2 + self.bits :]

    def copy(self, order, unit, stage):
        weight, bit = order[stage]
        if stage == 0:
            source = self.first.at[unit]
        else:
            start = pl.multiple_of(self.offset(order, 0, stage), self.rows)
            source = self.keep.at[unit, pl.ds(start, self.stage_rows(stage))]
        return pltpu.make_async_remote_copy(
            src_ref=source,
            dst_ref=self.recv[stage].at[unit],
            send_sem=self.send_sem.at[stage, unit],
            recv_sem=self.recv_sem.at[stage, unit],
            device_id=self.place(self.me + (1 - 2 * bit) * weight),
            device_id_type=MESH,
        )

    def gather(self, left, order, keep):
        return jnp.concatenate([left[chunk] for chunk in self.chunks(order, keep)], axis=0)

    def begin(self, unit, parity, left, right):
        order = self.order(parity)
        self.first[unit] = product(self.gather(left, order, False), right[...]).astype(BF16)
        self.copy(order, unit, 0).start()

    def hold(self, unit, parity, left, right):
        order = self.order(parity)
        self.keep[unit] = product(self.gather(left, order, True), right[...]).astype(BF16)

    def collect(self, order, unit, stage, rows):
        start = pl.multiple_of(self.offset(order, 0, stage), self.rows)
        total = self.keep[unit, pl.ds(start, rows)].astype(F32)
        for source in range(min(stage, self.bits)):
            start = pl.multiple_of(self.offset(order, source, stage), self.rows)
            total = total + self.recv[source][unit, pl.ds(start, rows)].astype(F32)
        return total

    def advance(self, unit, parity, stage):
        order = self.order(parity)
        self.copy(order, unit, stage - 1).wait_recv()
        rows = self.stage_rows(stage)
        total = self.collect(order, unit, stage, rows)
        start = pl.multiple_of(self.offset(order, 0, stage), self.rows)
        self.keep[unit, pl.ds(start, rows)] = total.astype(BF16)
        self.copy(order, unit, stage).start()

    def finish(self, unit, parity):
        order = self.order(parity)
        self.copy(order, unit, self.bits - 1).wait_recv()
        total = self.collect(order, unit, self.bits, self.rows)
        for stage in range(self.bits):
            self.copy(order, unit, stage).wait_send()
        return total


def ffn_kernel(
    plan,
    normed_ref,
    cot_ref,
    left_ref,
    gate_hbm,
    up_hbm,
    down_hbm,
    grads_ref,
    pn_ref,
    pn_recv,
    out_ref,
    out_recv,
    gate_buf,
    up_buf,
    down_buf,
    right_ref,
    pn_acc,
    out_acc,
    out_send,
    weight_sem,
    swap_send,
    swap_recv,
    *refs,
):
    total_rows, width = normed_ref.shape
    blocks = gate_hbm.shape[1] // UNIT
    step_rows = min(256, total_rows)
    half = width // 2
    plan.bind(refs)
    plan.enter()

    def weights(index):
        slot = index % 2
        span = pl.ds(pl.multiple_of(index * UNIT, UNIT), UNIT)
        return [
            pltpu.make_async_copy(gate_hbm.at[:, span], gate_buf.at[slot], weight_sem.at[0, slot]),
            pltpu.make_async_copy(up_hbm.at[:, span], up_buf.at[slot], weight_sem.at[1, slot]),
            pltpu.make_async_copy(down_hbm.at[span], down_buf.at[slot], weight_sem.at[2, slot]),
        ]

    for item in weights(0):
        item.start()
    plan.greet()
    pn_acc[...] = jnp.zeros_like(pn_acc)
    out_acc[...] = jnp.zeros_like(out_acc)

    def swaps():
        return [
            pltpu.make_async_remote_copy(
                src_ref=source,
                dst_ref=target,
                send_sem=swap_send.at[index],
                recv_sem=swap_recv.at[index],
                device_id=plan.other_core(),
                device_id_type=MESH,
            )
            for index, (source, target) in enumerate(((pn_ref, pn_recv), (out_send, out_recv)))
        ]

    def step(index, carry):
        @pl.when(index < blocks)
        def _():
            slot = index % 2

            @pl.when(index + 1 < blocks)
            def _():
                for item in weights(index + 1):
                    item.start()

            for item in weights(index):
                item.wait()
            for first in range(0, total_rows, step_rows):
                rows = pl.ds(first, step_rows)
                normed = normed_ref[rows]
                gate_pre = product(normed, gate_buf[slot])
                up_pre = product(normed, up_buf[slot])
                grad_hidden = product_t(cot_ref[rows], down_buf[slot])
                sigma = jax.nn.sigmoid(gate_pre)
                active = gate_pre * sigma
                right_ref[0, rows] = (
                    grad_hidden * up_pre * (sigma * (1.0 + gate_pre * (1.0 - sigma)))
                ).astype(BF16)
                right_ref[1, rows] = (grad_hidden * active).astype(BF16)
                right_ref[2, rows] = (active * up_pre).astype(BF16)
            for place in range(3):
                unit = index * 3 + place
                plan.begin(unit, unit % 2, left_ref.at[place // 2], right_ref.at[place])
            for first in range(0, total_rows, step_rows):
                rows = pl.ds(first, step_rows)
                pn_acc[rows] += product_t(right_ref[0, rows], gate_buf[slot]) + product_t(
                    right_ref[1, rows], up_buf[slot]
                )
                out_acc[rows] += product(right_ref[2, rows], down_buf[slot])
            for place in range(3):
                unit = index * 3 + place
                plan.hold(unit, unit % 2, left_ref.at[place // 2], right_ref.at[place])

        @pl.when(index == blocks)
        def _():
            own = pl.ds(pl.multiple_of(plan.core * half, half), half)
            other = pl.ds(pl.multiple_of((1 - plan.core) * half, half), half)
            pn_ref[...] = pn_acc[...].astype(BF16)
            out_send[...] = out_acc[:, other].astype(BF16)
            for item in swaps():
                item.start()
            out_ref[...] = out_acc[:, own]

        for stage in range(plan.bits, 0, -1):
            block = index - stage

            @pl.when((block >= 0) & (block < blocks))
            def _(stage=stage, block=block):
                for place in range(3):
                    unit = block * 3 + place
                    if stage < plan.bits:
                        plan.advance(unit, unit % 2, stage)
                    else:
                        span = pl.ds(pl.multiple_of(block * UNIT, UNIT), UNIT)
                        grads_ref[place, :, span] = plan.finish(unit, unit % 2)

        return carry

    lax.fori_loop(0, blocks + plan.bits, step, 0)
    for item in swaps():
        item.wait()


def whole():
    return pl.BlockSpec(memory_space=pltpu.VMEM)


def anywhere():
    return pl.BlockSpec(memory_space=pl.ANY)


def ffn(plan, normed, cotangent, left, gate_weight, up_weight, down_weight):
    total_rows, width = normed.shape
    hidden = gate_weight.shape[1]
    blocks = hidden // UNIT
    half = width // 2
    shape = jax.ShapeDtypeStruct
    return pl.pallas_call(
        functools.partial(ffn_kernel, plan),
        name="ffn",
        out_shape=(
            shape((3, plan.rows, hidden), F32),
            shape((total_rows, width), BF16),
            shape((total_rows, width), BF16),
            shape((total_rows, half), F32),
            shape((total_rows, half), BF16),
        ),
        in_specs=[whole()] * 3 + [anywhere()] * 3,
        out_specs=[whole()] * 5,
        scratch_shapes=[
            pltpu.VMEM((2, width, UNIT), BF16),
            pltpu.VMEM((2, width, UNIT), BF16),
            pltpu.VMEM((2, UNIT, width), BF16),
            pltpu.VMEM((3, total_rows, UNIT), BF16),
            pltpu.VMEM((total_rows, width), F32),
            pltpu.VMEM((total_rows, width), F32),
            pltpu.VMEM((total_rows, half), BF16),
            pltpu.SemaphoreType.DMA((3, 2)),
            pltpu.SemaphoreType.DMA((2,)),
            pltpu.SemaphoreType.DMA((2,)),
        ]
        + plan.scratch(3 * blocks),
        compiler_params=pltpu.CompilerParams(
            collective_id=0, has_side_effects=True, vmem_limit_bytes=VMEM_BYTES
        ),
    )(normed, cotangent, left, gate_weight, up_weight, down_weight)


def mix_kernel(
    plan,
    left_ref,
    mixed_ref,
    b_ref,
    c_ref,
    x_ref,
    weight_ref,
    grads_ref,
    part_ref,
    part_recv,
    swap_send,
    swap_recv,
    *refs,
):
    total_rows, width = part_ref.shape
    step_rows = min(256, total_rows)
    plan.bind(refs)
    plan.enter()
    plan.greet()
    rights = [mixed_ref, b_ref, c_ref, x_ref]
    pieces = mixed_ref.shape[1] // UNIT
    units = [(place, piece) for place in range(4) for piece in range(pieces)]
    for unit, (place, piece) in enumerate(units):
        right = rights[place].at[:, pl.ds(piece * UNIT, UNIT)]
        plan.begin(unit, unit % 2, left_ref.at[0 if place else 1], right)
    swaps = []
    for index, first in enumerate(range(0, total_rows, step_rows)):
        rows = pl.ds(first, step_rows)
        total = product_t(b_ref[rows], weight_ref[0])
        total = total + product_t(c_ref[rows], weight_ref[1])
        total = total + product_t(x_ref[rows], weight_ref[2])
        part_ref[rows] = total.astype(BF16)
        swaps.append(
            pltpu.make_async_remote_copy(
                src_ref=part_ref.at[rows],
                dst_ref=part_recv.at[rows],
                send_sem=swap_send.at[index],
                recv_sem=swap_recv.at[index],
                device_id=plan.other_core(),
                device_id_type=MESH,
            )
        )
        swaps[-1].start()
    for unit, (place, piece) in enumerate(units):
        right = rights[place].at[:, pl.ds(piece * UNIT, UNIT)]
        plan.hold(unit, unit % 2, left_ref.at[0 if place else 1], right)
    for stage in range(1, plan.bits):
        for unit in range(len(units)):
            plan.advance(unit, unit % 2, stage)
    for unit, (place, piece) in enumerate(units):
        grads_ref[place, :, piece * UNIT : (piece + 1) * UNIT] = plan.finish(unit, unit % 2)
    for item in swaps:
        item.wait()


def mix(plan, left, mixed_in, grad_b, grad_c, grad_x, in_weight):
    total_rows, half = mixed_in.shape
    width = in_weight.shape[1]
    swaps = total_rows // min(256, total_rows)
    shape = jax.ShapeDtypeStruct
    return pl.pallas_call(
        functools.partial(mix_kernel, plan),
        name="mix",
        out_shape=(
            shape((4, plan.rows, half), F32),
            shape((total_rows, width), BF16),
            shape((total_rows, width), BF16),
        ),
        in_specs=[whole()] * 6,
        out_specs=[whole()] * 3,
        scratch_shapes=[pltpu.SemaphoreType.DMA((swaps,)), pltpu.SemaphoreType.DMA((swaps,))]
        + plan.scratch(4 * half // UNIT),
        compiler_params=pltpu.CompilerParams(
            collective_id=1, has_side_effects=True, vmem_limit_bytes=VMEM_BYTES
        ),
    )(left, mixed_in, grad_b, grad_c, grad_x, in_weight)


def local(
    seq_size,
    shards,
    tokens,
    norm1_gain,
    in_weight,
    conv_weight,
    out_weight,
    norm2_gain,
    gate_weight,
    up_weight,
    down_weight,
    out_cotangent,
):
    seqs, length, width = tokens.shape
    half = in_weight.shape[2]
    total_rows = seqs * length
    chunk_rows = width // shards
    plan = Halving(seq_size, shards, chunk_rows)
    start = lax.axis_index("tensor") * half
    token_float = tokens.reshape(total_rows, width).astype(F32)
    scale_one = inverse_rms(token_float)
    unit_one = token_float * scale_one
    normed = (unit_one * norm1_gain).astype(BF16)
    b_signal = product(normed, in_weight[0])
    c_signal = product(normed, in_weight[1])
    x_signal = product(normed, in_weight[2])
    gated = (b_signal * x_signal).reshape(seqs, length, half)
    prior = shifted(gated[:, length - 2 :], "seq", 1)
    extended = jnp.concatenate([prior, gated], axis=1)
    conv_out = (
        conv_weight[0] * extended[:, 0:length]
        + conv_weight[1] * extended[:, 1 : length + 1]
        + conv_weight[2] * extended[:, 2 : length + 2]
    ).reshape(total_rows, half)
    mixed_in = (c_signal * conv_out).astype(BF16)
    resid = token_float + lax.psum(product(mixed_in, out_weight), "tensor")
    scale_two = inverse_rms(resid)
    unit_two = resid * scale_two
    normed_two = (unit_two * norm2_gain).astype(BF16)
    cotangent = lax.all_gather(
        out_cotangent.reshape(total_rows, half), "tensor", axis=1, tiled=True
    )
    left = jnp.stack([normed_two.T, cotangent.T]).reshape(2, shards, chunk_rows, total_rows)
    ffn_grads, pn_own, pn_other, out_own, out_other = ffn(
        plan, normed_two, cotangent, left, gate_weight, up_weight, down_weight
    )
    gate_grad, up_grad, down_grad = ffn_grads[0], ffn_grads[1], ffn_grads[2].T
    block_out = (
        (own_columns(resid, start, half) + out_own + out_other.astype(F32))
        .astype(BF16)
        .reshape(seqs, length, half)
    )
    grad_norm_two = pn_own.astype(F32) + pn_other.astype(F32)
    gain_two_term = lax.dynamic_slice_in_dim(
        jnp.sum(grad_norm_two * unit_two, axis=0), start, half, 0
    )
    grad_unit = grad_norm_two * norm2_gain
    grad_resid = cotangent.astype(F32) + scale_two * (
        grad_unit - unit_two * jnp.mean(grad_unit * unit_two, axis=-1, keepdims=True)
    )
    resid_bf = grad_resid.astype(BF16)
    grad_mixed = product(resid_bf, out_weight.T)
    grad_c = (grad_mixed * conv_out).astype(BF16)
    grad_conv = (grad_mixed * c_signal).reshape(seqs, length, half)
    following = shifted(grad_conv[:, 0:2], "seq", -1)
    grad_ext = jnp.concatenate([grad_conv, following], axis=1)
    grad_gated = (
        conv_weight[0] * grad_ext[:, 2 : length + 2]
        + conv_weight[1] * grad_ext[:, 1 : length + 1]
        + conv_weight[2] * grad_ext[:, 0:length]
    ).reshape(total_rows, half)
    kernel_term = jnp.stack(
        [
            jnp.sum(grad_conv * extended[:, index : index + length], axis=(0, 1))
            for index in range(3)
        ]
    )
    grad_b = (grad_gated * x_signal).astype(BF16)
    grad_x = (grad_gated * b_signal).astype(BF16)
    left = jnp.stack([normed.T, resid_bf.T]).reshape(2, shards, chunk_rows, total_rows)
    mix_grads, part_own, part_other = mix(
        plan, left, mixed_in, grad_b, grad_c, grad_x, in_weight
    )
    out_grad, in_grad = mix_grads[0].T, mix_grads[1:]
    grad_normed = part_own.astype(F32) + part_other.astype(F32)
    grad_unit_one = grad_normed * norm1_gain
    row_mean = jnp.mean(grad_unit_one * unit_one, axis=-1, keepdims=True)
    tokens_full = grad_resid + scale_one * (grad_unit_one - unit_one * row_mean)
    tokens_grad = own_columns(tokens_full, start, half)
    gain_one_term = lax.dynamic_slice_in_dim(
        jnp.sum(grad_normed * unit_one, axis=0), start, half, 0
    )
    conv_grad, norm1_grad, norm2_grad = lax.psum(
        (kernel_term, gain_one_term, gain_two_term), ("dp", "seq")
    )
    tokens_grad = tokens_grad.reshape(seqs, length, half)
    return (
        block_out,
        tokens_grad,
        norm1_grad,
        in_grad,
        conv_grad,
        out_grad,
        norm2_grad,
        gate_grad,
        up_grad,
        down_grad,
    )


def solution(mesh):
    seq_size = mesh.shape["seq"]
    shards = mesh.shape["dp"] * seq_size
    return jax.shard_map(
        functools.partial(local, seq_size, shards),
        mesh=mesh,
        in_specs=(
            P("dp", "seq", None),
            P(),
            P(None, None, "tensor"),
            P(None, "tensor"),
            P("tensor", None),
            P(),
            P(None, "tensor"),
            P(None, "tensor"),
            P("tensor", None),
            P("dp", "seq", "tensor"),
        ),
        out_specs=(
            P("dp", "seq", "tensor"),
            P("dp", "seq", "tensor"),
            P("tensor"),
            P(None, ("dp", "seq"), "tensor"),
            P(None, "tensor"),
            P("tensor", ("dp", "seq")),
            P("tensor"),
            P(("dp", "seq"), "tensor"),
            P(("dp", "seq"), "tensor"),
            P("tensor", ("dp", "seq")),
        ),
        check_vma=False,
    )
```

```python
import functools

import jax
import jax.numpy as jnp
from jax import lax
from jax.experimental import pallas as pl
from jax.experimental.pallas import tpu as pltpu
from jax.sharding import PartitionSpec as P

EPSILON = 1e-05
MESH = pl.DeviceIdType.MESH
UNIT = 256
VMEM_BYTES = 63 * 1024 * 1024
F32 = jnp.float32
BF16 = jnp.bfloat16


def shifted(value, axis, steps):
    count = lax.axis_size(axis)
    first, last = (max(0, -steps), min(count, count - steps))
    return lax.ppermute(value, axis, [(source, source + steps) for source in range(first, last)])


def inverse_rms(values):
    return lax.rsqrt(jnp.mean(values * values, axis=-1, keepdims=True) + EPSILON)


def product(left, right):
    return jnp.dot(left, right, preferred_element_type=F32)


def product_t(left, right):
    return lax.dot_general(left, right, (((1,), (1,)), ((), ())), preferred_element_type=F32)


def own_columns(values, start, count):
    return lax.dynamic_slice_in_dim(values, start, count, 1)


class Halving:
    def __init__(self, seq_size, shards, rows):
        self.seq_size = seq_size
        self.bits = shards.bit_length() - 1
        self.shards = shards
        self.rows = rows

    def stage_rows(self, stage):
        return self.rows << (self.bits - 1 - stage)

    def enter(self):
        self.me = lax.axis_index("dp") * self.seq_size + lax.axis_index("seq")
        self.core = lax.axis_index("tensor")

    def place(self, flat):
        return (flat // self.seq_size, flat % self.seq_size, self.core)

    def flipped(self, weight):
        return self.me + (1 - 2 * ((self.me // weight) % 2)) * weight

    def other_core(self):
        return (self.me // self.seq_size, self.me % self.seq_size, 1 - self.core)

    def along_seq(self, steps):
        seq = (self.me + steps) % self.seq_size
        return (self.me // self.seq_size, seq, self.core)

    def greet(self, steps=()):
        barrier = pltpu.get_barrier_semaphore()
        partners = [self.place(self.flipped(1 << bit)) for bit in range(self.bits)]
        partners.append(self.other_core())
        partners.extend(self.along_seq(count) for count in steps)
        for partner in partners:
            pl.semaphore_signal(barrier, inc=1, device_id=partner, device_id_type=MESH)
        pl.semaphore_wait(barrier, len(partners))

    def order(self, parity):
        top = self.shards // 2
        high = (self.me // top) % 2
        low = self.me % 2
        first = (top + parity * (1 - top), high + parity * (low - high))
        third = (1 + parity * (top - 1), low + parity * (high - low))
        middle = [(2, (self.me // 2) % 2)]
        rest = [(1 << bit, (self.me // (1 << bit)) % 2) for bit in range(2, self.bits - 1)]
        return [first] + middle + [third] + rest

    def chunks(self, order, keep):
        weight, bit = order[0]
        base = (bit if keep else 1 - bit) * weight
        found = []
        for code in range(self.shards // 2):
            chunk = base
            for place in range(1, self.bits):
                if (code >> (self.bits - 1 - place)) & 1:
                    chunk = chunk + order[place][0]
            found.append(chunk)
        return found

    def offset(self, order, source, stage):
        total = 0
        for place in range(source + 1, min(stage, self.bits - 1) + 1):
            bit = order[place][1]
            if place == stage:
                bit = 1 - bit
            total = total + bit * (1 << (self.bits - 1 - place))
        return total * self.rows

    def scratch(self, units):
        half = self.stage_rows(0)
        return (
            [pltpu.VMEM((units, half, UNIT), BF16), pltpu.VMEM((units, half, UNIT), BF16)]
            + [pltpu.VMEM((units, self.stage_rows(s), UNIT), BF16) for s in range(self.bits)]
            + [
                pltpu.SemaphoreType.DMA((self.bits, units)),
                pltpu.SemaphoreType.DMA((self.bits, units)),
            ]
        )

    def bind(self, refs):
        self.first, self.keep = refs[0], refs[1]
        self.recv = refs[2 : 2 + self.bits]
        self.send_sem, self.recv_sem = refs[2 + self.bits :]

    def copy(self, order, unit, stage):
        weight, bit = order[stage]
        if stage == 0:
            source = self.first.at[unit]
        else:
            start = pl.multiple_of(self.offset(order, 0, stage), self.rows)
            source = self.keep.at[unit, pl.ds(start, self.stage_rows(stage))]
        return pltpu.make_async_remote_copy(
            src_ref=source,
            dst_ref=self.recv[stage].at[unit],
            send_sem=self.send_sem.at[stage, unit],
            recv_sem=self.recv_sem.at[stage, unit],
            device_id=self.place(self.me + (1 - 2 * bit) * weight),
            device_id_type=MESH,
        )

    def gather(self, left, order, keep):
        return jnp.concatenate([left[chunk] for chunk in self.chunks(order, keep)], axis=0)

    def begin(self, unit, parity, left, right):
        order = self.order(parity)
        self.first[unit] = product(self.gather(left, order, False), right[...]).astype(BF16)
        self.copy(order, unit, 0).start()

    def hold(self, unit, parity, left, right):
        order = self.order(parity)
        self.keep[unit] = product(self.gather(left, order, True), right[...]).astype(BF16)

    def collect(self, order, unit, stage, rows):
        start = pl.multiple_of(self.offset(order, 0, stage), self.rows)
        total = self.keep[unit, pl.ds(start, rows)].astype(F32)
        for source in range(min(stage, self.bits)):
            start = pl.multiple_of(self.offset(order, source, stage), self.rows)
            total = total + self.recv[source][unit, pl.ds(start, rows)].astype(F32)
        return total

    def advance(self, unit, parity, stage):
        order = self.order(parity)
        self.copy(order, unit, stage - 1).wait_recv()
        rows = self.stage_rows(stage)
        total = self.collect(order, unit, stage, rows)
        start = pl.multiple_of(self.offset(order, 0, stage), self.rows)
        self.keep[unit, pl.ds(start, rows)] = total.astype(BF16)
        self.copy(order, unit, stage).start()

    def finish(self, unit, parity):
        order = self.order(parity)
        self.copy(order, unit, self.bits - 1).wait_recv()
        total = self.collect(order, unit, self.bits, self.rows)
        for stage in range(self.bits):
            self.copy(order, unit, stage).wait_send()
        return total


def ffn_kernel(
    plan,
    normed_ref,
    cot_ref,
    left_ref,
    gate_hbm,
    up_hbm,
    down_hbm,
    grads_ref,
    pn_ref,
    pn_recv,
    out_ref,
    out_recv,
    gate_buf,
    up_buf,
    down_buf,
    right_ref,
    pn_acc,
    out_acc,
    out_send,
    weight_sem,
    swap_send,
    swap_recv,
    *refs,
):
    total_rows, width = normed_ref.shape
    blocks = gate_hbm.shape[1] // UNIT
    step_rows = min(256, total_rows)
    half = width // 2
    plan.bind(refs)
    plan.enter()

    def weights(index):
        slot = index % 2
        span = pl.ds(pl.multiple_of(index * UNIT, UNIT), UNIT)
        return [
            pltpu.make_async_copy(gate_hbm.at[:, span], gate_buf.at[slot], weight_sem.at[0, slot]),
            pltpu.make_async_copy(up_hbm.at[:, span], up_buf.at[slot], weight_sem.at[1, slot]),
            pltpu.make_async_copy(down_hbm.at[span], down_buf.at[slot], weight_sem.at[2, slot]),
        ]

    for item in weights(0):
        item.start()
    plan.greet()
    pn_acc[...] = jnp.zeros_like(pn_acc)
    out_acc[...] = jnp.zeros_like(out_acc)

    def swaps():
        return [
            pltpu.make_async_remote_copy(
                src_ref=source,
                dst_ref=target,
                send_sem=swap_send.at[index],
                recv_sem=swap_recv.at[index],
                device_id=plan.other_core(),
                device_id_type=MESH,
            )
            for index, (source, target) in enumerate(((pn_ref, pn_recv), (out_send, out_recv)))
        ]

    def step(index, carry):
        @pl.when(index < blocks)
        def _():
            slot = index % 2

            @pl.when(index + 1 < blocks)
            def _():
                for item in weights(index + 1):
                    item.start()

            for item in weights(index):
                item.wait()
            for first in range(0, total_rows, step_rows):
                rows = pl.ds(first, step_rows)
                normed = normed_ref[rows]
                gate_pre = product(normed, gate_buf[slot])
                up_pre = product(normed, up_buf[slot])
                grad_hidden = product_t(cot_ref[rows], down_buf[slot])
                sigma = jax.nn.sigmoid(gate_pre)
                active = gate_pre * sigma
                right_ref[0, rows] = (
                    grad_hidden * up_pre * (sigma * (1.0 + gate_pre * (1.0 - sigma)))
                ).astype(BF16)
                right_ref[1, rows] = (grad_hidden * active).astype(BF16)
                right_ref[2, rows] = (active * up_pre).astype(BF16)
            for place in range(3):
                unit = index * 3 + place
                plan.begin(unit, unit % 2, left_ref.at[place // 2], right_ref.at[place])
            for first in range(0, total_rows, step_rows):
                rows = pl.ds(first, step_rows)
                pn_acc[rows] += product_t(right_ref[0, rows], gate_buf[slot]) + product_t(
                    right_ref[1, rows], up_buf[slot]
                )
                out_acc[rows] += product(right_ref[2, rows], down_buf[slot])
            for place in range(3):
                unit = index * 3 + place
                plan.hold(unit, unit % 2, left_ref.at[place // 2], right_ref.at[place])

        @pl.when(index == blocks)
        def _():
            own = pl.ds(pl.multiple_of(plan.core * half, half), half)
            other = pl.ds(pl.multiple_of((1 - plan.core) * half, half), half)
            pn_ref[...] = pn_acc[...].astype(BF16)
            out_send[...] = out_acc[:, other].astype(BF16)
            for item in swaps():
                item.start()
            out_ref[...] = out_acc[:, own]

        for stage in range(plan.bits, 0, -1):
            block = index - stage

            @pl.when((block >= 0) & (block < blocks))
            def _(stage=stage, block=block):
                for place in range(3):
                    unit = block * 3 + place
                    if stage < plan.bits:
                        plan.advance(unit, unit % 2, stage)
                    else:
                        span = pl.ds(pl.multiple_of(block * UNIT, UNIT), UNIT)
                        grads_ref[place, :, span] = plan.finish(unit, unit % 2)

        return carry

    lax.fori_loop(0, blocks + plan.bits, step, 0)
    for item in swaps():
        item.wait()


def whole():
    return pl.BlockSpec(memory_space=pltpu.VMEM)


def anywhere():
    return pl.BlockSpec(memory_space=pl.ANY)


def ffn(plan, normed, cotangent, left, gate_weight, up_weight, down_weight):
    total_rows, width = normed.shape
    hidden = gate_weight.shape[1]
    blocks = hidden // UNIT
    half = width // 2
    shape = jax.ShapeDtypeStruct
    return pl.pallas_call(
        functools.partial(ffn_kernel, plan),
        name="ffn",
        out_shape=(
            shape((3, plan.rows, hidden), F32),
            shape((total_rows, width), BF16),
            shape((total_rows, width), BF16),
            shape((total_rows, half), F32),
            shape((total_rows, half), BF16),
        ),
        in_specs=[whole()] * 3 + [anywhere()] * 3,
        out_specs=[whole()] * 5,
        scratch_shapes=[
            pltpu.VMEM((2, width, UNIT), BF16),
            pltpu.VMEM((2, width, UNIT), BF16),
            pltpu.VMEM((2, UNIT, width), BF16),
            pltpu.VMEM((3, total_rows, UNIT), BF16),
            pltpu.VMEM((total_rows, width), F32),
            pltpu.VMEM((total_rows, width), F32),
            pltpu.VMEM((total_rows, half), BF16),
            pltpu.SemaphoreType.DMA((3, 2)),
            pltpu.SemaphoreType.DMA((2,)),
            pltpu.SemaphoreType.DMA((2,)),
        ]
        + plan.scratch(3 * blocks),
        compiler_params=pltpu.CompilerParams(
            collective_id=0, has_side_effects=True, vmem_limit_bytes=VMEM_BYTES
        ),
    )(normed, cotangent, left, gate_weight, up_weight, down_weight)


def back_kernel(
    plan,
    gain_ref,
    tap_ref,
    pn_ref,
    pn_recv,
    cot_ref,
    mixed_ref,
    prior_ref,
    out_weight_ref,
    in_weight_ref,
    left_hbm,
    resid_hbm,
    token_hbm,
    b_hbm,
    c_hbm,
    x_hbm,
    grads_ref,
    tokens_ref,
    small_ref,
    left_ref,
    resid_ref,
    token_ref,
    b_ref,
    c_ref,
    x_ref,
    full_ref,
    gated_ref,
    conv_ref,
    grad_own,
    right_ref,
    part_ref,
    part_recv,
    sums_ref,
    small_send,
    small_recv,
    load_sem,
    left_sem,
    swap_send,
    swap_recv,
    halo_send,
    halo_recv,
    small_send_sem,
    small_recv_sem,
    *refs,
):
    total_rows, width = cot_ref.shape
    half = width // 2
    step = min(256, total_rows)
    steps = total_rows // step
    plan.bind(refs)
    plan.enter()
    seq = lax.axis_index("seq")
    last = plan.seq_size - 1

    def loads(index):
        rows = pl.ds(pl.multiple_of(index * step, step), step)
        pairs = (
            (resid_hbm, resid_ref),
            (b_hbm, b_ref),
            (x_hbm, x_ref),
            (c_hbm, c_ref),
            (token_hbm, token_ref),
        )
        return [
            pltpu.make_async_copy(source.at[rows], target.at[rows], load_sem.at[index, place])
            for place, (source, target) in enumerate(pairs)
        ]

    left_load = pltpu.make_async_copy(left_hbm, left_ref.at[0], left_sem.at[0])
    for index in range(steps):
        for item in loads(index):
            item.start()
    left_load.start()
    plan.greet((-1, 1))
    own = pl.ds(pl.multiple_of(plan.core * half, half), half)
    gain_one, gain_two = gain_ref[0:1], gain_ref[1:2]
    taps = [tap_ref[k : k + 1] for k in range(3)]
    sums_ref[...] = jnp.zeros_like(sums_ref)
    gated_ref[0:8] = prior_ref[...]

    def halo():
        return pltpu.make_async_remote_copy(
            src_ref=conv_ref.at[pl.ds(0, 8)],
            dst_ref=conv_ref.at[pl.ds(total_rows, 8)],
            send_sem=halo_send.at[0],
            recv_sem=halo_recv.at[0],
            device_id=plan.along_seq(-1),
            device_id_type=MESH,
        )

    def first_pass(index, carry):
        start = pl.multiple_of(index * step, step)
        rows = pl.ds(start, step)
        for item in loads(index):
            item.wait()
        resid = resid_ref[rows]
        scale = inverse_rms(resid)
        unit = resid * scale
        grad = pn_ref[rows].astype(F32) + pn_recv[rows].astype(F32)
        sums_ref[0:1] += jnp.sum(grad * unit, axis=0, keepdims=True)
        grad = grad * gain_two
        mean = jnp.mean(grad * unit, axis=-1, keepdims=True)
        grad = cot_ref[rows].astype(F32) + scale * (grad - unit * mean)
        full_ref[...] = grad
        grad_own[rows] = full_ref[:, own]
        rounded = grad.astype(BF16)
        left_ref[1, :, :, rows] = rounded.T.reshape(plan.shards, plan.rows, step)
        grad_mixed = product_t(rounded, out_weight_ref[...])
        gated_ref[pl.ds(start + 8, step)] = b_ref[rows] * x_ref[rows]
        window = gated_ref[pl.ds(start, step + 8)]
        views = [window[6 + k : 6 + k + step] for k in range(3)]
        conv_out = taps[0] * views[0] + taps[1] * views[1] + taps[2] * views[2]
        right_ref[1, rows] = (grad_mixed * conv_out).astype(BF16)
        grad_conv = grad_mixed * c_ref[rows]
        conv_ref[rows] = grad_conv
        for k in range(3):
            sums_ref[1 + k : 2 + k, 0:half] += jnp.sum(grad_conv * views[k], axis=0, keepdims=True)

        @pl.when((index == 0) & (seq > 0))
        def _():
            halo().start()

        return carry

    lax.fori_loop(0, steps, first_pass, 0)
    pieces = half // UNIT
    places = (3, 1, 0, 2)
    units = [(place, piece) for place in places for piece in range(pieces)]

    def right_of(place, piece):
        span = pl.ds(piece * UNIT, UNIT)
        return mixed_ref.at[:, span] if place == 3 else right_ref.at[place, :, span]

    def left_of(place):
        return left_ref.at[1 if place == 3 else 0]

    early = 2 * pieces
    left_load.wait()
    for unit, (place, piece) in enumerate(units[:early]):
        plan.begin(unit, unit % 2, left_of(place), right_of(place, piece))

    @pl.when(seq < last)
    def _():
        halo().wait_recv()

    @pl.when(seq == last)
    def _():
        conv_ref[pl.ds(total_rows, 8)] = jnp.zeros((8, half), F32)

    def second_pass(index, carry):
        start = pl.multiple_of(index * step, step)
        rows = pl.ds(start, step)
        window = conv_ref[pl.ds(start, step + 8)]
        grad_gated = (
            taps[0] * window[2 : 2 + step]
            + taps[1] * window[1 : 1 + step]
            + taps[2] * window[0:step]
        )
        right_ref[0, rows] = (grad_gated * x_ref[rows]).astype(BF16)
        right_ref[2, rows] = (grad_gated * b_ref[rows]).astype(BF16)
        return carry

    lax.fori_loop(0, steps, second_pass, 0)
    for unit, (place, piece) in list(enumerate(units))[early:]:
        plan.begin(unit, unit % 2, left_of(place), right_of(place, piece))

    def swap(index):
        rows = pl.ds(pl.multiple_of(index * step, step), step)
        return pltpu.make_async_remote_copy(
            src_ref=part_ref.at[rows],
            dst_ref=part_recv.at[rows],
            send_sem=swap_send.at[index],
            recv_sem=swap_recv.at[index],
            device_id=plan.other_core(),
            device_id_type=MESH,
        )

    def third_pass(index, carry):
        rows = pl.ds(pl.multiple_of(index * step, step), step)
        total = product_t(right_ref[0, rows], in_weight_ref[0])
        total = total + product_t(right_ref[1, rows], in_weight_ref[1])
        total = total + product_t(right_ref[2, rows], in_weight_ref[2])
        part_ref[rows] = total.astype(BF16)
        swap(index).start()
        return carry

    lax.fori_loop(0, steps, third_pass, 0)
    for unit, (place, piece) in enumerate(units):
        plan.hold(unit, unit % 2, left_of(place), right_of(place, piece))
    for unit in range(len(units)):
        plan.advance(unit, unit % 2, 1)

    def fourth_pass(index, carry):
        rows = pl.ds(pl.multiple_of(index * step, step), step)
        swap(index).wait_recv()
        value = token_ref[rows].astype(F32)
        scale = inverse_rms(value)
        unit = value * scale
        grad = part_ref[rows].astype(F32) + part_recv[rows].astype(F32)
        sums_ref[4:5] += jnp.sum(grad * unit, axis=0, keepdims=True)
        grad = grad * gain_one
        mean = jnp.mean(grad * unit, axis=-1, keepdims=True)
        full_ref[...] = scale * (grad - unit * mean)
        tokens_ref[rows] = grad_own[rows] + full_ref[:, own]
        return carry

    lax.fori_loop(0, steps, fourth_pass, 0)
    small_send[0] = jnp.zeros_like(small_ref)
    small_send[0, 0:3] = sums_ref[1:4, 0:half]
    small_send[0, 3:4] = sums_ref[4:5, own]
    small_send[0, 4:5] = sums_ref[0:1, own]

    def small(bit):
        return pltpu.make_async_remote_copy(
            src_ref=small_send.at[bit],
            dst_ref=small_recv.at[bit],
            send_sem=small_send_sem.at[bit],
            recv_sem=small_recv_sem.at[bit],
            device_id=plan.place(plan.flipped(1 << bit)),
            device_id_type=MESH,
        )

    for bit in range(plan.bits):
        small(bit).start()
        if bit + 2 < plan.bits + 0:
            for unit in range(len(units)):
                plan.advance(unit, unit % 2, bit + 2)
        elif bit == plan.bits - 1:
            for unit, (place, piece) in enumerate(units):
                grads_ref[place, :, piece * UNIT : (piece + 1) * UNIT] = plan.finish(unit, unit % 2)
        small(bit).wait_recv()
        total = small_send[bit] + small_recv[bit]
        if bit + 1 < plan.bits:
            small_send[bit + 1] = total
        else:
            small_ref[...] = total
    for bit in range(plan.bits):
        small(bit).wait_send()

    @pl.when(seq > 0)
    def _():
        halo().wait_send()

    for index in range(steps):
        swap(index).wait_send()


def back(plan, gains, taps, pn, pn_other, cot, mixed, prior, out_weight, in_weight, left, streams):
    total_rows, width = cot.shape
    half = width // 2
    steps = total_rows // min(256, total_rows)
    shape = jax.ShapeDtypeStruct
    dma = pltpu.SemaphoreType.DMA
    return pl.pallas_call(
        functools.partial(back_kernel, plan),
        name="back",
        out_shape=(
            shape((4, plan.rows, half), F32),
            shape((total_rows, half), F32),
            shape((8, half), F32),
        ),
        in_specs=[whole()] * 9 + [anywhere()] * 6,
        out_specs=[whole()] * 3,
        scratch_shapes=[
            pltpu.VMEM((2, plan.shards, plan.rows, total_rows), BF16),
            pltpu.VMEM((total_rows, width), F32),
            pltpu.VMEM((total_rows, width), BF16),
            pltpu.VMEM((total_rows, half), F32),
            pltpu.VMEM((total_rows, half), F32),
            pltpu.VMEM((total_rows, half), F32),
            pltpu.VMEM((total_rows // steps, width), F32),
            pltpu.VMEM((total_rows + 8, half), F32),
            pltpu.VMEM((total_rows + 8, half), F32),
            pltpu.VMEM((total_rows, half), F32),
            pltpu.VMEM((3, total_rows, half), BF16),
            pltpu.VMEM((total_rows, width), BF16),
            pltpu.VMEM((total_rows, width), BF16),
            pltpu.VMEM((8, width), F32),
            pltpu.VMEM((plan.bits, 8, half), F32),
            pltpu.VMEM((plan.bits, 8, half), F32),
            dma((steps, 5)),
            dma((1,)),
            dma((steps,)),
            dma((steps,)),
            dma((1,)),
            dma((1,)),
            dma((plan.bits,)),
            dma((plan.bits,)),
        ]
        + plan.scratch(4 * half // UNIT),
        compiler_params=pltpu.CompilerParams(
            collective_id=1, has_side_effects=True, vmem_limit_bytes=VMEM_BYTES
        ),
    )(gains, taps, pn, pn_other, cot, mixed, prior, out_weight, in_weight, left, *streams)


def local(
    seq_size,
    shards,
    tokens,
    norm1_gain,
    in_weight,
    conv_weight,
    out_weight,
    norm2_gain,
    gate_weight,
    up_weight,
    down_weight,
    out_cotangent,
):
    seqs, length, width = tokens.shape
    half = in_weight.shape[2]
    total_rows = seqs * length
    chunk_rows = width // shards
    plan = Halving(seq_size, shards, chunk_rows)
    start = lax.axis_index("tensor") * half
    token_float = tokens.reshape(total_rows, width).astype(F32)
    normed = (token_float * inverse_rms(token_float) * norm1_gain).astype(BF16)
    b_signal = product(normed, in_weight[0])
    c_signal = product(normed, in_weight[1])
    x_signal = product(normed, in_weight[2])
    gated = (b_signal * x_signal).reshape(seqs, length, half)
    prior = shifted(gated[:, length - 2 :], "seq", 1)
    extended = jnp.concatenate([prior, gated], axis=1)
    conv_out = (
        conv_weight[0] * extended[:, 0:length]
        + conv_weight[1] * extended[:, 1 : length + 1]
        + conv_weight[2] * extended[:, 2 : length + 2]
    ).reshape(total_rows, half)
    mixed_in = (c_signal * conv_out).astype(BF16)
    resid = token_float + lax.psum(product(mixed_in, out_weight), "tensor")
    normed_two = (resid * inverse_rms(resid) * norm2_gain).astype(BF16)
    cotangent = lax.all_gather(
        out_cotangent.reshape(total_rows, half), "tensor", axis=1, tiled=True
    )
    left = jnp.stack([normed_two.T, cotangent.T]).reshape(2, shards, chunk_rows, total_rows)
    ffn_grads, pn_own, pn_other, out_own, out_other = ffn(
        plan, normed_two, cotangent, left, gate_weight, up_weight, down_weight
    )
    gate_grad, up_grad, down_grad = ffn_grads[0], ffn_grads[1], ffn_grads[2].T
    block_out = (
        (own_columns(resid, start, half) + out_own + out_other.astype(F32))
        .astype(BF16)
        .reshape(seqs, length, half)
    )
    mix_grads, tokens_grad, small = back(
        plan,
        jnp.stack([norm1_gain, norm2_gain]),
        conv_weight,
        pn_own,
        pn_other,
        cotangent,
        mixed_in,
        jnp.pad(prior[0], ((6, 0), (0, 0))),
        out_weight,
        in_weight,
        normed.T.reshape(shards, chunk_rows, total_rows),
        (resid, tokens.reshape(total_rows, width), b_signal, c_signal, x_signal),
    )
    in_grad, out_grad = mix_grads[0:3], mix_grads[3].T
    conv_grad, norm1_grad, norm2_grad = small[0:3], small[3], small[4]
    tokens_grad = tokens_grad.reshape(seqs, length, half)
    return (
        block_out,
        tokens_grad,
        norm1_grad,
        in_grad,
        conv_grad,
        out_grad,
        norm2_grad,
        gate_grad,
        up_grad,
        down_grad,
    )


def solution(mesh):
    seq_size = mesh.shape["seq"]
    shards = mesh.shape["dp"] * seq_size
    return jax.shard_map(
        functools.partial(local, seq_size, shards),
        mesh=mesh,
        in_specs=(
            P("dp", "seq", None),
            P(),
            P(None, None, "tensor"),
            P(None, "tensor"),
            P("tensor", None),
            P(),
            P(None, "tensor"),
            P(None, "tensor"),
            P("tensor", None),
            P("dp", "seq", "tensor"),
        ),
        out_specs=(
            P("dp", "seq", "tensor"),
            P("dp", "seq", "tensor"),
            P("tensor"),
            P(None, ("dp", "seq"), "tensor"),
            P(None, "tensor"),
            P("tensor", ("dp", "seq")),
            P("tensor"),
            P(("dp", "seq"), "tensor"),
            P(("dp", "seq"), "tensor"),
            P("tensor", ("dp", "seq")),
        ),
        check_vma=False,
    )
```

```python
import functools

import jax
import jax.numpy as jnp
from jax import lax
from jax.experimental import pallas as pl
from jax.experimental.pallas import tpu as pltpu
from jax.sharding import PartitionSpec as P

EPSILON = 1e-05
MESH = pl.DeviceIdType.MESH
UNIT = 256
VMEM_BYTES = 63 * 1024 * 1024
F32 = jnp.float32
BF16 = jnp.bfloat16


def inverse_rms(values):
    return lax.rsqrt(jnp.mean(values * values, axis=-1, keepdims=True) + EPSILON)


def product(left, right):
    return jnp.dot(left, right, preferred_element_type=F32)


def product_t(left, right):
    return lax.dot_general(left, right, (((1,), (1,)), ((), ())), preferred_element_type=F32)


def own_columns(values, start, count):
    return lax.dynamic_slice_in_dim(values, start, count, 1)


class Halving:
    def __init__(self, seq_size, shards, rows):
        self.seq_size = seq_size
        self.bits = shards.bit_length() - 1
        self.shards = shards
        self.rows = rows

    def stage_rows(self, stage):
        return self.rows << (self.bits - 1 - stage)

    def enter(self):
        self.me = lax.axis_index("dp") * self.seq_size + lax.axis_index("seq")
        self.core = lax.axis_index("tensor")

    def place(self, flat):
        return (flat // self.seq_size, flat % self.seq_size, self.core)

    def flipped(self, weight):
        return self.me + (1 - 2 * ((self.me // weight) % 2)) * weight

    def other_core(self):
        return (self.me // self.seq_size, self.me % self.seq_size, 1 - self.core)

    def along_seq(self, steps):
        seq = (self.me + steps) % self.seq_size
        return (self.me // self.seq_size, seq, self.core)

    def greet(self, steps=(), shards=True):
        barrier = pltpu.get_barrier_semaphore()
        partners = [self.other_core()]
        if shards:
            partners += [self.place(self.flipped(1 << bit)) for bit in range(self.bits)]
        partners.extend(self.along_seq(count) for count in steps)
        for partner in partners:
            pl.semaphore_signal(barrier, inc=1, device_id=partner, device_id_type=MESH)
        pl.semaphore_wait(barrier, len(partners))

    def order(self, parity):
        top = self.shards // 2
        high = (self.me // top) % 2
        low = self.me % 2
        first = (top + parity * (1 - top), high + parity * (low - high))
        third = (1 + parity * (top - 1), low + parity * (high - low))
        middle = [(2, (self.me // 2) % 2)]
        rest = [(1 << bit, (self.me // (1 << bit)) % 2) for bit in range(2, self.bits - 1)]
        return [first] + middle + [third] + rest

    def chunks(self, order, keep):
        weight, bit = order[0]
        base = (bit if keep else 1 - bit) * weight
        found = []
        for code in range(self.shards // 2):
            chunk = base
            for place in range(1, self.bits):
                if (code >> (self.bits - 1 - place)) & 1:
                    chunk = chunk + order[place][0]
            found.append(chunk)
        return found

    def offset(self, order, source, stage):
        total = 0
        for place in range(source + 1, min(stage, self.bits - 1) + 1):
            bit = order[place][1]
            if place == stage:
                bit = 1 - bit
            total = total + bit * (1 << (self.bits - 1 - place))
        return total * self.rows

    def scratch(self, units):
        half = self.stage_rows(0)
        return (
            [pltpu.VMEM((units, half, UNIT), BF16), pltpu.VMEM((units, half, UNIT), BF16)]
            + [pltpu.VMEM((units, self.stage_rows(s), UNIT), BF16) for s in range(self.bits)]
            + [
                pltpu.SemaphoreType.DMA((self.bits, units)),
                pltpu.SemaphoreType.DMA((self.bits, units)),
            ]
        )

    def bind(self, refs):
        self.first, self.keep = refs[0], refs[1]
        self.recv = refs[2 : 2 + self.bits]
        self.send_sem, self.recv_sem = refs[2 + self.bits :]

    def copy(self, order, unit, stage):
        weight, bit = order[stage]
        if stage == 0:
            source = self.first.at[unit]
        else:
            start = pl.multiple_of(self.offset(order, 0, stage), self.rows)
            source = self.keep.at[unit, pl.ds(start, self.stage_rows(stage))]
        return pltpu.make_async_remote_copy(
            src_ref=source,
            dst_ref=self.recv[stage].at[unit],
            send_sem=self.send_sem.at[stage, unit],
            recv_sem=self.recv_sem.at[stage, unit],
            device_id=self.place(self.me + (1 - 2 * bit) * weight),
            device_id_type=MESH,
        )

    def gather(self, left, order, keep):
        return jnp.concatenate([left[chunk] for chunk in self.chunks(order, keep)], axis=0)

    def begin(self, unit, parity, left, right):
        order = self.order(parity)
        self.first[unit] = product(self.gather(left, order, False), right[...]).astype(BF16)
        self.copy(order, unit, 0).start()

    def hold(self, unit, parity, left, right):
        order = self.order(parity)
        self.keep[unit] = product(self.gather(left, order, True), right[...]).astype(BF16)

    def collect(self, order, unit, stage, rows):
        start = pl.multiple_of(self.offset(order, 0, stage), self.rows)
        total = self.keep[unit, pl.ds(start, rows)].astype(F32)
        for source in range(min(stage, self.bits)):
            start = pl.multiple_of(self.offset(order, source, stage), self.rows)
            total = total + self.recv[source][unit, pl.ds(start, rows)].astype(F32)
        return total

    def advance(self, unit, parity, stage):
        order = self.order(parity)
        self.copy(order, unit, stage - 1).wait_recv()
        rows = self.stage_rows(stage)
        total = self.collect(order, unit, stage, rows)
        start = pl.multiple_of(self.offset(order, 0, stage), self.rows)
        self.keep[unit, pl.ds(start, rows)] = total.astype(BF16)
        self.copy(order, unit, stage).start()

    def finish(self, unit, parity):
        order = self.order(parity)
        self.copy(order, unit, self.bits - 1).wait_recv()
        total = self.collect(order, unit, self.bits, self.rows)
        for stage in range(self.bits):
            self.copy(order, unit, stage).wait_send()
        return total


def front_kernel(
    plan,
    gain_ref,
    tap_ref,
    token_hbm,
    cot_hbm,
    in_weight_hbm,
    out_weight_hbm,
    normed_ref,
    cot_ref,
    left_ref,
    resid_hbm,
    b_hbm,
    c_hbm,
    x_hbm,
    mixed_hbm,
    first_hbm,
    prior_ref,
    token_ref,
    edge_ref,
    in_weight_ref,
    out_weight_ref,
    b_ref,
    c_ref,
    x_ref,
    gated_ref,
    mixed_ref,
    first_ref,
    resid_ref,
    part_ref,
    part_recv,
    token_sem,
    weight_sem,
    cot_sem,
    cot_send,
    cot_recv,
    edge_send,
    edge_recv,
    swap_send,
    swap_recv,
    store_sem,
):
    total_rows, width = token_ref.shape
    half = width // 2
    step = min(256, total_rows)
    steps = total_rows // step
    edge = edge_ref.shape[0]
    plan.enter()
    seq = lax.axis_index("seq")
    last = plan.seq_size - 1

    def span(index):
        return pl.ds(pl.multiple_of(index * step, step), step)

    def load(index):
        rows = span(index)
        return pltpu.make_async_copy(token_hbm.at[rows], token_ref.at[rows], token_sem.at[index])

    own = pl.ds(pl.multiple_of(plan.core * half, half), half)
    for index in range(steps):
        load(index).start()
    weights = [
        pltpu.make_async_copy(in_weight_hbm, in_weight_ref, weight_sem.at[0]),
        pltpu.make_async_copy(out_weight_hbm, out_weight_ref, weight_sem.at[1]),
    ]
    for item in weights:
        item.start()
    cot_own = pltpu.make_async_copy(cot_hbm, cot_ref.at[:, own], cot_sem.at[0])
    cot_own.start()
    plan.greet((-1, 1), shards=False)
    cot_swap = pltpu.make_async_remote_copy(
        src_ref=cot_hbm,
        dst_ref=cot_ref.at[:, own],
        send_sem=cot_send.at[0],
        recv_sem=cot_recv.at[0],
        device_id=plan.other_core(),
        device_id_type=MESH,
    )

    def edge_copy():
        return pltpu.make_async_remote_copy(
            src_ref=token_hbm.at[pl.ds(total_rows - edge, edge)],
            dst_ref=edge_ref,
            send_sem=edge_send.at[0],
            recv_sem=edge_recv.at[0],
            device_id=plan.along_seq(1),
            device_id_type=MESH,
        )

    @pl.when(seq < last)
    def _():
        edge_copy().start()

    cot_swap.start()
    gain_one, gain_two = gain_ref[0:1], gain_ref[1:2]
    taps = [tap_ref[k : k + 1] for k in range(3)]

    def stores(index, pairs, first):
        return [
            pltpu.make_async_copy(source, target, store_sem.at[first + place, index])
            for place, (source, target) in enumerate(pairs)
        ]

    def early_stores(index):
        rows = span(index)
        return stores(
            index,
            (
                (b_ref.at[rows], b_hbm.at[rows]),
                (c_ref.at[rows], c_hbm.at[rows]),
                (x_ref.at[rows], x_hbm.at[rows]),
                (first_ref.at[:, :, rows], first_hbm.at[:, :, rows]),
            ),
            0,
        )

    def late_stores(index):
        rows = span(index)
        return stores(
            index,
            (
                (mixed_ref.at[rows], mixed_hbm.at[rows]),
                (resid_ref.at[rows], resid_hbm.at[rows]),
            ),
            4,
        )

    def normalise(value, gain):
        return (value * inverse_rms(value) * gain).astype(BF16)

    weights[0].wait()

    def first_pass(index, carry):
        start = pl.multiple_of(index * step, step)
        rows = pl.ds(start, step)
        load(index).wait()
        normed = normalise(token_ref[rows].astype(F32), gain_one)
        b_signal = product(normed, in_weight_ref[0])
        x_signal = product(normed, in_weight_ref[2])
        b_ref[rows] = b_signal
        x_ref[rows] = x_signal
        gated_ref[pl.ds(start + 8, step)] = b_signal * x_signal
        c_ref[rows] = product(normed, in_weight_ref[1])
        first_ref[:, :, rows] = normed.T.reshape(plan.shards, plan.rows, step)
        for item in early_stores(index):
            item.start()
        return carry

    lax.fori_loop(0, steps, first_pass, 0)

    @pl.when(seq > 0)
    def _():
        edge_copy().wait_recv()

    @pl.when(seq == 0)
    def _():
        edge_ref[...] = jnp.zeros_like(edge_ref)

    normed = normalise(edge_ref[...].astype(F32), gain_one)
    gated = product(normed, in_weight_ref[0]) * product(normed, in_weight_ref[2])
    gated_ref[0:8] = gated[edge - 8 : edge]
    prior_ref[...] = gated[edge - 8 : edge]
    weights[1].wait()

    def swap(index):
        rows = span(index)
        return pltpu.make_async_remote_copy(
            src_ref=part_ref.at[rows],
            dst_ref=part_recv.at[rows],
            send_sem=swap_send.at[index],
            recv_sem=swap_recv.at[index],
            device_id=plan.other_core(),
            device_id_type=MESH,
        )

    def second_pass(index, carry):
        start = pl.multiple_of(index * step, step)
        rows = pl.ds(start, step)
        window = gated_ref[pl.ds(start, step + 8)]
        views = [window[6 + k : 6 + k + step] for k in range(3)]
        conv_out = taps[0] * views[0] + taps[1] * views[1] + taps[2] * views[2]
        mixed = (c_ref[rows] * conv_out).astype(BF16)
        mixed_ref[rows] = mixed
        part = product(mixed, out_weight_ref[...])
        part_ref[rows] = part.astype(BF16)
        swap(index).start()
        resid_ref[rows] = token_ref[rows].astype(F32) + part
        return carry

    lax.fori_loop(0, steps, second_pass, 0)
    cot_own.wait()
    cot_swap.wait_recv()

    def third_pass(index, carry):
        rows = span(index)
        swap(index).wait_recv()
        resid = resid_ref[rows] + part_recv[rows].astype(F32)
        resid_ref[rows] = resid
        for item in late_stores(index):
            item.start()
        normed = normalise(resid, gain_two)
        normed_ref[rows] = normed
        left_ref[0, :, :, rows] = normed.T.reshape(plan.shards, plan.rows, step)
        left_ref[1, :, :, rows] = cot_ref[rows].T.reshape(plan.shards, plan.rows, step)
        return carry

    lax.fori_loop(0, steps, third_pass, 0)
    for index in range(steps):
        for item in early_stores(index) + late_stores(index):
            item.wait()
        swap(index).wait_send()
    cot_swap.wait_send()

    @pl.when(seq < last)
    def _():
        edge_copy().wait_send()


def front(plan, gains, taps, tokens, cotangent, in_weight, out_weight):
    total_rows, width = tokens.shape
    half = in_weight.shape[2]
    steps = total_rows // min(256, total_rows)
    shape = jax.ShapeDtypeStruct
    dma = pltpu.SemaphoreType.DMA
    chunked = (plan.shards, plan.rows, total_rows)
    return pl.pallas_call(
        functools.partial(front_kernel, plan),
        name="front",
        out_shape=(
            shape((total_rows, width), BF16),
            shape((total_rows, width), BF16),
            shape((2,) + chunked, BF16),
            shape((total_rows, width), F32),
            shape((total_rows, half), F32),
            shape((total_rows, half), F32),
            shape((total_rows, half), F32),
            shape((total_rows, half), BF16),
            shape(chunked, BF16),
            shape((8, half), F32),
        ),
        in_specs=[whole()] * 2 + [anywhere()] * 4,
        out_specs=[whole()] * 3 + [anywhere()] * 6 + [whole()],
        scratch_shapes=[
            pltpu.VMEM((total_rows, width), BF16),
            pltpu.VMEM((16, width), BF16),
            pltpu.VMEM((3, width, half), BF16),
            pltpu.VMEM((half, width), BF16),
            pltpu.VMEM((total_rows, half), F32),
            pltpu.VMEM((total_rows, half), F32),
            pltpu.VMEM((total_rows, half), F32),
            pltpu.VMEM((total_rows + 8, half), F32),
            pltpu.VMEM((total_rows, half), BF16),
            pltpu.VMEM(chunked, BF16),
            pltpu.VMEM((total_rows, width), F32),
            pltpu.VMEM((total_rows, width), BF16),
            pltpu.VMEM((total_rows, width), BF16),
            dma((steps,)),
            dma((2,)),
            dma((1,)),
            dma((1,)),
            dma((1,)),
            dma((1,)),
            dma((1,)),
            dma((steps,)),
            dma((steps,)),
            dma((6, steps)),
        ],
        compiler_params=pltpu.CompilerParams(
            collective_id=2, has_side_effects=True, vmem_limit_bytes=VMEM_BYTES
        ),
    )(gains, taps, tokens, cotangent, in_weight, out_weight)


def ffn_kernel(
    plan,
    normed_ref,
    cot_ref,
    left_ref,
    gate_hbm,
    up_hbm,
    down_hbm,
    grads_ref,
    pn_ref,
    pn_recv,
    out_ref,
    out_recv,
    gate_buf,
    up_buf,
    down_buf,
    right_ref,
    pn_acc,
    out_acc,
    out_send,
    weight_sem,
    swap_send,
    swap_recv,
    *refs,
):
    total_rows, width = normed_ref.shape
    blocks = gate_hbm.shape[1] // UNIT
    step_rows = min(256, total_rows)
    half = width // 2
    plan.bind(refs)
    plan.enter()

    def weights(index):
        slot = index % 2
        span = pl.ds(pl.multiple_of(index * UNIT, UNIT), UNIT)
        return [
            pltpu.make_async_copy(gate_hbm.at[:, span], gate_buf.at[slot], weight_sem.at[0, slot]),
            pltpu.make_async_copy(up_hbm.at[:, span], up_buf.at[slot], weight_sem.at[1, slot]),
            pltpu.make_async_copy(down_hbm.at[span], down_buf.at[slot], weight_sem.at[2, slot]),
        ]

    for item in weights(0):
        item.start()
    plan.greet()
    pn_acc[...] = jnp.zeros_like(pn_acc)
    out_acc[...] = jnp.zeros_like(out_acc)

    def swaps():
        return [
            pltpu.make_async_remote_copy(
                src_ref=source,
                dst_ref=target,
                send_sem=swap_send.at[index],
                recv_sem=swap_recv.at[index],
                device_id=plan.other_core(),
                device_id_type=MESH,
            )
            for index, (source, target) in enumerate(((pn_ref, pn_recv), (out_send, out_recv)))
        ]

    def step(index, carry):
        @pl.when(index < blocks)
        def _():
            slot = index % 2

            @pl.when(index + 1 < blocks)
            def _():
                for item in weights(index + 1):
                    item.start()

            for item in weights(index):
                item.wait()
            for first in range(0, total_rows, step_rows):
                rows = pl.ds(first, step_rows)
                normed = normed_ref[rows]
                gate_pre = product(normed, gate_buf[slot])
                up_pre = product(normed, up_buf[slot])
                grad_hidden = product_t(cot_ref[rows], down_buf[slot])
                sigma = jax.nn.sigmoid(gate_pre)
                active = gate_pre * sigma
                right_ref[0, rows] = (
                    grad_hidden * up_pre * (sigma * (1.0 + gate_pre * (1.0 - sigma)))
                ).astype(BF16)
                right_ref[1, rows] = (grad_hidden * active).astype(BF16)
                right_ref[2, rows] = (active * up_pre).astype(BF16)
            for place in range(3):
                unit = index * 3 + place
                plan.begin(unit, unit % 2, left_ref.at[place // 2], right_ref.at[place])
            for first in range(0, total_rows, step_rows):
                rows = pl.ds(first, step_rows)
                pn_acc[rows] += product_t(right_ref[0, rows], gate_buf[slot]) + product_t(
                    right_ref[1, rows], up_buf[slot]
                )
                out_acc[rows] += product(right_ref[2, rows], down_buf[slot])
            for place in range(3):
                unit = index * 3 + place
                plan.hold(unit, unit % 2, left_ref.at[place // 2], right_ref.at[place])

        @pl.when(index == blocks)
        def _():
            own = pl.ds(pl.multiple_of(plan.core * half, half), half)
            other = pl.ds(pl.multiple_of((1 - plan.core) * half, half), half)
            pn_ref[...] = pn_acc[...].astype(BF16)
            out_send[...] = out_acc[:, other].astype(BF16)
            for item in swaps():
                item.start()
            out_ref[...] = out_acc[:, own]

        for stage in range(plan.bits, 0, -1):
            block = index - stage

            @pl.when((block >= 0) & (block < blocks))
            def _(stage=stage, block=block):
                for place in range(3):
                    unit = block * 3 + place
                    if stage < plan.bits:
                        plan.advance(unit, unit % 2, stage)
                    else:
                        span = pl.ds(pl.multiple_of(block * UNIT, UNIT), UNIT)
                        grads_ref[place, :, span] = plan.finish(unit, unit % 2)

        return carry

    lax.fori_loop(0, blocks + plan.bits, step, 0)
    for item in swaps():
        item.wait()


def whole():
    return pl.BlockSpec(memory_space=pltpu.VMEM)


def anywhere():
    return pl.BlockSpec(memory_space=pl.ANY)


def ffn(plan, normed, cotangent, left, gate_weight, up_weight, down_weight):
    total_rows, width = normed.shape
    hidden = gate_weight.shape[1]
    blocks = hidden // UNIT
    half = width // 2
    shape = jax.ShapeDtypeStruct
    return pl.pallas_call(
        functools.partial(ffn_kernel, plan),
        name="ffn",
        out_shape=(
            shape((3, plan.rows, hidden), F32),
            shape((total_rows, width), BF16),
            shape((total_rows, width), BF16),
            shape((total_rows, half), F32),
            shape((total_rows, half), BF16),
        ),
        in_specs=[whole()] * 3 + [anywhere()] * 3,
        out_specs=[whole()] * 5,
        scratch_shapes=[
            pltpu.VMEM((2, width, UNIT), BF16),
            pltpu.VMEM((2, width, UNIT), BF16),
            pltpu.VMEM((2, UNIT, width), BF16),
            pltpu.VMEM((3, total_rows, UNIT), BF16),
            pltpu.VMEM((total_rows, width), F32),
            pltpu.VMEM((total_rows, width), F32),
            pltpu.VMEM((total_rows, half), BF16),
            pltpu.SemaphoreType.DMA((3, 2)),
            pltpu.SemaphoreType.DMA((2,)),
            pltpu.SemaphoreType.DMA((2,)),
        ]
        + plan.scratch(3 * blocks),
        compiler_params=pltpu.CompilerParams(
            collective_id=0, has_side_effects=True, vmem_limit_bytes=VMEM_BYTES
        ),
    )(normed, cotangent, left, gate_weight, up_weight, down_weight)


def back_kernel(
    plan,
    gain_ref,
    tap_ref,
    pn_ref,
    pn_recv,
    cot_ref,
    mixed_ref,
    prior_ref,
    out_weight_ref,
    in_weight_ref,
    left_hbm,
    resid_hbm,
    token_hbm,
    b_hbm,
    c_hbm,
    x_hbm,
    grads_ref,
    tokens_ref,
    small_ref,
    left_ref,
    resid_ref,
    token_ref,
    b_ref,
    c_ref,
    x_ref,
    full_ref,
    gated_ref,
    conv_ref,
    grad_own,
    right_ref,
    part_ref,
    part_recv,
    sums_ref,
    small_send,
    small_recv,
    load_sem,
    left_sem,
    swap_send,
    swap_recv,
    halo_send,
    halo_recv,
    small_send_sem,
    small_recv_sem,
    *refs,
):
    total_rows, width = cot_ref.shape
    half = width // 2
    step = min(256, total_rows)
    steps = total_rows // step
    plan.bind(refs)
    plan.enter()
    seq = lax.axis_index("seq")
    last = plan.seq_size - 1

    def loads(index):
        rows = pl.ds(pl.multiple_of(index * step, step), step)
        pairs = (
            (resid_hbm, resid_ref),
            (b_hbm, b_ref),
            (x_hbm, x_ref),
            (c_hbm, c_ref),
            (token_hbm, token_ref),
        )
        return [
            pltpu.make_async_copy(source.at[rows], target.at[rows], load_sem.at[index, place])
            for place, (source, target) in enumerate(pairs)
        ]

    left_load = pltpu.make_async_copy(left_hbm, left_ref.at[0], left_sem.at[0])
    for index in range(steps):
        for item in loads(index):
            item.start()
    left_load.start()
    plan.greet((-1, 1))
    own = pl.ds(pl.multiple_of(plan.core * half, half), half)
    gain_one, gain_two = gain_ref[0:1], gain_ref[1:2]
    taps = [tap_ref[k : k + 1] for k in range(3)]
    sums_ref[...] = jnp.zeros_like(sums_ref)
    gated_ref[0:8] = prior_ref[...]

    def halo():
        return pltpu.make_async_remote_copy(
            src_ref=conv_ref.at[pl.ds(0, 8)],
            dst_ref=conv_ref.at[pl.ds(total_rows, 8)],
            send_sem=halo_send.at[0],
            recv_sem=halo_recv.at[0],
            device_id=plan.along_seq(-1),
            device_id_type=MESH,
        )

    def first_pass(index, carry):
        start = pl.multiple_of(index * step, step)
        rows = pl.ds(start, step)
        for item in loads(index):
            item.wait()
        resid = resid_ref[rows]
        scale = inverse_rms(resid)
        unit = resid * scale
        grad = pn_ref[rows].astype(F32) + pn_recv[rows].astype(F32)
        sums_ref[0:1] += jnp.sum(grad * unit, axis=0, keepdims=True)
        grad = grad * gain_two
        mean = jnp.mean(grad * unit, axis=-1, keepdims=True)
        grad = cot_ref[rows].astype(F32) + scale * (grad - unit * mean)
        full_ref[...] = grad
        grad_own[rows] = full_ref[:, own]
        rounded = grad.astype(BF16)
        left_ref[1, :, :, rows] = rounded.T.reshape(plan.shards, plan.rows, step)
        grad_mixed = product_t(rounded, out_weight_ref[...])
        gated_ref[pl.ds(start + 8, step)] = b_ref[rows] * x_ref[rows]
        window = gated_ref[pl.ds(start, step + 8)]
        views = [window[6 + k : 6 + k + step] for k in range(3)]
        conv_out = taps[0] * views[0] + taps[1] * views[1] + taps[2] * views[2]
        right_ref[1, rows] = (grad_mixed * conv_out).astype(BF16)
        grad_conv = grad_mixed * c_ref[rows]
        conv_ref[rows] = grad_conv
        for k in range(3):
            sums_ref[1 + k : 2 + k, 0:half] += jnp.sum(grad_conv * views[k], axis=0, keepdims=True)

        @pl.when((index == 0) & (seq > 0))
        def _():
            halo().start()

        return carry

    lax.fori_loop(0, steps, first_pass, 0)
    pieces = half // UNIT
    places = (3, 1, 0, 2)
    units = [(place, piece) for place in places for piece in range(pieces)]

    def right_of(place, piece):
        span = pl.ds(piece * UNIT, UNIT)
        return mixed_ref.at[:, span] if place == 3 else right_ref.at[place, :, span]

    def left_of(place):
        return left_ref.at[1 if place == 3 else 0]

    early = 2 * pieces
    left_load.wait()
    for unit, (place, piece) in enumerate(units[:early]):
        plan.begin(unit, unit % 2, left_of(place), right_of(place, piece))

    @pl.when(seq < last)
    def _():
        halo().wait_recv()

    @pl.when(seq == last)
    def _():
        conv_ref[pl.ds(total_rows, 8)] = jnp.zeros((8, half), F32)

    def second_pass(index, carry):
        start = pl.multiple_of(index * step, step)
        rows = pl.ds(start, step)
        window = conv_ref[pl.ds(start, step + 8)]
        grad_gated = (
            taps[0] * window[2 : 2 + step]
            + taps[1] * window[1 : 1 + step]
            + taps[2] * window[0:step]
        )
        right_ref[0, rows] = (grad_gated * x_ref[rows]).astype(BF16)
        right_ref[2, rows] = (grad_gated * b_ref[rows]).astype(BF16)
        return carry

    lax.fori_loop(0, steps, second_pass, 0)
    for unit, (place, piece) in list(enumerate(units))[early:]:
        plan.begin(unit, unit % 2, left_of(place), right_of(place, piece))

    def swap(index):
        rows = pl.ds(pl.multiple_of(index * step, step), step)
        return pltpu.make_async_remote_copy(
            src_ref=part_ref.at[rows],
            dst_ref=part_recv.at[rows],
            send_sem=swap_send.at[index],
            recv_sem=swap_recv.at[index],
            device_id=plan.other_core(),
            device_id_type=MESH,
        )

    def third_pass(index, carry):
        rows = pl.ds(pl.multiple_of(index * step, step), step)
        total = product_t(right_ref[0, rows], in_weight_ref[0])
        total = total + product_t(right_ref[1, rows], in_weight_ref[1])
        total = total + product_t(right_ref[2, rows], in_weight_ref[2])
        part_ref[rows] = total.astype(BF16)
        swap(index).start()
        return carry

    lax.fori_loop(0, steps, third_pass, 0)
    for unit, (place, piece) in enumerate(units):
        plan.hold(unit, unit % 2, left_of(place), right_of(place, piece))
    for unit in range(len(units)):
        plan.advance(unit, unit % 2, 1)

    def fourth_pass(index, carry):
        rows = pl.ds(pl.multiple_of(index * step, step), step)
        swap(index).wait_recv()
        value = token_ref[rows].astype(F32)
        scale = inverse_rms(value)
        unit = value * scale
        grad = part_ref[rows].astype(F32) + part_recv[rows].astype(F32)
        sums_ref[4:5] += jnp.sum(grad * unit, axis=0, keepdims=True)
        grad = grad * gain_one
        mean = jnp.mean(grad * unit, axis=-1, keepdims=True)
        full_ref[...] = scale * (grad - unit * mean)
        tokens_ref[rows] = grad_own[rows] + full_ref[:, own]
        return carry

    lax.fori_loop(0, steps, fourth_pass, 0)
    small_send[0] = jnp.zeros_like(small_ref)
    small_send[0, 0:3] = sums_ref[1:4, 0:half]
    small_send[0, 3:4] = sums_ref[4:5, own]
    small_send[0, 4:5] = sums_ref[0:1, own]

    def small(bit):
        return pltpu.make_async_remote_copy(
            src_ref=small_send.at[bit],
            dst_ref=small_recv.at[bit],
            send_sem=small_send_sem.at[bit],
            recv_sem=small_recv_sem.at[bit],
            device_id=plan.place(plan.flipped(1 << bit)),
            device_id_type=MESH,
        )

    for bit in range(plan.bits):
        small(bit).start()
        if bit + 2 < plan.bits + 0:
            for unit in range(len(units)):
                plan.advance(unit, unit % 2, bit + 2)
        elif bit == plan.bits - 1:
            for unit, (place, piece) in enumerate(units):
                grads_ref[place, :, piece * UNIT : (piece + 1) * UNIT] = plan.finish(unit, unit % 2)
        small(bit).wait_recv()
        total = small_send[bit] + small_recv[bit]
        if bit + 1 < plan.bits:
            small_send[bit + 1] = total
        else:
            small_ref[...] = total
    for bit in range(plan.bits):
        small(bit).wait_send()

    @pl.when(seq > 0)
    def _():
        halo().wait_send()

    for index in range(steps):
        swap(index).wait_send()


def back(plan, gains, taps, pn, pn_other, cot, mixed, prior, out_weight, in_weight, left, streams):
    total_rows, width = cot.shape
    half = width // 2
    steps = total_rows // min(256, total_rows)
    shape = jax.ShapeDtypeStruct
    dma = pltpu.SemaphoreType.DMA
    return pl.pallas_call(
        functools.partial(back_kernel, plan),
        name="back",
        out_shape=(
            shape((4, plan.rows, half), F32),
            shape((total_rows, half), F32),
            shape((8, half), F32),
        ),
        in_specs=[whole()] * 9 + [anywhere()] * 6,
        out_specs=[whole()] * 3,
        scratch_shapes=[
            pltpu.VMEM((2, plan.shards, plan.rows, total_rows), BF16),
            pltpu.VMEM((total_rows, width), F32),
            pltpu.VMEM((total_rows, width), BF16),
            pltpu.VMEM((total_rows, half), F32),
            pltpu.VMEM((total_rows, half), F32),
            pltpu.VMEM((total_rows, half), F32),
            pltpu.VMEM((total_rows // steps, width), F32),
            pltpu.VMEM((total_rows + 8, half), F32),
            pltpu.VMEM((total_rows + 8, half), F32),
            pltpu.VMEM((total_rows, half), F32),
            pltpu.VMEM((3, total_rows, half), BF16),
            pltpu.VMEM((total_rows, width), BF16),
            pltpu.VMEM((total_rows, width), BF16),
            pltpu.VMEM((8, width), F32),
            pltpu.VMEM((plan.bits, 8, half), F32),
            pltpu.VMEM((plan.bits, 8, half), F32),
            dma((steps, 5)),
            dma((1,)),
            dma((steps,)),
            dma((steps,)),
            dma((1,)),
            dma((1,)),
            dma((plan.bits,)),
            dma((plan.bits,)),
        ]
        + plan.scratch(4 * half // UNIT),
        compiler_params=pltpu.CompilerParams(
            collective_id=1, has_side_effects=True, vmem_limit_bytes=VMEM_BYTES
        ),
    )(gains, taps, pn, pn_other, cot, mixed, prior, out_weight, in_weight, left, *streams)


def local(
    seq_size,
    shards,
    tokens,
    norm1_gain,
    in_weight,
    conv_weight,
    out_weight,
    norm2_gain,
    gate_weight,
    up_weight,
    down_weight,
    out_cotangent,
):
    seqs, length, width = tokens.shape
    assert seqs == 1
    half = in_weight.shape[2]
    total_rows = seqs * length
    chunk_rows = width // shards
    plan = Halving(seq_size, shards, chunk_rows)
    start = lax.axis_index("tensor") * half
    gains = jnp.stack([norm1_gain, norm2_gain])
    tokens = tokens.reshape(total_rows, width)
    normed_two, cotangent, left, resid, b_signal, c_signal, x_signal, mixed_in, first, prior = front(
        plan,
        gains,
        conv_weight,
        tokens,
        out_cotangent.reshape(total_rows, half),
        in_weight,
        out_weight,
    )
    ffn_grads, pn_own, pn_other, out_own, out_other = ffn(
        plan, normed_two, cotangent, left, gate_weight, up_weight, down_weight
    )
    gate_grad, up_grad, down_grad = ffn_grads[0], ffn_grads[1], ffn_grads[2].T
    block_out = (
        (own_columns(resid, start, half) + out_own + out_other.astype(F32))
        .astype(BF16)
        .reshape(seqs, length, half)
    )
    mix_grads, tokens_grad, small = back(
        plan,
        gains,
        conv_weight,
        pn_own,
        pn_other,
        cotangent,
        mixed_in,
        prior,
        out_weight,
        in_weight,
        first,
        (resid, tokens, b_signal, c_signal, x_signal),
    )
    in_grad, out_grad = mix_grads[0:3], mix_grads[3].T
    conv_grad, norm1_grad, norm2_grad = small[0:3], small[3], small[4]
    tokens_grad = tokens_grad.reshape(seqs, length, half)
    return (
        block_out,
        tokens_grad,
        norm1_grad,
        in_grad,
        conv_grad,
        out_grad,
        norm2_grad,
        gate_grad,
        up_grad,
        down_grad,
    )


def solution(mesh):
    seq_size = mesh.shape["seq"]
    shards = mesh.shape["dp"] * seq_size
    return jax.shard_map(
        functools.partial(local, seq_size, shards),
        mesh=mesh,
        in_specs=(
            P("dp", "seq", None),
            P(),
            P(None, None, "tensor"),
            P(None, "tensor"),
            P("tensor", None),
            P(),
            P(None, "tensor"),
            P(None, "tensor"),
            P("tensor", None),
            P("dp", "seq", "tensor"),
        ),
        out_specs=(
            P("dp", "seq", "tensor"),
            P("dp", "seq", "tensor"),
            P("tensor"),
            P(None, ("dp", "seq"), "tensor"),
            P(None, "tensor"),
            P("tensor", ("dp", "seq")),
            P("tensor"),
            P(("dp", "seq"), "tensor"),
            P(("dp", "seq"), "tensor"),
            P("tensor", ("dp", "seq")),
        ),
        check_vma=False,
    )
```

```python
import functools

import jax
import jax.numpy as jnp
from jax import lax
from jax.experimental import pallas as pl
from jax.experimental.pallas import tpu as pltpu
from jax.sharding import PartitionSpec as P

EPSILON = 1e-05
MESH = pl.DeviceIdType.MESH
UNIT = 256
RING = 8
PACE = (5, 28)
LAGS = (-30, 9, 35, 65, 90)
STEPS = (5, 7, 2, 3, 2, 4, 4)
VMEM_BYTES = 67043328
F32 = jnp.float32
BF16 = jnp.bfloat16


def inverse_rms(values):
    return lax.rsqrt(jnp.mean(values * values, axis=-1, keepdims=True) + EPSILON)


def product(left, right):
    return jnp.dot(left, right, preferred_element_type=F32)


def product_t(left, right):
    return lax.dot_general(left, right, (((1,), (1,)), ((), ())), preferred_element_type=F32)


class Halving:
    def __init__(self, seq_size, shards, rows):
        self.seq_size = seq_size
        self.bits = shards.bit_length() - 1
        self.shards = shards
        self.rows = rows

    def stage_rows(self, stage):
        return self.rows << (self.bits - 1 - stage)

    def enter(self):
        self.me = lax.axis_index("dp") * self.seq_size + lax.axis_index("seq")
        self.core = lax.axis_index("tensor")

    def place(self, flat):
        return (flat // self.seq_size, flat % self.seq_size, self.core)

    def flipped(self, weight):
        return self.me + (1 - 2 * ((self.me // weight) % 2)) * weight

    def other_core(self):
        return (self.me // self.seq_size, self.me % self.seq_size, 1 - self.core)

    def along_seq(self, steps):
        seq = (self.me + steps) % self.seq_size
        return (self.me // self.seq_size, seq, self.core)

    def greet(self, steps=(), shards=True):
        barrier = pltpu.get_barrier_semaphore()
        partners = [self.other_core()]
        if shards:
            partners += [self.place(self.flipped(1 << bit)) for bit in range(self.bits)]
        partners.extend(self.along_seq(count) for count in steps)
        for partner in partners:
            pl.semaphore_signal(barrier, inc=1, device_id=partner, device_id_type=MESH)
        pl.semaphore_wait(barrier, len(partners))

    def order(self, parity):
        top = self.shards // 2
        high = (self.me // top) % 2
        low = self.me % 2
        first = (top + parity * (1 - top), high + parity * (low - high))
        third = (1 + parity * (top - 1), low + parity * (high - low))
        middle = [(2, (self.me // 2) % 2)]
        rest = [(1 << bit, (self.me // (1 << bit)) % 2) for bit in range(2, self.bits - 1)]
        return [first] + middle + [third] + rest

    def chunks(self, order, keep):
        weight, bit = order[0]
        base = (bit if keep else 1 - bit) * weight
        found = []
        for code in range(self.shards // 2):
            chunk = base
            for place in range(1, self.bits):
                if (code >> (self.bits - 1 - place)) & 1:
                    chunk = chunk + order[place][0]
            found.append(chunk)
        return found

    def offset(self, order, source, stage):
        total = 0
        for place in range(source + 1, min(stage, self.bits - 1) + 1):
            bit = order[place][1]
            if place == stage:
                bit = 1 - bit
            total = total + bit * (1 << (self.bits - 1 - place))
        return total * self.rows

    def scratch(self, units):
        half = self.stage_rows(0)
        ring = min(RING, units)
        return (
            [pltpu.VMEM((ring, half, UNIT), BF16), pltpu.VMEM((units, half, UNIT), BF16)]
            + [pltpu.VMEM((units, self.stage_rows(s), UNIT), BF16) for s in range(self.bits)]
            + [
                pltpu.SemaphoreType.DMA((self.bits, units)),
                pltpu.SemaphoreType.DMA((self.bits, units)),
            ]
        )

    def bind(self, refs):
        self.first, self.keep = refs[0], refs[1]
        self.recv = refs[2 : 2 + self.bits]
        self.send_sem, self.recv_sem = refs[2 + self.bits :]

    def copy(self, order, unit, stage):
        weight, bit = order[stage]
        if stage == 0:
            source = self.first.at[unit % RING]
        else:
            start = pl.multiple_of(self.offset(order, 0, stage), self.rows)
            source = self.keep.at[unit, pl.ds(start, self.stage_rows(stage))]
        return pltpu.make_async_remote_copy(
            src_ref=source,
            dst_ref=self.recv[stage].at[unit],
            send_sem=self.send_sem.at[stage, unit],
            recv_sem=self.recv_sem.at[stage, unit],
            device_id=self.place(self.me + (1 - 2 * bit) * weight),
            device_id_type=MESH,
        )

    def gather(self, left, order, keep):
        return jnp.concatenate([left[chunk] for chunk in self.chunks(order, keep)], axis=0)

    def begin(self, unit, parity, left, right):
        order = self.order(parity)

        @pl.when(unit >= RING)
        def _():
            self.copy(order, unit - RING, 0).wait_send()

        value = product(self.gather(left, order, False), right[...]).astype(BF16)
        self.first[unit % RING] = value

    def launch(self, unit, parity):
        self.copy(self.order(parity), unit, 0).start()

    def hold(self, unit, parity, left, right):
        order = self.order(parity)
        self.keep[unit] = product(self.gather(left, order, True), right[...]).astype(BF16)

    def collect(self, order, unit, stage, rows):
        start = pl.multiple_of(self.offset(order, 0, stage), self.rows)
        total = self.keep[unit, pl.ds(start, rows)].astype(F32)
        for source in range(min(stage, self.bits)):
            start = pl.multiple_of(self.offset(order, source, stage), self.rows)
            total = total + self.recv[source][unit, pl.ds(start, rows)].astype(F32)
        return total

    def advance(self, unit, parity, stage):
        order = self.order(parity)
        self.copy(order, unit, stage - 1).wait_recv()
        rows = self.stage_rows(stage)
        total = self.collect(order, unit, stage, rows)
        start = pl.multiple_of(self.offset(order, 0, stage), self.rows)
        self.keep[unit, pl.ds(start, rows)] = total.astype(BF16)
        self.copy(order, unit, stage).start()

    def finish(self, unit, parity):
        order = self.order(parity)
        self.copy(order, unit, self.bits - 1).wait_recv()
        total = self.collect(order, unit, self.bits, self.rows)
        for stage in range(1, self.bits):
            self.copy(order, unit, stage).wait_send()
        return total


def front_kernel(
    plan,
    gain_ref,
    tap_ref,
    token_hbm,
    cot_hbm,
    in_weight_hbm,
    out_weight_hbm,
    normed_hbm,
    cot_full_hbm,
    left_hbm,
    resid_hbm,
    b_hbm,
    c_hbm,
    x_hbm,
    mixed_hbm,
    first_hbm,
    prior_ref,
    normed_ref,
    cot_ref,
    left_ref,
    token_ref,
    edge_ref,
    in_weight_ref,
    out_weight_ref,
    b_ref,
    c_ref,
    x_ref,
    gated_ref,
    mixed_ref,
    first_ref,
    resid_ref,
    part_ref,
    part_recv,
    token_sem,
    weight_sem,
    cot_sem,
    cot_send,
    cot_recv,
    edge_send,
    edge_recv,
    swap_send,
    swap_recv,
    store_sem,
):
    total_rows, width = token_ref.shape
    half = width // 2
    step = min(256, total_rows)
    steps = total_rows // step
    edge = edge_ref.shape[0]
    plan.enter()
    seq = lax.axis_index("seq")
    last = plan.seq_size - 1

    def span(index):
        return pl.ds(pl.multiple_of(index * step, step), step)

    def load(index):
        rows = span(index)
        return pltpu.make_async_copy(token_hbm.at[rows], token_ref.at[rows], token_sem.at[index])

    own = pl.ds(pl.multiple_of(plan.core * half, half), half)
    for index in range(steps):
        load(index).start()
    weights = [
        pltpu.make_async_copy(in_weight_hbm, in_weight_ref, weight_sem.at[0]),
        pltpu.make_async_copy(out_weight_hbm, out_weight_ref, weight_sem.at[1]),
    ]
    for item in weights:
        item.start()
    cot_own = pltpu.make_async_copy(cot_hbm, cot_ref.at[:, own], cot_sem.at[0])
    cot_own.start()
    plan.greet((-1, 1), shards=False)
    cot_swap = pltpu.make_async_remote_copy(
        src_ref=cot_hbm,
        dst_ref=cot_ref.at[:, own],
        send_sem=cot_send.at[0],
        recv_sem=cot_recv.at[0],
        device_id=plan.other_core(),
        device_id_type=MESH,
    )

    def edge_copy():
        return pltpu.make_async_remote_copy(
            src_ref=token_hbm.at[pl.ds(total_rows - edge, edge)],
            dst_ref=edge_ref,
            send_sem=edge_send.at[0],
            recv_sem=edge_recv.at[0],
            device_id=plan.along_seq(1),
            device_id_type=MESH,
        )

    @pl.when(seq < last)
    def _():
        edge_copy().start()

    cot_swap.start()
    gain_one, gain_two = gain_ref[0:1], gain_ref[1:2]
    taps = [tap_ref[k : k + 1] for k in range(3)]

    def stores(index, pairs, first):
        return [
            pltpu.make_async_copy(source, target, store_sem.at[first + place, index])
            for place, (source, target) in enumerate(pairs)
        ]

    def early_stores(index):
        rows = span(index)
        return stores(
            index,
            (
                (b_ref.at[rows], b_hbm.at[rows]),
                (c_ref.at[rows], c_hbm.at[rows]),
                (x_ref.at[rows], x_hbm.at[rows]),
                (first_ref.at[:, :, rows], first_hbm.at[:, :, rows]),
            ),
            0,
        )

    def late_stores(index):
        rows = span(index)
        return stores(
            index,
            (
                (mixed_ref.at[rows], mixed_hbm.at[rows]),
                (resid_ref.at[rows], resid_hbm.at[rows]),
                (normed_ref.at[rows], normed_hbm.at[rows]),
                (cot_ref.at[rows], cot_full_hbm.at[rows]),
                (left_ref.at[:, :, :, rows], left_hbm.at[:, :, :, rows]),
            ),
            4,
        )

    def normalise(value, gain):
        return (value * inverse_rms(value) * gain).astype(BF16)

    weights[0].wait()

    def first_pass(index, carry):
        start = pl.multiple_of(index * step, step)
        rows = pl.ds(start, step)
        load(index).wait()
        normed = normalise(token_ref[rows].astype(F32), gain_one)
        b_signal = product(normed, in_weight_ref[0])
        x_signal = product(normed, in_weight_ref[2])
        b_ref[rows] = b_signal
        x_ref[rows] = x_signal
        gated_ref[pl.ds(start + 8, step)] = b_signal * x_signal
        c_ref[rows] = product(normed, in_weight_ref[1])
        first_ref[:, :, rows] = normed.T.reshape(plan.shards, plan.rows, step)
        for item in early_stores(index):
            item.start()
        return carry

    lax.fori_loop(0, steps, first_pass, 0)

    @pl.when(seq > 0)
    def _():
        edge_copy().wait_recv()

    @pl.when(seq == 0)
    def _():
        edge_ref[...] = jnp.zeros_like(edge_ref)

    normed = normalise(edge_ref[...].astype(F32), gain_one)
    gated = product(normed, in_weight_ref[0]) * product(normed, in_weight_ref[2])
    gated_ref[0:8] = gated[edge - 8 : edge]
    prior_ref[...] = gated[edge - 8 : edge]
    weights[1].wait()

    def swap(index):
        rows = span(index)
        return pltpu.make_async_remote_copy(
            src_ref=part_ref.at[rows],
            dst_ref=part_recv.at[rows],
            send_sem=swap_send.at[index],
            recv_sem=swap_recv.at[index],
            device_id=plan.other_core(),
            device_id_type=MESH,
        )

    def second_pass(index, carry):
        start = pl.multiple_of(index * step, step)
        rows = pl.ds(start, step)
        window = gated_ref[pl.ds(start, step + 8)]
        views = [window[6 + k : 6 + k + step] for k in range(3)]
        conv_out = taps[0] * views[0] + taps[1] * views[1] + taps[2] * views[2]
        mixed = (c_ref[rows] * conv_out).astype(BF16)
        mixed_ref[rows] = mixed
        part = product(mixed, out_weight_ref[...])
        part_ref[rows] = part.astype(BF16)
        swap(index).start()
        resid_ref[rows] = token_ref[rows].astype(F32) + part
        return carry

    lax.fori_loop(0, steps, second_pass, 0)
    cot_own.wait()
    cot_swap.wait_recv()

    def third_pass(index, carry):
        rows = span(index)
        swap(index).wait_recv()
        resid = resid_ref[rows] + part_recv[rows].astype(F32)
        resid_ref[rows] = resid
        normed = normalise(resid, gain_two)
        normed_ref[rows] = normed
        left_ref[0, :, :, rows] = normed.T.reshape(plan.shards, plan.rows, step)
        left_ref[1, :, :, rows] = cot_ref[rows].T.reshape(plan.shards, plan.rows, step)
        for item in late_stores(index):
            item.start()
        return carry

    lax.fori_loop(0, steps, third_pass, 0)
    for index in range(steps):
        for item in early_stores(index) + late_stores(index):
            item.wait()
        swap(index).wait_send()
    cot_swap.wait_send()

    @pl.when(seq < last)
    def _():
        edge_copy().wait_send()


def front(plan, gains, taps, tokens, cotangent, in_weight, out_weight):
    total_rows, width = tokens.shape
    half = in_weight.shape[2]
    steps = total_rows // min(256, total_rows)
    shape = jax.ShapeDtypeStruct
    dma = pltpu.SemaphoreType.DMA
    chunked = (plan.shards, plan.rows, total_rows)
    return pl.pallas_call(
        functools.partial(front_kernel, plan),
        name="front",
        out_shape=(
            shape((total_rows, width), BF16),
            shape((total_rows, width), BF16),
            shape((2,) + chunked, BF16),
            shape((total_rows, width), F32),
            shape((total_rows, half), F32),
            shape((total_rows, half), F32),
            shape((total_rows, half), F32),
            shape((total_rows, half), BF16),
            shape(chunked, BF16),
            shape((8, half), F32),
        ),
        in_specs=[whole()] * 2 + [anywhere()] * 4,
        out_specs=[anywhere()] * 9 + [whole()],
        scratch_shapes=[
            pltpu.VMEM((total_rows, width), BF16),
            pltpu.VMEM((total_rows, width), BF16),
            pltpu.VMEM((2,) + chunked, BF16),
            pltpu.VMEM((total_rows, width), BF16),
            pltpu.VMEM((16, width), BF16),
            pltpu.VMEM((3, width, half), BF16),
            pltpu.VMEM((half, width), BF16),
            pltpu.VMEM((total_rows, half), F32),
            pltpu.VMEM((total_rows, half), F32),
            pltpu.VMEM((total_rows, half), F32),
            pltpu.VMEM((total_rows + 8, half), F32),
            pltpu.VMEM((total_rows, half), BF16),
            pltpu.VMEM(chunked, BF16),
            pltpu.VMEM((total_rows, width), F32),
            pltpu.VMEM((total_rows, width), BF16),
            pltpu.VMEM((total_rows, width), BF16),
            dma((steps,)),
            dma((2,)),
            dma((1,)),
            dma((1,)),
            dma((1,)),
            dma((1,)),
            dma((1,)),
            dma((steps,)),
            dma((steps,)),
            dma((9, steps)),
        ],
        compiler_params=pltpu.CompilerParams(
            collective_id=2, has_side_effects=True, vmem_limit_bytes=VMEM_BYTES
        ),
    )(gains, taps, tokens, cotangent, in_weight, out_weight)


def whole():
    return pl.BlockSpec(memory_space=pltpu.VMEM)


def anywhere():
    return pl.BlockSpec(memory_space=pl.ANY)


def main_kernel(
    plan,
    gain_ref,
    tap_ref,
    prior_ref,
    normed_hbm,
    cot_hbm,
    left_hbm,
    gate_hbm,
    up_hbm,
    down_hbm,
    out_weight_hbm,
    in_weight_hbm,
    first_hbm,
    mixed_hbm,
    resid_hbm,
    token_hbm,
    b_hbm,
    c_hbm,
    x_hbm,
    grads_ref,
    small_ref,
    block_hbm,
    tokens_hbm,
    normed_ref,
    cot_ref,
    left_ref,
    gate_buf,
    up_buf,
    down_buf,
    right_ref,
    pn_acc,
    out_acc,
    mixed_ref,
    pn_recv,
    out_recv,
    out_weight_ref,
    x_weight_ref,
    resid_buf,
    token_buf,
    full_ref,
    block_buf,
    sums_ref,
    small_send,
    small_recv,
    weight_sem,
    load_sem,
    late_sem,
    resid_sem,
    token_sem,
    block_sem,
    store_sem,
    pn_send_sem,
    pn_recv_sem,
    out_send_sem,
    out_recv_sem,
    part_send_sem,
    part_recv_sem,
    halo_send,
    halo_recv,
    small_send_sem,
    small_recv_sem,
    free_sem,
    *refs,
):
    total_rows, width = normed_ref.shape
    blocks = gate_hbm.shape[1] // UNIT
    half = width // 2
    step = min(256, total_rows)
    steps = total_rows // step
    pieces = half // UNIT
    early = 3 * blocks
    units = early + 4 * pieces
    plan.bind(refs)
    plan.enter()
    seq = lax.axis_index("seq")
    last = plan.seq_size - 1
    own = pl.ds(pl.multiple_of(plan.core * half, half), half)
    other = pl.ds(pl.multiple_of((1 - plan.core) * half, half), half)

    def span(index):
        return pl.ds(pl.multiple_of(index * step, step), step)

    def later(index):
        return pl.ds(pl.multiple_of(index * step + 8, 8), step)

    def local_copy(source, target, sem):
        return pltpu.make_async_copy(source, target, sem)

    def core_copy(source, target, send, recv):
        return pltpu.make_async_remote_copy(
            src_ref=source,
            dst_ref=target,
            send_sem=send,
            recv_sem=recv,
            device_id=plan.other_core(),
            device_id_type=MESH,
        )

    def weights(index):
        slot = index % 2
        columns = pl.ds(pl.multiple_of(index * UNIT, UNIT), UNIT)
        tall = pl.ds(0, width)
        return [
            local_copy(gate_hbm.at[:, columns], gate_buf.at[slot, tall], weight_sem.at[0, slot]),
            local_copy(up_hbm.at[:, columns], up_buf.at[slot, tall], weight_sem.at[1, slot]),
            local_copy(down_hbm.at[columns], down_buf.at[slot], weight_sem.at[2, slot]),
        ]

    def rows_loads(index):
        rows = span(index)
        return [
            local_copy(normed_hbm.at[rows], normed_ref.at[rows], load_sem.at[0, index]),
            local_copy(cot_hbm.at[rows], cot_ref.at[rows], load_sem.at[1, index]),
        ]

    def side_loads():
        return [
            local_copy(left_hbm, left_ref, late_sem.at[0]),
            local_copy(out_weight_hbm, out_weight_ref, late_sem.at[1]),
            local_copy(in_weight_hbm.at[2], x_weight_ref, late_sem.at[2]),
        ]

    def back_loads(index):
        rows = span(index)
        low, high = pl.ds(0, half), pl.ds(half, half)
        return [
            local_copy(b_hbm.at[rows], pn_acc.at[later(index), low], load_sem.at[2, index]),
            local_copy(x_hbm.at[rows], pn_acc.at[later(index), high], load_sem.at[3, index]),
            local_copy(c_hbm.at[rows], out_acc.at[rows, other], load_sem.at[4, index]),
        ]

    def resid_load(index):
        slot = index % 2
        return local_copy(resid_hbm.at[span(index)], resid_buf.at[slot], resid_sem.at[slot])

    def token_load(index):
        slot = index % 2
        return local_copy(token_hbm.at[span(index)], token_buf.at[slot], token_sem.at[slot])

    def block_store(index):
        slot = index % 2
        return local_copy(block_buf.at[slot], block_hbm.at[span(index)], block_sem.at[slot])

    def token_store(index):
        rows = span(index)
        return local_copy(out_acc.at[rows, own], tokens_hbm.at[rows], store_sem.at[index])

    def in_weight_loads():
        tall = pl.ds(0, width)
        return [
            local_copy(
                in_weight_hbm.at[place],
                cot_ref.at[tall, pl.ds(place * half, half)],
                late_sem.at[3 + place],
            )
            for place in range(2)
        ]

    def first_load():
        return local_copy(first_hbm, left_ref.at[0], late_sem.at[5])

    def mixed_load():
        return local_copy(mixed_hbm, mixed_ref, late_sem.at[6])

    def pn_swap(index):
        rows = span(index)
        return core_copy(
            normed_ref.at[rows], pn_recv.at[rows], pn_send_sem.at[index], pn_recv_sem.at[index]
        )

    def out_swap(index):
        rows = span(index)
        return core_copy(
            mixed_ref.at[rows], out_recv.at[rows], out_send_sem.at[index], out_recv_sem.at[index]
        )

    def part_swap(index):
        rows = span(index)
        return core_copy(
            normed_ref.at[rows],
            pn_recv.at[rows],
            part_send_sem.at[index],
            part_recv_sem.at[index],
        )

    def halo():
        return pltpu.make_async_remote_copy(
            src_ref=out_acc.at[pl.ds(0, 8), other],
            dst_ref=out_acc.at[pl.ds(total_rows, 8), other],
            send_sem=halo_send.at[0],
            recv_sem=halo_recv.at[0],
            device_id=plan.along_seq(-1),
            device_id_type=MESH,
        )

    def small(bit):
        return pltpu.make_async_remote_copy(
            src_ref=small_send.at[bit],
            dst_ref=small_recv.at[bit],
            send_sem=small_send_sem.at[bit],
            recv_sem=small_recv_sem.at[bit],
            device_id=plan.place(plan.flipped(1 << bit)),
            device_id_type=MESH,
        )

    def limit(stage, clock, floor, cap):
        lag = LAGS[min(stage, len(LAGS) - 1)] + 12 * max(0, stage - len(LAGS) + 1)
        if stage:
            floor = 0
        count = (clock - lag) * PACE[0] // PACE[1]
        if all(isinstance(value, int) for value in (clock, floor, cap)):
            return max(floor, min(count, cap), 0)
        return jnp.maximum(jnp.maximum(jnp.minimum(count, cap), floor), 0)

    def tick(before, after):
        for stage in range(plan.bits + 1):
            low = limit(stage, before[0], before[1], before[2 + (stage > 0)])
            high = limit(stage, after[0], after[1], after[2 + (stage > 0)])
            if isinstance(low, int) and isinstance(high, int) and low >= high:
                continue

            def advance(unit, carry, stage=stage):
                if stage == 0:
                    plan.launch(unit, unit % 2)
                elif stage < plan.bits:
                    plan.advance(unit, unit % 2, stage)
                else:
                    grads_ref[unit] = plan.finish(unit, unit % 2)
                return carry

            lax.fori_loop(low, high, advance, 0)

    for item in weights(0):
        item.start()
    for index in range(steps):
        for item in rows_loads(index):
            item.start()
    for item in side_loads():
        item.start()
    for index in range(min(2, steps)):
        resid_load(index).start()
        token_load(index).start()
    plan.greet((-1, 1))
    pn_acc[...] = jnp.zeros_like(pn_acc)
    out_acc[...] = jnp.zeros_like(out_acc)
    sums_ref[...] = jnp.zeros_like(sums_ref)

    def block_step(index, carry):
        slot = index % 2

        @pl.when(index + 1 < blocks)
        def _():
            for item in weights(index + 1):
                item.start()

        for item in weights(index):
            item.wait()
        for place in range(steps):
            rows = pl.ds(place * step, step)

            @pl.when(index == 0)
            def _(place=place):
                for item in rows_loads(place):
                    item.wait()

            normed = normed_ref[rows]
            gate_pre = product(normed, gate_buf[slot, 0:width])
            up_pre = product(normed, up_buf[slot, 0:width])
            grad_hidden = product_t(cot_ref[rows], down_buf[slot])
            sigma = jax.nn.sigmoid(gate_pre)
            active = gate_pre * sigma
            right_ref[0, rows] = (
                grad_hidden * up_pre * (sigma * (1.0 + gate_pre * (1.0 - sigma)))
            ).astype(BF16)
            right_ref[1, rows] = (grad_hidden * active).astype(BF16)
            right_ref[2, rows] = (active * up_pre).astype(BF16)

        @pl.when(index == 0)
        def _():
            for item in side_loads():
                item.wait()

        start, stop = index * 3, index * 3 + 3
        marks = [
            (12 * index, start - RING, start, start),
            (12 * index + 4, stop - RING, start, start),
            (12 * index + 6, stop - RING, stop, start),
            (12 * index + 10, stop - RING, stop, start),
            (12 * index + 12, stop - RING, stop, stop),
        ]
        tick(marks[0], marks[1])
        for place in range(3):
            unit = index * 3 + place
            plan.begin(unit, unit % 2, left_ref.at[place // 2], right_ref.at[place])
        tick(marks[1], marks[2])
        for place in range(steps):
            rows = pl.ds(place * step, step)
            pn_acc[pl.ds(place * step + 8, step)] += product_t(
                right_ref[0, rows], gate_buf[slot, 0:width]
            ) + product_t(right_ref[1, rows], up_buf[slot, 0:width])
            out_acc[rows] += product(right_ref[2, rows], down_buf[slot])
        tick(marks[2], marks[3])
        for place in range(3):
            unit = index * 3 + place
            plan.hold(unit, unit % 2, left_ref.at[place // 2], right_ref.at[place])
        tick(marks[3], marks[4])
        return carry

    lax.fori_loop(0, blocks, block_step, 0)
    mark = (12 * blocks, early - RING, early, early)

    def paced(mark, clock, body):
        def run(index, carry):
            body(index)
            before = mark[0] + clock * index
            tick((before,) + mark[1:], (before + clock,) + mark[1:])
            return carry

        lax.fori_loop(0, steps, run, 0)
        return (mark[0] + clock * steps,) + mark[1:]

    def move(mark, clock, begun=None, held=None):
        begun = mark[2] if begun is None else begun
        held = mark[3] if held is None else held
        new = (mark[0] + clock, max(mark[1], begun - RING), begun, held)
        tick(mark, new)
        return new

    pn_acc[0:8, 0:half] = prior_ref[...]
    pn_acc[0:8, half:width] = jnp.ones((8, half), F32)

    def hand_over(index, carry):
        rows = span(index)
        normed_ref[rows] = pn_acc[later(index)].astype(BF16)
        pn_swap(index).start()
        mixed_ref[rows] = out_acc[rows, other].astype(BF16)
        out_swap(index).start()
        for item in back_loads(index):
            item.start()
        return carry

    lax.fori_loop(0, steps, hand_over, 0)
    mark = move(mark, STEPS[0])
    first_load().start()
    gain_one, gain_two = gain_ref[0:1], gain_ref[1:2]
    taps = [tap_ref[k : k + 1] for k in range(3)]

    def right_of(place, piece):
        tall = pl.ds(0, total_rows)
        if place == 0:
            return gate_buf.at[piece, tall]
        if place == 1:
            return up_buf.at[piece, tall]
        if place == 2:
            return right_ref.at[piece]
        return mixed_ref.at[:, pl.ds(piece * UNIT, UNIT)]

    def first_pass(index):
        start = pl.multiple_of(index * step, step)
        rows = span(index)
        slot = index % 2
        resid_load(index).wait()
        for item in back_loads(index):
            item.wait()
        pn_swap(index).wait_recv()
        out_swap(index).wait_recv()

        @pl.when(index >= 2)
        def _():
            block_store(index - 2).wait()

        block_buf[slot] = (
            resid_buf[slot, :, own] + out_acc[rows, own] + out_recv[rows].astype(F32)
        ).astype(BF16)
        block_store(index).start()
        resid = resid_buf[slot]
        scale = inverse_rms(resid)
        unit = resid * scale
        grad = normed_ref[rows].astype(F32) + pn_recv[rows].astype(F32)
        sums_ref[0:1] += jnp.sum(grad * unit, axis=0, keepdims=True)
        grad = grad * gain_two
        mean = jnp.mean(grad * unit, axis=-1, keepdims=True)
        grad = cot_ref[rows].astype(F32) + scale * (grad - unit * mean)
        full_ref[...] = grad
        out_acc[rows, own] = full_ref[:, own]

        @pl.when(index + 2 < steps)
        def _():
            resid_load(index + 2).start()

        rounded = grad.astype(BF16)
        left_ref[1, :, :, rows] = rounded.T.reshape(plan.shards, plan.rows, step)
        grad_mixed = product_t(rounded, out_weight_ref[...])
        window = pn_acc[pl.ds(start, step + 8), 0:half] * pn_acc[pl.ds(start, step + 8), half:width]
        views = [window[6 + k : 6 + k + step] for k in range(3)]
        conv_out = taps[0] * views[0] + taps[1] * views[1] + taps[2] * views[2]
        grad_c = (grad_mixed * conv_out).astype(BF16)
        for piece in range(pieces):
            up_buf[piece, rows] = grad_c[:, piece * UNIT : (piece + 1) * UNIT]
        grad_conv = grad_mixed * out_acc[rows, other]
        out_acc[rows, other] = grad_conv
        for k in range(3):
            sums_ref[1 + k : 2 + k, 0:half] += jnp.sum(grad_conv * views[k], axis=0, keepdims=True)

        @pl.when((index == 0) & (seq > 0))
        def _():
            halo().start()

    mark = paced(mark, STEPS[1], first_pass)
    pl.semaphore_signal(
        free_sem.at[0], inc=1, device_id=plan.other_core(), device_id_type=MESH
    )
    for index in range(steps):
        out_swap(index).wait_send()
        pn_swap(index).wait_send()
    mixed_load().start()
    for item in in_weight_loads():
        item.start()
    first_load().wait()
    places = (1, 3, 0, 2)
    work = [(place, piece) for place in places for piece in range(pieces)]

    def produce(mark, count, stop):
        room = (mark[0], max(mark[1], early + stop - RING)) + mark[2:]
        tick(mark, room)
        for hold in (False, True):
            for index in range(count, stop):
                place, piece = work[index]
                unit = early + index
                call = plan.hold if hold else plan.begin
                call(unit, unit % 2, left_ref.at[int(place == 3)], right_of(place, piece))
            if not hold:
                room = move(room, STEPS[2], early + stop)
        return move(room, STEPS[2], None, early + stop)

    mark = produce(mark, 0, pieces)
    mixed_load().wait()
    mark = produce(mark, pieces, 2 * pieces)

    @pl.when(seq < last)
    def _():
        halo().wait_recv()

    @pl.when(seq == last)
    def _():
        out_acc[pl.ds(total_rows, 8), other] = jnp.zeros((8, half), F32)

    def second_pass(index):
        start = pl.multiple_of(index * step, step)
        rows = span(index)
        window = out_acc[pl.ds(start, step + 8), other]
        grad_gated = (
            taps[0] * window[2 : 2 + step]
            + taps[1] * window[1 : 1 + step]
            + taps[2] * window[0:step]
        )
        grad_b = (grad_gated * pn_acc[later(index), half:width]).astype(BF16)
        grad_x = (grad_gated * pn_acc[later(index), 0:half]).astype(BF16)
        for piece in range(pieces):
            columns = slice(piece * UNIT, (piece + 1) * UNIT)
            gate_buf[piece, rows] = grad_b[:, columns]
            right_ref[piece, rows] = grad_x[:, columns]

    mark = paced(mark, STEPS[3], second_pass)
    mark = produce(mark, 2 * pieces, 3 * pieces)
    mark = produce(mark, 3 * pieces, 4 * pieces)
    pl.semaphore_wait(free_sem.at[0], 1)
    for item in in_weight_loads():
        item.wait()

    def third_pass(index):
        rows = span(index)
        total = None
        for place in range(3):
            for piece in range(pieces):
                columns = pl.ds(piece * UNIT, UNIT)
                if place < 2:
                    weight = cot_ref[pl.ds(0, width), pl.ds(place * half + piece * UNIT, UNIT)]
                else:
                    weight = x_weight_ref[:, columns]
                term = product_t(right_of(place, piece)[rows], weight)
                total = term if total is None else total + term
        normed_ref[rows] = total.astype(BF16)
        part_swap(index).start()

    mark = paced(mark, STEPS[4], third_pass)

    def fourth_pass(index):
        rows = span(index)
        slot = index % 2
        part_swap(index).wait_recv()
        token_load(index).wait()
        value = token_buf[slot].astype(F32)
        scale = inverse_rms(value)
        unit = value * scale
        grad = normed_ref[rows].astype(F32) + pn_recv[rows].astype(F32)
        sums_ref[4:5] += jnp.sum(grad * unit, axis=0, keepdims=True)
        grad = grad * gain_one
        mean = jnp.mean(grad * unit, axis=-1, keepdims=True)
        full_ref[...] = scale * (grad - unit * mean)
        out_acc[rows, own] += full_ref[:, own]
        token_store(index).start()

        @pl.when(index + 2 < steps)
        def _():
            token_load(index + 2).start()

    mark = paced(mark, STEPS[5], fourth_pass)
    small_send[0] = jnp.zeros_like(small_ref)
    small_send[0, 0:3] = sums_ref[1:4, 0:half]
    small_send[0, 3:4] = sums_ref[4:5, own]
    small_send[0, 4:5] = sums_ref[0:1, own]
    small(0).start()
    mark = move(mark, STEPS[6])
    for bit in range(plan.bits):
        small(bit).wait_recv()
        total = small_send[bit] + small_recv[bit]
        if bit + 1 < plan.bits:
            small_send[bit + 1] = total
            small(bit + 1).start()
            mark = move(mark, STEPS[6])
        else:
            small_ref[...] = total
    rest = 0
    while limit(plan.bits, mark[0] + 3 * rest, 0, units) < units:
        rest += 1

    def drain(index, carry):
        clock = mark[0] + 3 * index
        tick((clock,) + mark[1:], (clock + 3,) + mark[1:])
        return carry

    lax.fori_loop(0, rest, drain, 0)
    for unit in range(units - RING, units):
        plan.copy(plan.order(unit % 2), unit, 0).wait_send()
    for bit in range(plan.bits):
        small(bit).wait_send()

    @pl.when(seq > 0)
    def _():
        halo().wait_send()

    for index in range(steps):
        part_swap(index).wait_send()
        token_store(index).wait()
    for index in range(max(0, steps - 2), steps):
        block_store(index).wait()


def main(plan, smalls, operands, hidden):
    total_rows, width = operands[0].shape
    half = width // 2
    step = min(256, total_rows)
    steps = total_rows // step
    tall = max(total_rows, width)
    units = (3 * hidden + 4 * half) // UNIT
    shape = jax.ShapeDtypeStruct
    dma = pltpu.SemaphoreType.DMA
    vmem = pltpu.VMEM
    assert total_rows >= width
    return pl.pallas_call(
        functools.partial(main_kernel, plan),
        name="main",
        out_shape=(
            shape((units, plan.rows, UNIT), F32),
            shape((8, half), F32),
            shape((total_rows, half), BF16),
            shape((total_rows, half), F32),
        ),
        in_specs=[whole()] * 3 + [anywhere()] * 15,
        out_specs=[whole()] * 2 + [anywhere()] * 2,
        scratch_shapes=[
            vmem((total_rows, width), BF16),
            vmem((total_rows, width), BF16),
            vmem((2, plan.shards, plan.rows, total_rows), BF16),
            vmem((2, tall, UNIT), BF16),
            vmem((2, tall, UNIT), BF16),
            vmem((2, UNIT, width), BF16),
            vmem((3, total_rows, UNIT), BF16),
            vmem((total_rows + 8, width), F32),
            vmem((total_rows + 8, width), F32),
            vmem((total_rows, half), BF16),
            vmem((total_rows, width), BF16),
            vmem((total_rows, half), BF16),
            vmem((half, width), BF16),
            vmem((width, half), BF16),
            vmem((2, step, width), F32),
            vmem((2, step, width), BF16),
            vmem((step, width), F32),
            vmem((2, step, half), BF16),
            vmem((8, width), F32),
            vmem((plan.bits, 8, half), F32),
            vmem((plan.bits, 8, half), F32),
            dma((3, 2)),
            dma((5, steps)),
            dma((7,)),
            dma((2,)),
            dma((2,)),
            dma((2,)),
            dma((steps,)),
            dma((steps,)),
            dma((steps,)),
            dma((steps,)),
            dma((steps,)),
            dma((steps,)),
            dma((steps,)),
            dma((1,)),
            dma((1,)),
            dma((plan.bits,)),
            dma((plan.bits,)),
            pltpu.SemaphoreType.REGULAR((1,)),
        ]
        + plan.scratch(units),
        compiler_params=pltpu.CompilerParams(
            collective_id=0, has_side_effects=True, vmem_limit_bytes=VMEM_BYTES
        ),
    )(*smalls, *operands)


def local(
    seq_size,
    shards,
    tokens,
    norm1_gain,
    in_weight,
    conv_weight,
    out_weight,
    norm2_gain,
    gate_weight,
    up_weight,
    down_weight,
    out_cotangent,
):
    seqs, length, width = tokens.shape
    assert seqs == 1
    half = in_weight.shape[2]
    total_rows = seqs * length
    chunk_rows = width // shards
    plan = Halving(seq_size, shards, chunk_rows)
    gains = jnp.stack([norm1_gain, norm2_gain])
    tokens = tokens.reshape(total_rows, width)
    normed_two, cotangent, left, resid, b_signal, c_signal, x_signal, mixed_in, first, prior = front(
        plan,
        gains,
        conv_weight,
        tokens,
        out_cotangent.reshape(total_rows, half),
        in_weight,
        out_weight,
    )
    hidden = gate_weight.shape[1]
    grads, small, block_out, tokens_grad = main(
        plan,
        (gains, conv_weight, prior),
        (
            normed_two,
            cotangent,
            left,
            gate_weight,
            up_weight,
            down_weight,
            out_weight,
            in_weight,
            first,
            mixed_in,
            resid,
            tokens,
            b_signal,
            c_signal,
            x_signal,
        ),
        hidden,
    )
    blocks, pieces = hidden // UNIT, half // UNIT
    late = grads[3 * blocks :].reshape(4, pieces, chunk_rows, UNIT)
    grads = grads[: 3 * blocks].reshape(blocks, 3, chunk_rows, UNIT)
    gate_grad = grads[:, 0].transpose(1, 0, 2).reshape(chunk_rows, hidden)
    up_grad = grads[:, 1].transpose(1, 0, 2).reshape(chunk_rows, hidden)
    down_grad = grads[:, 2].transpose(0, 2, 1).reshape(hidden, chunk_rows)
    in_grad = jnp.stack([late[2], late[0], late[3]]).transpose(0, 2, 1, 3)
    in_grad = in_grad.reshape(3, chunk_rows, half)
    out_grad = late[1].transpose(0, 2, 1).reshape(half, chunk_rows)
    conv_grad, norm1_grad, norm2_grad = small[0:3], small[3], small[4]
    block_out = block_out.reshape(seqs, length, half)
    tokens_grad = tokens_grad.reshape(seqs, length, half)
    return (
        block_out,
        tokens_grad,
        norm1_grad,
        in_grad,
        conv_grad,
        out_grad,
        norm2_grad,
        gate_grad,
        up_grad,
        down_grad,
    )


def solution(mesh):
    seq_size = mesh.shape["seq"]
    shards = mesh.shape["dp"] * seq_size
    return jax.shard_map(
        functools.partial(local, seq_size, shards),
        mesh=mesh,
        in_specs=(
            P("dp", "seq", None),
            P(),
            P(None, None, "tensor"),
            P(None, "tensor"),
            P("tensor", None),
            P(),
            P(None, "tensor"),
            P(None, "tensor"),
            P("tensor", None),
            P("dp", "seq", "tensor"),
        ),
        out_specs=(
            P("dp", "seq", "tensor"),
            P("dp", "seq", "tensor"),
            P("tensor"),
            P(None, ("dp", "seq"), "tensor"),
            P(None, "tensor"),
            P("tensor", ("dp", "seq")),
            P("tensor"),
            P(("dp", "seq"), "tensor"),
            P(("dp", "seq"), "tensor"),
            P("tensor", ("dp", "seq")),
        ),
        check_vma=False,
    )
```

```python
import functools

import jax
import jax.numpy as jnp
from jax import lax
from jax.experimental import pallas as pl
from jax.experimental.pallas import tpu as pltpu
from jax.sharding import PartitionSpec as P

EPSILON = 1e-05
MESH = pl.DeviceIdType.MESH
UNIT = 256
RING = 8
PACE = (5, 25)
LATE_FIRST = 1
LAGS = (-10, 9, 29, 47, 126)
STEPS = (7, 7, 2, 1, 4, 4, 5)
VMEM_BYTES = 67043328
F32 = jnp.float32
BF16 = jnp.bfloat16


def inverse_rms(values):
    return lax.rsqrt(jnp.mean(values * values, axis=-1, keepdims=True) + EPSILON)


def product(left, right):
    return jnp.dot(left, right, preferred_element_type=F32)


def product_t(left, right):
    return lax.dot_general(left, right, (((1,), (1,)), ((), ())), preferred_element_type=F32)


class Halving:
    def __init__(self, seq_size, shards, rows):
        self.seq_size = seq_size
        self.bits = shards.bit_length() - 1
        self.shards = shards
        self.rows = rows

    def stage_rows(self, stage):
        return self.rows << (self.bits - 1 - stage)

    def enter(self):
        self.me = lax.axis_index("dp") * self.seq_size + lax.axis_index("seq")
        self.core = lax.axis_index("tensor")

    def place(self, flat):
        return (flat // self.seq_size, flat % self.seq_size, self.core)

    def flipped(self, weight):
        return self.me + (1 - 2 * ((self.me // weight) % 2)) * weight

    def other_core(self):
        return (self.me // self.seq_size, self.me % self.seq_size, 1 - self.core)

    def along_seq(self, steps):
        seq = (self.me + steps) % self.seq_size
        return (self.me // self.seq_size, seq, self.core)

    def greet(self, steps=(), shards=True):
        barrier = pltpu.get_barrier_semaphore()
        partners = [self.other_core()]
        if shards:
            partners += [self.place(self.flipped(1 << bit)) for bit in range(self.bits)]
        partners.extend(self.along_seq(count) for count in steps)
        for partner in partners:
            pl.semaphore_signal(barrier, inc=1, device_id=partner, device_id_type=MESH)
        pl.semaphore_wait(barrier, len(partners))

    def order(self, parity):
        top = self.shards // 2
        high = (self.me // top) % 2
        low = self.me % 2
        first = (top + parity * (1 - top), high + parity * (low - high))
        third = (1 + parity * (top - 1), low + parity * (high - low))
        middle = [(2, (self.me // 2) % 2)]
        rest = [(1 << bit, (self.me // (1 << bit)) % 2) for bit in range(2, self.bits - 1)]
        return [first] + middle + [third] + rest

    def chunks(self, order, keep):
        weight, bit = order[0]
        base = (bit if keep else 1 - bit) * weight
        found = []
        for code in range(self.shards // 2):
            chunk = base
            for place in range(1, self.bits):
                if (code >> (self.bits - 1 - place)) & 1:
                    chunk = chunk + order[place][0]
            found.append(chunk)
        return found

    def offset(self, order, source, stage):
        total = 0
        for place in range(source + 1, min(stage, self.bits - 1) + 1):
            bit = order[place][1]
            if place == stage:
                bit = 1 - bit
            total = total + bit * (1 << (self.bits - 1 - place))
        return total * self.rows

    def scratch(self, units):
        half = self.stage_rows(0)
        ring = min(RING, units)
        return (
            [pltpu.VMEM((ring, half, UNIT), BF16), pltpu.VMEM((units, half, UNIT), BF16)]
            + [pltpu.VMEM((units, self.stage_rows(s), UNIT), BF16) for s in range(self.bits)]
            + [
                pltpu.SemaphoreType.DMA((self.bits, units)),
                pltpu.SemaphoreType.DMA((self.bits, units)),
            ]
        )

    def bind(self, refs):
        self.first, self.keep = refs[0], refs[1]
        self.recv = refs[2 : 2 + self.bits]
        self.send_sem, self.recv_sem = refs[2 + self.bits :]

    def copy(self, order, unit, stage):
        weight, bit = order[stage]
        if stage == 0:
            source = self.first.at[unit % RING]
        else:
            start = pl.multiple_of(self.offset(order, 0, stage), self.rows)
            source = self.keep.at[unit, pl.ds(start, self.stage_rows(stage))]
        return pltpu.make_async_remote_copy(
            src_ref=source,
            dst_ref=self.recv[stage].at[unit],
            send_sem=self.send_sem.at[stage, unit],
            recv_sem=self.recv_sem.at[stage, unit],
            device_id=self.place(self.me + (1 - 2 * bit) * weight),
            device_id_type=MESH,
        )

    def gather(self, left, order, keep):
        return jnp.concatenate([left[chunk] for chunk in self.chunks(order, keep)], axis=0)

    def begin(self, unit, parity, left, right):
        order = self.order(parity)

        @pl.when(unit >= RING)
        def _():
            self.copy(order, unit - RING, 0).wait_send()

        value = product(self.gather(left, order, False), right[...]).astype(BF16)
        self.first[unit % RING] = value

    def launch(self, unit, parity):
        self.copy(self.order(parity), unit, 0).start()

    def hold(self, unit, parity, left, right):
        order = self.order(parity)
        self.keep[unit] = product(self.gather(left, order, True), right[...]).astype(BF16)

    def collect(self, order, unit, stage, rows):
        start = pl.multiple_of(self.offset(order, 0, stage), self.rows)
        total = self.keep[unit, pl.ds(start, rows)].astype(F32)
        for source in range(min(stage, self.bits)):
            start = pl.multiple_of(self.offset(order, source, stage), self.rows)
            total = total + self.recv[source][unit, pl.ds(start, rows)].astype(F32)
        return total

    def advance(self, unit, parity, stage):
        order = self.order(parity)
        self.copy(order, unit, stage - 1).wait_recv()
        rows = self.stage_rows(stage)
        total = self.collect(order, unit, stage, rows)
        start = pl.multiple_of(self.offset(order, 0, stage), self.rows)
        self.keep[unit, pl.ds(start, rows)] = total.astype(BF16)
        self.copy(order, unit, stage).start()

    def finish(self, unit, parity):
        order = self.order(parity)
        self.copy(order, unit, self.bits - 1).wait_recv()
        total = self.collect(order, unit, self.bits, self.rows)
        for stage in range(1, self.bits):
            self.copy(order, unit, stage).wait_send()
        return total


def front_kernel(
    plan,
    gain_one_ref,
    gain_two_ref,
    tap_ref,
    token_hbm,
    cot_hbm,
    in_weight_hbm,
    out_weight_hbm,
    normed_hbm,
    cot_full_hbm,
    left_hbm,
    resid_hbm,
    b_hbm,
    c_hbm,
    x_hbm,
    mixed_hbm,
    first_hbm,
    prior_ref,
    normed_ref,
    cot_ref,
    left_ref,
    token_ref,
    edge_ref,
    in_weight_ref,
    out_weight_ref,
    b_ref,
    c_ref,
    x_ref,
    gated_ref,
    mixed_ref,
    first_ref,
    resid_ref,
    part_ref,
    part_recv,
    token_sem,
    weight_sem,
    cot_sem,
    cot_send,
    cot_recv,
    edge_send,
    edge_recv,
    swap_send,
    swap_recv,
    store_sem,
):
    total_rows, width = token_ref.shape
    half = width // 2
    step = min(256, total_rows)
    steps = total_rows // step
    edge = edge_ref.shape[0]
    plan.enter()
    seq = lax.axis_index("seq")
    last = plan.seq_size - 1

    def span(index):
        return pl.ds(pl.multiple_of(index * step, step), step)

    def load(index):
        rows = span(index)
        return pltpu.make_async_copy(token_hbm.at[rows], token_ref.at[rows], token_sem.at[index])

    own = pl.ds(pl.multiple_of(plan.core * half, half), half)
    for index in range(steps):
        load(index).start()
    weights = [
        pltpu.make_async_copy(in_weight_hbm, in_weight_ref, weight_sem.at[0]),
        pltpu.make_async_copy(out_weight_hbm, out_weight_ref, weight_sem.at[1]),
    ]
    for item in weights:
        item.start()
    cot_own = pltpu.make_async_copy(cot_hbm, cot_ref.at[:, own], cot_sem.at[0])
    cot_own.start()
    plan.greet((-1, 1), shards=False)
    cot_swap = pltpu.make_async_remote_copy(
        src_ref=cot_hbm,
        dst_ref=cot_ref.at[:, own],
        send_sem=cot_send.at[0],
        recv_sem=cot_recv.at[0],
        device_id=plan.other_core(),
        device_id_type=MESH,
    )

    def edge_copy():
        return pltpu.make_async_remote_copy(
            src_ref=token_hbm.at[pl.ds(total_rows - edge, edge)],
            dst_ref=edge_ref,
            send_sem=edge_send.at[0],
            recv_sem=edge_recv.at[0],
            device_id=plan.along_seq(1),
            device_id_type=MESH,
        )

    @pl.when(seq < last)
    def _():
        edge_copy().start()

    cot_swap.start()
    gain_one, gain_two = gain_one_ref[...], gain_two_ref[...]
    taps = [tap_ref[k : k + 1] for k in range(3)]

    def stores(index, pairs, first):
        return [
            pltpu.make_async_copy(source, target, store_sem.at[first + place, index])
            for place, (source, target) in enumerate(pairs)
        ]

    def early_stores(index):
        rows = span(index)
        return stores(
            index,
            (
                (b_ref.at[rows], b_hbm.at[rows]),
                (c_ref.at[rows], c_hbm.at[rows]),
                (x_ref.at[rows], x_hbm.at[rows]),
                (first_ref.at[:, :, rows], first_hbm.at[:, :, rows]),
            ),
            0,
        )

    def late_stores(index):
        rows = span(index)
        return stores(
            index,
            (
                (mixed_ref.at[rows], mixed_hbm.at[rows]),
                (resid_ref.at[rows], resid_hbm.at[rows]),
                (normed_ref.at[rows], normed_hbm.at[rows]),
                (cot_ref.at[rows], cot_full_hbm.at[rows]),
                (left_ref.at[:, :, :, rows], left_hbm.at[:, :, :, rows]),
            ),
            4,
        )

    def normalise(value, gain):
        return (value * inverse_rms(value) * gain).astype(BF16)

    weights[0].wait()

    def first_pass(index, carry):
        start = pl.multiple_of(index * step, step)
        rows = pl.ds(start, step)
        load(index).wait()
        normed = normalise(token_ref[rows].astype(F32), gain_one)
        b_signal = product(normed, in_weight_ref[0])
        x_signal = product(normed, in_weight_ref[2])
        b_ref[rows] = b_signal
        x_ref[rows] = x_signal
        gated_ref[pl.ds(start + 8, step)] = b_signal * x_signal
        c_ref[rows] = product(normed, in_weight_ref[1])
        first_ref[:, :, rows] = normed.T.reshape(plan.shards, plan.rows, step)
        for item in early_stores(index):
            item.start()
        return carry

    lax.fori_loop(0, steps, first_pass, 0)

    @pl.when(seq > 0)
    def _():
        edge_copy().wait_recv()

    @pl.when(seq == 0)
    def _():
        edge_ref[...] = jnp.zeros_like(edge_ref)

    normed = normalise(edge_ref[...].astype(F32), gain_one)
    gated = product(normed, in_weight_ref[0]) * product(normed, in_weight_ref[2])
    gated_ref[0:8] = gated[edge - 8 : edge]
    prior_ref[...] = gated[edge - 8 : edge]
    weights[1].wait()

    def swap(index):
        rows = span(index)
        return pltpu.make_async_remote_copy(
            src_ref=part_ref.at[rows],
            dst_ref=part_recv.at[rows],
            send_sem=swap_send.at[index],
            recv_sem=swap_recv.at[index],
            device_id=plan.other_core(),
            device_id_type=MESH,
        )

    def second_pass(index, carry):
        start = pl.multiple_of(index * step, step)
        rows = pl.ds(start, step)
        window = gated_ref[pl.ds(start, step + 8)]
        views = [window[6 + k : 6 + k + step] for k in range(3)]
        conv_out = taps[0] * views[0] + taps[1] * views[1] + taps[2] * views[2]
        mixed = (c_ref[rows] * conv_out).astype(BF16)
        mixed_ref[rows] = mixed
        part = product(mixed, out_weight_ref[...])
        part_ref[rows] = part.astype(BF16)
        swap(index).start()
        resid_ref[rows] = token_ref[rows].astype(F32) + part
        return carry

    lax.fori_loop(0, steps, second_pass, 0)
    cot_own.wait()
    cot_swap.wait_recv()

    def third_pass(index, carry):
        rows = span(index)
        swap(index).wait_recv()
        resid = resid_ref[rows] + part_recv[rows].astype(F32)
        resid_ref[rows] = resid
        normed = normalise(resid, gain_two)
        normed_ref[rows] = normed
        left_ref[0, :, :, rows] = normed.T.reshape(plan.shards, plan.rows, step)
        left_ref[1, :, :, rows] = cot_ref[rows].T.reshape(plan.shards, plan.rows, step)
        for item in late_stores(index):
            item.start()
        return carry

    lax.fori_loop(0, steps, third_pass, 0)
    for index in range(steps):
        for item in early_stores(index) + late_stores(index):
            item.wait()
        swap(index).wait_send()
    cot_swap.wait_send()

    @pl.when(seq < last)
    def _():
        edge_copy().wait_send()


def front(plan, gains, taps, tokens, cotangent, in_weight, out_weight):
    total_rows, width = tokens.shape
    half = in_weight.shape[2]
    steps = total_rows // min(256, total_rows)
    shape = jax.ShapeDtypeStruct
    dma = pltpu.SemaphoreType.DMA
    chunked = (plan.shards, plan.rows, total_rows)
    return pl.pallas_call(
        functools.partial(front_kernel, plan),
        name="front",
        out_shape=(
            shape((total_rows, width), BF16),
            shape((total_rows, width), BF16),
            shape((2,) + chunked, BF16),
            shape((total_rows, width), F32),
            shape((total_rows, half), F32),
            shape((total_rows, half), F32),
            shape((total_rows, half), F32),
            shape((total_rows, half), BF16),
            shape(chunked, BF16),
            shape((8, half), F32),
        ),
        in_specs=[whole()] * 3 + [anywhere()] * 4,
        out_specs=[anywhere()] * 9 + [whole()],
        scratch_shapes=[
            pltpu.VMEM((total_rows, width), BF16),
            pltpu.VMEM((total_rows, width), BF16),
            pltpu.VMEM((2,) + chunked, BF16),
            pltpu.VMEM((total_rows, width), BF16),
            pltpu.VMEM((16, width), BF16),
            pltpu.VMEM((3, width, half), BF16),
            pltpu.VMEM((half, width), BF16),
            pltpu.VMEM((total_rows, half), F32),
            pltpu.VMEM((total_rows, half), F32),
            pltpu.VMEM((total_rows, half), F32),
            pltpu.VMEM((total_rows + 8, half), F32),
            pltpu.VMEM((total_rows, half), BF16),
            pltpu.VMEM(chunked, BF16),
            pltpu.VMEM((total_rows, width), F32),
            pltpu.VMEM((total_rows, width), BF16),
            pltpu.VMEM((total_rows, width), BF16),
            dma((steps,)),
            dma((2,)),
            dma((1,)),
            dma((1,)),
            dma((1,)),
            dma((1,)),
            dma((1,)),
            dma((steps,)),
            dma((steps,)),
            dma((9, steps)),
        ],
        compiler_params=pltpu.CompilerParams(
            collective_id=2, has_side_effects=True, vmem_limit_bytes=VMEM_BYTES
        ),
    )(*gains, taps, tokens, cotangent, in_weight, out_weight)


def whole():
    return pl.BlockSpec(memory_space=pltpu.VMEM)


def anywhere():
    return pl.BlockSpec(memory_space=pl.ANY)


def main_kernel(
    plan,
    gain_one_ref,
    gain_two_ref,
    tap_ref,
    prior_ref,
    normed_hbm,
    cot_hbm,
    left_hbm,
    gate_hbm,
    up_hbm,
    down_hbm,
    out_weight_hbm,
    in_weight_hbm,
    first_hbm,
    mixed_hbm,
    resid_hbm,
    token_hbm,
    b_hbm,
    c_hbm,
    x_hbm,
    small_ref,
    grads_hbm,
    block_hbm,
    tokens_hbm,
    grads_ref,
    normed_ref,
    cot_ref,
    left_ref,
    gate_buf,
    up_buf,
    down_buf,
    right_ref,
    pn_acc,
    out_acc,
    mixed_ref,
    pn_recv,
    out_recv,
    out_weight_ref,
    x_weight_ref,
    resid_buf,
    token_buf,
    full_ref,
    block_buf,
    sums_ref,
    small_send,
    small_recv,
    weight_sem,
    load_sem,
    late_sem,
    resid_sem,
    token_sem,
    block_sem,
    store_sem,
    pn_send_sem,
    pn_recv_sem,
    out_send_sem,
    out_recv_sem,
    part_send_sem,
    part_recv_sem,
    halo_send,
    halo_recv,
    small_send_sem,
    small_recv_sem,
    free_sem,
    grads_sem,
    *refs,
):
    total_rows, width = normed_ref.shape
    blocks = gate_hbm.shape[1] // UNIT
    half = width // 2
    step = min(256, total_rows)
    steps = total_rows // step
    pieces = half // UNIT
    early = 3 * blocks
    units = early + 4 * pieces
    plan.bind(refs)
    plan.enter()
    seq = lax.axis_index("seq")
    last = plan.seq_size - 1
    own = pl.ds(pl.multiple_of(plan.core * half, half), half)
    other = pl.ds(pl.multiple_of((1 - plan.core) * half, half), half)

    def span(index):
        return pl.ds(pl.multiple_of(index * step, step), step)

    def later(index):
        return pl.ds(pl.multiple_of(index * step + 8, 8), step)

    def local_copy(source, target, sem):
        return pltpu.make_async_copy(source, target, sem)

    def core_copy(source, target, send, recv):
        return pltpu.make_async_remote_copy(
            src_ref=source,
            dst_ref=target,
            send_sem=send,
            recv_sem=recv,
            device_id=plan.other_core(),
            device_id_type=MESH,
        )

    def weights(index):
        slot = index % 2
        columns = pl.ds(pl.multiple_of(index * UNIT, UNIT), UNIT)
        tall = pl.ds(0, width)
        return [
            local_copy(gate_hbm.at[:, columns], gate_buf.at[slot, tall], weight_sem.at[0, slot]),
            local_copy(up_hbm.at[:, columns], up_buf.at[slot, tall], weight_sem.at[1, slot]),
            local_copy(down_hbm.at[columns], down_buf.at[slot], weight_sem.at[2, slot]),
        ]

    def rows_loads(index):
        rows = span(index)
        return [
            local_copy(normed_hbm.at[rows], normed_ref.at[rows], load_sem.at[0, index]),
            local_copy(cot_hbm.at[rows], cot_ref.at[rows], load_sem.at[1, index]),
        ]

    def side_loads():
        return [
            local_copy(left_hbm, left_ref, late_sem.at[0]),
            local_copy(out_weight_hbm, out_weight_ref, late_sem.at[1]),
            local_copy(in_weight_hbm.at[2], x_weight_ref, late_sem.at[2]),
        ]

    def back_loads(index):
        rows = span(index)
        low, high = pl.ds(0, half), pl.ds(half, half)
        return [
            local_copy(b_hbm.at[rows], pn_acc.at[later(index), low], load_sem.at[2, index]),
            local_copy(x_hbm.at[rows], pn_acc.at[later(index), high], load_sem.at[3, index]),
            local_copy(c_hbm.at[rows], out_acc.at[rows, other], load_sem.at[4, index]),
        ]

    def resid_load(index):
        slot = index % 2
        return local_copy(resid_hbm.at[span(index)], resid_buf.at[slot], resid_sem.at[slot])

    def token_load(index):
        slot = index % 2
        return local_copy(token_hbm.at[span(index)], token_buf.at[slot], token_sem.at[slot])

    def block_store(index):
        slot = index % 2
        return local_copy(block_buf.at[slot], block_hbm.at[span(index)], block_sem.at[slot])

    def token_store(index):
        rows = span(index)
        return local_copy(out_acc.at[rows, own], tokens_hbm.at[rows], store_sem.at[index])

    def grads_store(unit):
        return local_copy(grads_ref.at[unit], grads_hbm.at[unit], grads_sem.at[unit])

    def in_weight_loads():
        tall = pl.ds(0, width)
        return [
            local_copy(
                in_weight_hbm.at[place],
                cot_ref.at[tall, pl.ds(place * half, half)],
                late_sem.at[3 + place],
            )
            for place in range(2)
        ]

    def first_load():
        return local_copy(first_hbm, left_ref.at[0], late_sem.at[5])

    def mixed_load():
        return local_copy(mixed_hbm, mixed_ref, late_sem.at[6])

    def pn_swap(index):
        rows = span(index)
        return core_copy(
            normed_ref.at[rows], pn_recv.at[rows], pn_send_sem.at[index], pn_recv_sem.at[index]
        )

    def out_swap(index):
        rows = span(index)
        return core_copy(
            mixed_ref.at[rows], out_recv.at[rows], out_send_sem.at[index], out_recv_sem.at[index]
        )

    def part_swap(index):
        rows = span(index)
        return core_copy(
            normed_ref.at[rows],
            pn_recv.at[rows],
            part_send_sem.at[index],
            part_recv_sem.at[index],
        )

    def halo():
        return pltpu.make_async_remote_copy(
            src_ref=out_acc.at[pl.ds(0, 8), other],
            dst_ref=out_acc.at[pl.ds(total_rows, 8), other],
            send_sem=halo_send.at[0],
            recv_sem=halo_recv.at[0],
            device_id=plan.along_seq(-1),
            device_id_type=MESH,
        )

    def small(bit):
        return pltpu.make_async_remote_copy(
            src_ref=small_send.at[bit],
            dst_ref=small_recv.at[bit],
            send_sem=small_send_sem.at[bit],
            recv_sem=small_recv_sem.at[bit],
            device_id=plan.place(plan.flipped(1 << bit)),
            device_id_type=MESH,
        )

    def limit(stage, clock, floor, cap):
        lag = LAGS[min(stage, len(LAGS) - 1)] + 12 * max(0, stage - len(LAGS) + 1)
        if stage:
            floor = 0
        count = (clock - lag) * PACE[0] // PACE[1]
        if all(isinstance(value, int) for value in (clock, floor, cap)):
            return max(floor, min(count, cap), 0)
        return jnp.maximum(jnp.maximum(jnp.minimum(count, cap), floor), 0)

    def tick(before, after):
        for stage in [0] + sorted(range(1, plan.bits + 1), reverse=bool(LATE_FIRST)):
            low = limit(stage, before[0], before[1], before[2 + (stage > 0)])
            high = limit(stage, after[0], after[1], after[2 + (stage > 0)])
            if isinstance(low, int) and isinstance(high, int) and low >= high:
                continue

            def advance(unit, carry, stage=stage):
                if stage == 0:
                    plan.launch(unit, unit % 2)
                elif stage < plan.bits:
                    plan.advance(unit, unit % 2, stage)
                else:
                    grads_ref[unit] = plan.finish(unit, unit % 2)
                    grads_store(unit).start()
                return carry

            lax.fori_loop(low, high, advance, 0)

    for item in weights(0):
        item.start()
    for index in range(steps):
        for item in rows_loads(index):
            item.start()
    for item in side_loads():
        item.start()
    for index in range(min(2, steps)):
        resid_load(index).start()
        token_load(index).start()
    pn_acc[...] = jnp.zeros_like(pn_acc)
    out_acc[...] = jnp.zeros_like(out_acc)
    sums_ref[...] = jnp.zeros_like(sums_ref)
    plan.greet((-1, 1))

    def block_step(index, carry):
        slot = index % 2

        @pl.when(index + 1 < blocks)
        def _():
            for item in weights(index + 1):
                item.start()

        for item in weights(index):
            item.wait()
        for place in range(steps):
            rows = pl.ds(place * step, step)

            @pl.when(index == 0)
            def _(place=place):
                for item in rows_loads(place):
                    item.wait()

            normed = normed_ref[rows]
            gate_pre = product(normed, gate_buf[slot, 0:width])
            up_pre = product(normed, up_buf[slot, 0:width])
            grad_hidden = product_t(cot_ref[rows], down_buf[slot])
            sigma = jax.nn.sigmoid(gate_pre)
            active = gate_pre * sigma
            right_ref[0, rows] = (
                grad_hidden * up_pre * (sigma * (1.0 + gate_pre * (1.0 - sigma)))
            ).astype(BF16)
            right_ref[1, rows] = (grad_hidden * active).astype(BF16)
            right_ref[2, rows] = (active * up_pre).astype(BF16)

        @pl.when(index == 0)
        def _():
            for item in side_loads():
                item.wait()

        start, stop = index * 3, index * 3 + 3
        marks = [
            (12 * index, start - RING, start, start),
            (12 * index + 4, stop - RING, start, start),
            (12 * index + 6, stop - RING, stop, start),
            (12 * index + 10, stop - RING, stop, start),
            (12 * index + 12, stop - RING, stop, stop),
        ]
        tick(marks[0], marks[1])
        for place in range(3):
            unit = index * 3 + place
            plan.begin(unit, unit % 2, left_ref.at[place // 2], right_ref.at[place])
        tick(marks[1], marks[2])
        for place in range(steps):
            rows = pl.ds(place * step, step)
            pn_acc[pl.ds(place * step + 8, step)] += product_t(
                right_ref[0, rows], gate_buf[slot, 0:width]
            ) + product_t(right_ref[1, rows], up_buf[slot, 0:width])
            out_acc[rows] += product(right_ref[2, rows], down_buf[slot])
        tick(marks[2], marks[3])
        for place in range(3):
            unit = index * 3 + place
            plan.hold(unit, unit % 2, left_ref.at[place // 2], right_ref.at[place])
        tick(marks[3], marks[4])
        return carry

    lax.fori_loop(0, blocks, block_step, 0)
    mark = (12 * blocks, early - RING, early, early)

    def paced(mark, clock, body):
        def run(index, carry):
            body(index)
            before = mark[0] + clock * index
            tick((before,) + mark[1:], (before + clock,) + mark[1:])
            return carry

        lax.fori_loop(0, steps, run, 0)
        return (mark[0] + clock * steps,) + mark[1:]

    def move(mark, clock, begun=None, held=None):
        begun = mark[2] if begun is None else begun
        held = mark[3] if held is None else held
        new = (mark[0] + clock, max(mark[1], begun - RING), begun, held)
        tick(mark, new)
        return new

    pn_acc[0:8, 0:half] = prior_ref[...]
    pn_acc[0:8, half:width] = jnp.ones((8, half), F32)

    def hand_over(index, carry):
        rows = span(index)
        normed_ref[rows] = pn_acc[later(index)].astype(BF16)
        pn_swap(index).start()
        mixed_ref[rows] = out_acc[rows, other].astype(BF16)
        out_swap(index).start()
        for item in back_loads(index):
            item.start()
        return carry

    lax.fori_loop(0, steps, hand_over, 0)
    mark = move(mark, STEPS[0])
    first_load().start()
    gain_one, gain_two = gain_one_ref[...], gain_two_ref[...]
    taps = [tap_ref[k : k + 1] for k in range(3)]

    def right_of(place, piece):
        tall = pl.ds(0, total_rows)
        if place == 0:
            return gate_buf.at[piece, tall]
        if place == 1:
            return up_buf.at[piece, tall]
        if place == 2:
            return right_ref.at[piece]
        return mixed_ref.at[:, pl.ds(piece * UNIT, UNIT)]

    def first_pass(index):
        start = pl.multiple_of(index * step, step)
        rows = span(index)
        slot = index % 2
        resid_load(index).wait()
        for item in back_loads(index):
            item.wait()
        pn_swap(index).wait_recv()
        out_swap(index).wait_recv()

        @pl.when(index >= 2)
        def _():
            block_store(index - 2).wait()

        block_buf[slot] = (
            resid_buf[slot, :, own] + out_acc[rows, own] + out_recv[rows].astype(F32)
        ).astype(BF16)
        block_store(index).start()
        resid = resid_buf[slot]
        scale = inverse_rms(resid)
        unit = resid * scale
        grad = normed_ref[rows].astype(F32) + pn_recv[rows].astype(F32)
        sums_ref[0:1] += jnp.sum(grad * unit, axis=0, keepdims=True)
        grad = grad * gain_two
        mean = jnp.mean(grad * unit, axis=-1, keepdims=True)
        grad = cot_ref[rows].astype(F32) + scale * (grad - unit * mean)
        full_ref[...] = grad
        out_acc[rows, own] = full_ref[:, own]

        @pl.when(index + 2 < steps)
        def _():
            resid_load(index + 2).start()

        rounded = grad.astype(BF16)
        left_ref[1, :, :, rows] = rounded.T.reshape(plan.shards, plan.rows, step)
        grad_mixed = product_t(rounded, out_weight_ref[...])
        window = pn_acc[pl.ds(start, step + 8), 0:half] * pn_acc[pl.ds(start, step + 8), half:width]
        views = [window[6 + k : 6 + k + step] for k in range(3)]
        conv_out = taps[0] * views[0] + taps[1] * views[1] + taps[2] * views[2]
        grad_c = (grad_mixed * conv_out).astype(BF16)
        for piece in range(pieces):
            up_buf[piece, rows] = grad_c[:, piece * UNIT : (piece + 1) * UNIT]
        grad_conv = grad_mixed * out_acc[rows, other]
        out_acc[rows, other] = grad_conv
        for k in range(3):
            sums_ref[1 + k : 2 + k, 0:half] += jnp.sum(grad_conv * views[k], axis=0, keepdims=True)

        @pl.when((index == 0) & (seq > 0))
        def _():
            halo().start()

    mark = paced(mark, STEPS[1], first_pass)
    pl.semaphore_signal(
        free_sem.at[0], inc=1, device_id=plan.other_core(), device_id_type=MESH
    )
    for index in range(steps):
        out_swap(index).wait_send()
        pn_swap(index).wait_send()
    mixed_load().start()
    for item in in_weight_loads():
        item.start()
    first_load().wait()
    places = (1, 3, 0, 2)
    work = [(place, piece) for place in places for piece in range(pieces)]

    def produce(mark, count, stop):
        room = (mark[0], max(mark[1], early + stop - RING)) + mark[2:]
        tick(mark, room)
        for hold in (False, True):
            for index in range(count, stop):
                place, piece = work[index]
                unit = early + index
                call = plan.hold if hold else plan.begin
                call(unit, unit % 2, left_ref.at[int(place == 3)], right_of(place, piece))
            if not hold:
                room = move(room, STEPS[2], early + stop)
        return move(room, STEPS[2], None, early + stop)

    mark = produce(mark, 0, pieces)
    mixed_load().wait()
    mark = produce(mark, pieces, 2 * pieces)

    @pl.when(seq < last)
    def _():
        halo().wait_recv()

    @pl.when(seq == last)
    def _():
        out_acc[pl.ds(total_rows, 8), other] = jnp.zeros((8, half), F32)

    def second_pass(index):
        start = pl.multiple_of(index * step, step)
        rows = span(index)
        window = out_acc[pl.ds(start, step + 8), other]
        grad_gated = (
            taps[0] * window[2 : 2 + step]
            + taps[1] * window[1 : 1 + step]
            + taps[2] * window[0:step]
        )
        grad_b = (grad_gated * pn_acc[later(index), half:width]).astype(BF16)
        grad_x = (grad_gated * pn_acc[later(index), 0:half]).astype(BF16)
        for piece in range(pieces):
            columns = slice(piece * UNIT, (piece + 1) * UNIT)
            gate_buf[piece, rows] = grad_b[:, columns]
            right_ref[piece, rows] = grad_x[:, columns]

    mark = paced(mark, STEPS[3], second_pass)
    mark = produce(mark, 2 * pieces, 3 * pieces)
    mark = produce(mark, 3 * pieces, 4 * pieces)
    pl.semaphore_wait(free_sem.at[0], 1)
    for item in in_weight_loads():
        item.wait()

    def third_pass(index):
        rows = span(index)
        total = None
        for place in range(3):
            for piece in range(pieces):
                columns = pl.ds(piece * UNIT, UNIT)
                if place < 2:
                    weight = cot_ref[pl.ds(0, width), pl.ds(place * half + piece * UNIT, UNIT)]
                else:
                    weight = x_weight_ref[:, columns]
                term = product_t(right_of(place, piece)[rows], weight)
                total = term if total is None else total + term
        normed_ref[rows] = total.astype(BF16)
        part_swap(index).start()

    mark = paced(mark, STEPS[4], third_pass)

    def fourth_pass(index):
        rows = span(index)
        slot = index % 2
        part_swap(index).wait_recv()
        token_load(index).wait()
        value = token_buf[slot].astype(F32)
        scale = inverse_rms(value)
        unit = value * scale
        grad = normed_ref[rows].astype(F32) + pn_recv[rows].astype(F32)
        sums_ref[4:5] += jnp.sum(grad * unit, axis=0, keepdims=True)
        grad = grad * gain_one
        mean = jnp.mean(grad * unit, axis=-1, keepdims=True)
        full_ref[...] = scale * (grad - unit * mean)
        out_acc[rows, own] += full_ref[:, own]
        token_store(index).start()

        @pl.when(index + 2 < steps)
        def _():
            token_load(index + 2).start()

    mark = paced(mark, STEPS[5], fourth_pass)
    small_send[0] = jnp.zeros_like(small_ref)
    small_send[0, 0:3] = sums_ref[1:4, 0:half]
    small_send[0, 3:4] = sums_ref[4:5, own]
    small_send[0, 4:5] = sums_ref[0:1, own]
    small(0).start()
    mark = move(mark, STEPS[6])
    for bit in range(plan.bits):
        small(bit).wait_recv()
        total = small_send[bit] + small_recv[bit]
        if bit + 1 < plan.bits:
            small_send[bit + 1] = total
            small(bit + 1).start()
            mark = move(mark, STEPS[6])
        else:
            small_ref[...] = total
    rest = 0
    while limit(plan.bits, mark[0] + 3 * rest, 0, units) < units:
        rest += 1

    def drain(index, carry):
        clock = mark[0] + 3 * index
        tick((clock,) + mark[1:], (clock + 3,) + mark[1:])
        return carry

    lax.fori_loop(0, rest, drain, 0)
    for unit in range(units - RING, units):
        plan.copy(plan.order(unit % 2), unit, 0).wait_send()
    for unit in range(units):
        grads_store(unit).wait()
    for bit in range(plan.bits):
        small(bit).wait_send()

    @pl.when(seq > 0)
    def _():
        halo().wait_send()

    for index in range(steps):
        part_swap(index).wait_send()
        token_store(index).wait()
    for index in range(max(0, steps - 2), steps):
        block_store(index).wait()


def main(plan, smalls, operands, hidden):
    total_rows, width = operands[0].shape
    half = width // 2
    step = min(256, total_rows)
    steps = total_rows // step
    tall = max(total_rows, width)
    units = (3 * hidden + 4 * half) // UNIT
    shape = jax.ShapeDtypeStruct
    dma = pltpu.SemaphoreType.DMA
    vmem = pltpu.VMEM
    assert total_rows >= width
    return pl.pallas_call(
        functools.partial(main_kernel, plan),
        name="main",
        out_shape=(
            shape((8, half), F32),
            shape((units, plan.rows, UNIT), F32),
            shape((total_rows, half), BF16),
            shape((total_rows, half), F32),
        ),
        in_specs=[whole()] * 4 + [anywhere()] * 15,
        out_specs=[whole()] + [anywhere()] * 3,
        scratch_shapes=[
            vmem((units, plan.rows, UNIT), F32),
            vmem((total_rows, width), BF16),
            vmem((total_rows, width), BF16),
            vmem((2, plan.shards, plan.rows, total_rows), BF16),
            vmem((2, tall, UNIT), BF16),
            vmem((2, tall, UNIT), BF16),
            vmem((2, UNIT, width), BF16),
            vmem((3, total_rows, UNIT), BF16),
            vmem((total_rows + 8, width), F32),
            vmem((total_rows + 8, width), F32),
            vmem((total_rows, half), BF16),
            vmem((total_rows, width), BF16),
            vmem((total_rows, half), BF16),
            vmem((half, width), BF16),
            vmem((width, half), BF16),
            vmem((2, step, width), F32),
            vmem((2, step, width), BF16),
            vmem((step, width), F32),
            vmem((2, step, half), BF16),
            vmem((8, width), F32),
            vmem((plan.bits, 8, half), F32),
            vmem((plan.bits, 8, half), F32),
            dma((3, 2)),
            dma((5, steps)),
            dma((7,)),
            dma((2,)),
            dma((2,)),
            dma((2,)),
            dma((steps,)),
            dma((steps,)),
            dma((steps,)),
            dma((steps,)),
            dma((steps,)),
            dma((steps,)),
            dma((steps,)),
            dma((1,)),
            dma((1,)),
            dma((plan.bits,)),
            dma((plan.bits,)),
            pltpu.SemaphoreType.REGULAR((1,)),
            dma((units,)),
        ]
        + plan.scratch(units),
        compiler_params=pltpu.CompilerParams(
            collective_id=0, has_side_effects=True, vmem_limit_bytes=VMEM_BYTES
        ),
    )(*smalls, *operands)


def finish_kernel(
    grads_in,
    block_in,
    tokens_in,
    small_ref,
    gate_hbm,
    up_hbm,
    down_hbm,
    in_hbm,
    out_hbm,
    block_hbm,
    tokens_hbm,
    conv_ref,
    one_ref,
    two_ref,
    grads_buf,
    block_buf,
    tokens_buf,
    load_sem,
    store_sem,
):
    hidden, half = gate_hbm.shape[1], out_hbm.shape[1]
    blocks, pieces = hidden // UNIT, half // UNIT
    early = 3 * blocks
    total_rows = block_buf.shape[0]
    step = min(256, total_rows)
    moves = []

    def move(source, buf, target):
        index = len(moves)
        moves.append(
            (
                pltpu.make_async_copy(source, buf, load_sem.at[index]),
                pltpu.make_async_copy(buf, target, store_sem.at[index]),
            )
        )
        moves[-1][0].start()

    for index in range(total_rows // step):
        part = pl.ds(index * step, step)
        move(tokens_in.at[part], tokens_buf.at[part], tokens_hbm.at[part])
        move(block_in.at[part], block_buf.at[part], block_hbm.at[part])
    for block in range(blocks):
        columns = pl.ds(block * UNIT, UNIT)
        for place, target in enumerate((gate_hbm, up_hbm, down_hbm)):
            unit = 3 * block + place
            move(grads_in.at[unit], grads_buf.at[unit], target.at[:, columns])
    for index, place in enumerate((1, 3, 0, 2)):
        for piece in range(pieces):
            unit = early + index * pieces + piece
            columns = pl.ds(piece * UNIT, UNIT)
            target = out_hbm if place == 3 else in_hbm.at[place]
            move(grads_in.at[unit], grads_buf.at[unit], target.at[:, columns])
    conv_ref[...] = small_ref[0:3]
    one_ref[...] = small_ref[3:4]
    two_ref[...] = small_ref[4:5]
    for load, store in moves:
        load.wait()
        store.start()
    for load, store in moves:
        store.wait()


def finish(rows, hidden, grads, small, block_out, tokens_grad):
    total_rows, half = block_out.shape
    shape = jax.ShapeDtypeStruct
    moves = 2 * (total_rows // min(256, total_rows)) + grads.shape[0]
    return pl.pallas_call(
        finish_kernel,
        name="finish",
        out_shape=(
            shape((rows, hidden), F32),
            shape((rows, hidden), F32),
            shape((rows, hidden), F32),
            shape((3, rows, half), F32),
            shape((rows, half), F32),
            shape((total_rows, half), BF16),
            shape((total_rows, half), F32),
            shape((3, half), F32),
            shape((1, half), F32),
            shape((1, half), F32),
        ),
        in_specs=[anywhere()] * 3 + [whole()],
        out_specs=[anywhere()] * 7 + [whole()] * 3,
        scratch_shapes=[
            pltpu.VMEM(grads.shape, F32),
            pltpu.VMEM((total_rows, half), BF16),
            pltpu.VMEM((total_rows, half), F32),
            pltpu.SemaphoreType.DMA((moves,)),
            pltpu.SemaphoreType.DMA((moves,)),
        ],
        compiler_params=pltpu.CompilerParams(vmem_limit_bytes=VMEM_BYTES),
    )(grads, block_out, tokens_grad, small)


def local(
    seq_size,
    shards,
    tokens,
    norm1_gain,
    in_weight,
    conv_weight,
    out_weight,
    norm2_gain,
    gate_weight,
    up_weight,
    down_weight,
    out_cotangent,
):
    seqs, length, width = tokens.shape
    assert seqs == 1
    half = in_weight.shape[2]
    total_rows = seqs * length
    chunk_rows = width // shards
    plan = Halving(seq_size, shards, chunk_rows)
    gains = (norm1_gain.reshape(1, width), norm2_gain.reshape(1, width))
    tokens = tokens.reshape(total_rows, width)
    normed_two, cotangent, left, resid, b_signal, c_signal, x_signal, mixed_in, first, prior = front(
        plan,
        gains,
        conv_weight,
        tokens,
        out_cotangent.reshape(total_rows, half),
        in_weight,
        out_weight,
    )
    hidden = gate_weight.shape[1]
    small, grads, block_out, tokens_grad = main(
        plan,
        (*gains, conv_weight, prior),
        (
            normed_two,
            cotangent,
            left,
            gate_weight,
            up_weight,
            down_weight,
            out_weight,
            in_weight,
            first,
            mixed_in,
            resid,
            tokens,
            b_signal,
            c_signal,
            x_signal,
        ),
        hidden,
    )
    (
        gate_grad,
        up_grad,
        down_grad,
        in_grad,
        out_grad,
        block_out,
        tokens_grad,
        conv_grad,
        norm1_grad,
        norm2_grad,
    ) = finish(chunk_rows, hidden, grads, small, block_out, tokens_grad)
    norm1_grad, norm2_grad = norm1_grad[0], norm2_grad[0]
    down_grad, out_grad = down_grad.T, out_grad.T
    block_out = block_out.reshape(seqs, length, half)
    tokens_grad = tokens_grad.reshape(seqs, length, half)
    return (
        block_out,
        tokens_grad,
        norm1_grad,
        in_grad,
        conv_grad,
        out_grad,
        norm2_grad,
        gate_grad,
        up_grad,
        down_grad,
    )


def solution(mesh):
    seq_size = mesh.shape["seq"]
    shards = mesh.shape["dp"] * seq_size
    return jax.shard_map(
        functools.partial(local, seq_size, shards),
        mesh=mesh,
        in_specs=(
            P("dp", "seq", None),
            P(),
            P(None, None, "tensor"),
            P(None, "tensor"),
            P("tensor", None),
            P(),
            P(None, "tensor"),
            P(None, "tensor"),
            P("tensor", None),
            P("dp", "seq", "tensor"),
        ),
        out_specs=(
            P("dp", "seq", "tensor"),
            P("dp", "seq", "tensor"),
            P("tensor"),
            P(None, ("dp", "seq"), "tensor"),
            P(None, "tensor"),
            P("tensor", ("dp", "seq")),
            P("tensor"),
            P(("dp", "seq"), "tensor"),
            P(("dp", "seq"), "tensor"),
            P("tensor", ("dp", "seq")),
        ),
        check_vma=False,
    )
```

```python
import functools

import jax
import jax.numpy as jnp
from jax import lax
from jax.experimental import pallas as pl
from jax.experimental.pallas import tpu as pltpu
from jax.sharding import PartitionSpec as P

EPSILON = 1e-05
MESH = pl.DeviceIdType.MESH
UNIT = 256
RING = 8
PACE = (5, 25)
LATE_FIRST = 1
LAGS = (-10, 9, 29, 47, 126)
STEPS = (7, 7, 2, 1, 4, 4, 5)
VMEM_BYTES = 67043328
F32 = jnp.float32
BF16 = jnp.bfloat16


def inverse_rms(values):
    return lax.rsqrt(jnp.mean(values * values, axis=-1, keepdims=True) + EPSILON)


def product(left, right):
    return jnp.dot(left, right, preferred_element_type=F32)


def product_t(left, right):
    return lax.dot_general(left, right, (((1,), (1,)), ((), ())), preferred_element_type=F32)


class Halving:
    def __init__(self, seq_size, shards, rows):
        self.seq_size = seq_size
        self.bits = shards.bit_length() - 1
        self.shards = shards
        self.rows = rows

    def stage_rows(self, stage):
        return self.rows << (self.bits - 1 - stage)

    def enter(self):
        self.me = lax.axis_index("dp") * self.seq_size + lax.axis_index("seq")
        self.core = lax.axis_index("tensor")

    def place(self, flat):
        return (flat // self.seq_size, flat % self.seq_size, self.core)

    def flipped(self, weight):
        return self.me + (1 - 2 * ((self.me // weight) % 2)) * weight

    def other_core(self):
        return (self.me // self.seq_size, self.me % self.seq_size, 1 - self.core)

    def along_seq(self, steps):
        seq = (self.me + steps) % self.seq_size
        return (self.me // self.seq_size, seq, self.core)

    def greet(self, steps):
        barrier = pltpu.get_barrier_semaphore()
        partners = [self.other_core()]
        partners += [self.place(self.flipped(1 << bit)) for bit in range(self.bits)]
        partners.extend(self.along_seq(count) for count in steps)
        for partner in partners:
            pl.semaphore_signal(barrier, inc=1, device_id=partner, device_id_type=MESH)
        pl.semaphore_wait(barrier, len(partners))

    def order(self, parity):
        top = self.shards // 2
        high = (self.me // top) % 2
        low = self.me % 2
        first = (top + parity * (1 - top), high + parity * (low - high))
        third = (1 + parity * (top - 1), low + parity * (high - low))
        middle = [(2, (self.me // 2) % 2)]
        rest = [(1 << bit, (self.me // (1 << bit)) % 2) for bit in range(2, self.bits - 1)]
        return [first] + middle + [third] + rest

    def chunks(self, order, keep):
        weight, bit = order[0]
        base = (bit if keep else 1 - bit) * weight
        found = []
        for code in range(self.shards // 2):
            chunk = base
            for place in range(1, self.bits):
                if (code >> (self.bits - 1 - place)) & 1:
                    chunk = chunk + order[place][0]
            found.append(chunk)
        return found

    def offset(self, order, source, stage):
        total = 0
        for place in range(source + 1, min(stage, self.bits - 1) + 1):
            bit = order[place][1]
            if place == stage:
                bit = 1 - bit
            total = total + bit * (1 << (self.bits - 1 - place))
        return total * self.rows

    def scratch(self, units):
        half = self.stage_rows(0)
        ring = min(RING, units)
        return (
            [pltpu.VMEM((ring, half, UNIT), BF16), pltpu.VMEM((units, half, UNIT), BF16)]
            + [pltpu.VMEM((units, self.stage_rows(s), UNIT), BF16) for s in range(self.bits)]
            + [
                pltpu.SemaphoreType.DMA((self.bits, units)),
                pltpu.SemaphoreType.DMA((self.bits, units)),
            ]
        )

    def bind(self, refs):
        self.first, self.keep = refs[0], refs[1]
        self.recv = refs[2 : 2 + self.bits]
        self.send_sem, self.recv_sem = refs[2 + self.bits :]

    def copy(self, order, unit, stage):
        weight, bit = order[stage]
        if stage == 0:
            source = self.first.at[unit % RING]
        else:
            start = pl.multiple_of(self.offset(order, 0, stage), self.rows)
            source = self.keep.at[unit, pl.ds(start, self.stage_rows(stage))]
        return pltpu.make_async_remote_copy(
            src_ref=source,
            dst_ref=self.recv[stage].at[unit],
            send_sem=self.send_sem.at[stage, unit],
            recv_sem=self.recv_sem.at[stage, unit],
            device_id=self.place(self.me + (1 - 2 * bit) * weight),
            device_id_type=MESH,
        )

    def gather(self, left, order, keep):
        return jnp.concatenate([left[chunk] for chunk in self.chunks(order, keep)], axis=0)

    def begin(self, unit, parity, left, right):
        order = self.order(parity)

        @pl.when(unit >= RING)
        def _():
            self.copy(order, unit - RING, 0).wait_send()

        value = product(self.gather(left, order, False), right[...]).astype(BF16)
        self.first[unit % RING] = value

    def launch(self, unit, parity):
        self.copy(self.order(parity), unit, 0).start()

    def hold(self, unit, parity, left, right):
        order = self.order(parity)
        self.keep[unit] = product(self.gather(left, order, True), right[...]).astype(BF16)

    def collect(self, order, unit, stage, rows):
        start = pl.multiple_of(self.offset(order, 0, stage), self.rows)
        total = self.keep[unit, pl.ds(start, rows)].astype(F32)
        for source in range(min(stage, self.bits)):
            start = pl.multiple_of(self.offset(order, source, stage), self.rows)
            total = total + self.recv[source][unit, pl.ds(start, rows)].astype(F32)
        return total

    def advance(self, unit, parity, stage):
        order = self.order(parity)
        self.copy(order, unit, stage - 1).wait_recv()
        rows = self.stage_rows(stage)
        total = self.collect(order, unit, stage, rows)
        start = pl.multiple_of(self.offset(order, 0, stage), self.rows)
        self.keep[unit, pl.ds(start, rows)] = total.astype(BF16)
        self.copy(order, unit, stage).start()

    def finish(self, unit, parity):
        order = self.order(parity)
        self.copy(order, unit, self.bits - 1).wait_recv()
        total = self.collect(order, unit, self.bits, self.rows)
        for stage in range(1, self.bits):
            self.copy(order, unit, stage).wait_send()
        return total


def whole():
    return pl.BlockSpec(memory_space=pltpu.VMEM)


def anywhere():
    return pl.BlockSpec(memory_space=pl.ANY)


def main_kernel(
    plan,
    gain_one_ref,
    gain_two_ref,
    tap_ref,
    token_hbm,
    cot_hbm,
    gate_hbm,
    up_hbm,
    down_hbm,
    out_weight_hbm,
    in_weight_hbm,
    small_ref,
    grads_hbm,
    block_hbm,
    tokens_hbm,
    resid_hbm,
    b_hbm,
    c_hbm,
    x_hbm,
    mixed_hbm,
    edge_ref,
    prior_ref,
    grads_ref,
    normed_ref,
    cot_ref,
    left_ref,
    gate_buf,
    up_buf,
    down_buf,
    right_ref,
    pn_acc,
    out_acc,
    mixed_ref,
    pn_recv,
    out_recv,
    out_weight_ref,
    x_weight_ref,
    resid_buf,
    token_buf,
    full_ref,
    block_buf,
    sums_ref,
    small_send,
    small_recv,
    weight_sem,
    load_sem,
    late_sem,
    resid_sem,
    token_sem,
    block_sem,
    store_sem,
    pn_send_sem,
    pn_recv_sem,
    out_send_sem,
    out_recv_sem,
    part_send_sem,
    part_recv_sem,
    halo_send,
    halo_recv,
    small_send_sem,
    small_recv_sem,
    free_sem,
    grads_sem,
    front_sem,
    cot_sem,
    edge_send,
    edge_recv,
    first_send_sem,
    first_recv_sem,
    *refs,
):
    total_rows, width = normed_ref.shape
    blocks = gate_hbm.shape[1] // UNIT
    half = width // 2
    step = min(256, total_rows)
    steps = total_rows // step
    pieces = half // UNIT
    early = 3 * blocks
    units = early + 4 * pieces
    plan.bind(refs)
    plan.enter()
    seq = lax.axis_index("seq")
    last = plan.seq_size - 1
    own = pl.ds(pl.multiple_of(plan.core * half, half), half)
    other = pl.ds(pl.multiple_of((1 - plan.core) * half, half), half)

    def span(index):
        return pl.ds(pl.multiple_of(index * step, step), step)

    def later(index):
        return pl.ds(pl.multiple_of(index * step + 8, 8), step)

    def local_copy(source, target, sem):
        return pltpu.make_async_copy(source, target, sem)

    def core_copy(source, target, send, recv):
        return pltpu.make_async_remote_copy(
            src_ref=source,
            dst_ref=target,
            send_sem=send,
            recv_sem=recv,
            device_id=plan.other_core(),
            device_id_type=MESH,
        )

    def weights(index):
        slot = index % 2
        columns = pl.ds(pl.multiple_of(index * UNIT, UNIT), UNIT)
        tall = pl.ds(0, width)
        return [
            local_copy(gate_hbm.at[:, columns], gate_buf.at[slot, tall], weight_sem.at[0, slot]),
            local_copy(up_hbm.at[:, columns], up_buf.at[slot, tall], weight_sem.at[1, slot]),
            local_copy(down_hbm.at[columns], down_buf.at[slot], weight_sem.at[2, slot]),
        ]

    def front_loads():
        tall = pl.ds(0, width)
        pairs = [(in_weight_hbm.at[2], x_weight_ref), (out_weight_hbm, out_weight_ref)]
        for piece in range(pieces):
            columns = pl.ds(piece * UNIT, UNIT)
            pairs.append((in_weight_hbm.at[0, :, columns], gate_buf.at[piece, tall]))
            pairs.append((in_weight_hbm.at[1, :, columns], up_buf.at[piece, tall]))
        pairs.append((cot_hbm, cot_ref.at[:, own]))
        return [
            local_copy(source, target, front_sem.at[place])
            for place, (source, target) in enumerate(pairs)
        ]

    def c_place(index):
        columns = pl.ds(pl.multiple_of((index % 2) * half, half), half)
        return resid_buf.at[index // 2, :, columns]

    def early_stores(index):
        rows = span(index)
        low, high = pl.ds(0, half), pl.ds(half, half)
        return [
            local_copy(pn_acc.at[later(index), low], b_hbm.at[rows], load_sem.at[0, index]),
            local_copy(pn_acc.at[later(index), high], x_hbm.at[rows], load_sem.at[1, index]),
            local_copy(c_place(index), c_hbm.at[rows], load_sem.at[5, index]),
        ]

    def mixed_store(index):
        rows = span(index)
        return local_copy(mixed_ref.at[rows], mixed_hbm.at[rows], load_sem.at[6, index])

    def resid_store(index):
        rows = span(index)
        return local_copy(out_acc.at[rows], resid_hbm.at[rows], load_sem.at[7, index])

    def cot_swap():
        return core_copy(cot_hbm, cot_ref.at[:, own], cot_sem.at[0], cot_sem.at[1])

    def first_swap(index):
        rows = span(index)
        return core_copy(
            normed_ref.at[rows],
            pn_recv.at[rows],
            first_send_sem.at[index],
            first_recv_sem.at[index],
        )

    def edge_copy():
        return pltpu.make_async_remote_copy(
            src_ref=token_hbm.at[pl.ds(total_rows - edge_ref.shape[0], edge_ref.shape[0])],
            dst_ref=edge_ref,
            send_sem=edge_send.at[0],
            recv_sem=edge_recv.at[0],
            device_id=plan.along_seq(1),
            device_id_type=MESH,
        )

    def back_loads(index):
        rows = span(index)
        low, high = pl.ds(0, half), pl.ds(half, half)
        return [
            local_copy(b_hbm.at[rows], pn_acc.at[later(index), low], load_sem.at[2, index]),
            local_copy(x_hbm.at[rows], pn_acc.at[later(index), high], load_sem.at[3, index]),
            local_copy(c_hbm.at[rows], out_acc.at[rows, other], load_sem.at[4, index]),
        ]

    def resid_load(index):
        slot = index % 2
        return local_copy(resid_hbm.at[span(index)], resid_buf.at[slot], resid_sem.at[slot])

    def token_load(index):
        slot = index % 2
        return local_copy(token_hbm.at[span(index)], token_buf.at[slot], token_sem.at[slot])

    def block_store(index):
        slot = index % 2
        return local_copy(block_buf.at[slot], block_hbm.at[span(index)], block_sem.at[slot])

    def token_store(index):
        rows = span(index)
        return local_copy(out_acc.at[rows, own], tokens_hbm.at[rows], store_sem.at[index])

    def grads_store(unit):
        return local_copy(grads_ref.at[unit], grads_hbm.at[unit], grads_sem.at[unit])

    def in_weight_loads():
        tall = pl.ds(0, width)
        return [
            local_copy(
                in_weight_hbm.at[place],
                cot_ref.at[tall, pl.ds(place * half, half)],
                late_sem.at[place],
            )
            for place in range(2)
        ]

    def mixed_load():
        return local_copy(mixed_hbm, mixed_ref, late_sem.at[2])

    def pn_swap(index):
        rows = span(index)
        return core_copy(
            normed_ref.at[rows], pn_recv.at[rows], pn_send_sem.at[index], pn_recv_sem.at[index]
        )

    def out_swap(index):
        rows = span(index)
        return core_copy(
            mixed_ref.at[rows], out_recv.at[rows], out_send_sem.at[index], out_recv_sem.at[index]
        )

    def part_swap(index):
        rows = span(index)
        return core_copy(
            normed_ref.at[rows],
            pn_recv.at[rows],
            part_send_sem.at[index],
            part_recv_sem.at[index],
        )

    def halo():
        return pltpu.make_async_remote_copy(
            src_ref=out_acc.at[pl.ds(0, 8), other],
            dst_ref=out_acc.at[pl.ds(total_rows, 8), other],
            send_sem=halo_send.at[0],
            recv_sem=halo_recv.at[0],
            device_id=plan.along_seq(-1),
            device_id_type=MESH,
        )

    def small(bit):
        return pltpu.make_async_remote_copy(
            src_ref=small_send.at[bit],
            dst_ref=small_recv.at[bit],
            send_sem=small_send_sem.at[bit],
            recv_sem=small_recv_sem.at[bit],
            device_id=plan.place(plan.flipped(1 << bit)),
            device_id_type=MESH,
        )

    def limit(stage, clock, floor, cap):
        lag = LAGS[min(stage, len(LAGS) - 1)] + 12 * max(0, stage - len(LAGS) + 1)
        if stage:
            floor = 0
        count = (clock - lag) * PACE[0] // PACE[1]
        if all(isinstance(value, int) for value in (clock, floor, cap)):
            return max(floor, min(count, cap), 0)
        return jnp.maximum(jnp.maximum(jnp.minimum(count, cap), floor), 0)

    def tick(before, after):
        for stage in [0] + sorted(range(1, plan.bits + 1), reverse=bool(LATE_FIRST)):
            low = limit(stage, before[0], before[1], before[2 + (stage > 0)])
            high = limit(stage, after[0], after[1], after[2 + (stage > 0)])
            if isinstance(low, int) and isinstance(high, int) and low >= high:
                continue

            def advance(unit, carry, stage=stage):
                if stage == 0:
                    plan.launch(unit, unit % 2)
                elif stage < plan.bits:
                    plan.advance(unit, unit % 2, stage)
                else:
                    grads_ref[unit] = plan.finish(unit, unit % 2)
                    grads_store(unit).start()
                return carry

            lax.fori_loop(low, high, advance, 0)

    def normalise(value, gain):
        return (value * inverse_rms(value) * gain).astype(BF16)

    def chunked(value):
        return value.T.reshape(plan.shards, plan.rows, step)

    gain_one, gain_two = gain_one_ref[...], gain_two_ref[...]
    taps = [tap_ref[k : k + 1] for k in range(3)]

    def start_tokens():
        for index in range(min(2, steps)):
            token_load(index).start()

    def next_tokens(index):
        @pl.when(index + 2 < steps)
        def _():
            token_load(index + 2).start()

    start_tokens()
    for item in front_loads():
        item.start()
    sums_ref[...] = jnp.zeros_like(sums_ref)
    plan.greet((-1, 1))

    @pl.when(seq < last)
    def _():
        edge_copy().start()

    cot_swap().start()
    for item in front_loads():
        item.wait()

    def project(index, carry):
        rows = span(index)
        slot = index % 2
        token_load(index).wait()
        value = token_buf[slot].astype(F32)
        out_acc[rows] = value
        normed = normalise(value, gain_one)
        next_tokens(index)
        for piece in range(pieces):
            columns = pl.ds(piece * UNIT, UNIT)
            pn_acc[later(index), columns] = product(normed, gate_buf[piece, 0:width])
            pn_acc[later(index), pl.ds(half + piece * UNIT, UNIT)] = product(
                normed, x_weight_ref[:, columns]
            )
            place = pl.ds(pl.multiple_of((index % 2) * half + piece * UNIT, UNIT), UNIT)
            resid_buf[index // 2, :, place] = product(normed, up_buf[piece, 0:width])
        for item in early_stores(index):
            item.start()
        return carry

    lax.fori_loop(0, steps, project, 0)
    start_tokens()

    @pl.when(seq > 0)
    def _():
        edge_copy().wait_recv()

    @pl.when(seq == 0)
    def _():
        edge_ref[...] = jnp.zeros_like(edge_ref)

    normed = normalise(edge_ref[...].astype(F32), gain_one)
    edge = edge_ref.shape[0]
    for piece in range(pieces):
        columns = pl.ds(piece * UNIT, UNIT)
        gated = product(normed, gate_buf[piece, 0:width]) * product(
            normed, x_weight_ref[:, columns]
        )
        prior_ref[:, columns] = gated[edge - 8 : edge]
    for item in weights(0):
        item.start()
    pn_acc[0:8, 0:half] = prior_ref[...]
    pn_acc[0:8, half:width] = jnp.ones((8, half), F32)

    def convolve(index, carry):
        start = pl.multiple_of(index * step, step)
        rows = span(index)
        window = pn_acc[pl.ds(start, step + 8), 0:half] * pn_acc[pl.ds(start, step + 8), half:width]
        views = [window[6 + k : 6 + k + step] for k in range(3)]
        conv_out = taps[0] * views[0] + taps[1] * views[1] + taps[2] * views[2]
        mixed = (c_place(index)[...] * conv_out).astype(BF16)
        mixed_ref[rows] = mixed
        part = product(mixed, out_weight_ref[...])
        normed_ref[rows] = part.astype(BF16)
        first_swap(index).start()
        out_acc[rows] += part
        mixed_store(index).start()
        return carry

    lax.fori_loop(0, steps, convolve, 0)
    cot_swap().wait_recv()

    def settle(index, carry):
        rows = span(index)
        first_swap(index).wait_recv()
        first_swap(index).wait_send()
        resid = out_acc[rows] + pn_recv[rows].astype(F32)
        out_acc[rows] = resid
        normed = normalise(resid, gain_two)
        normed_ref[rows] = normed
        resid_store(index).start()
        left_ref[0, :, :, rows] = chunked(normed)
        left_ref[1, :, :, rows] = chunked(cot_ref[rows])
        return carry

    lax.fori_loop(0, steps, settle, 0)
    pl.semaphore_signal(
        free_sem.at[0], inc=1, device_id=plan.other_core(), device_id_type=MESH
    )

    def block_step(index, carry):
        slot = index % 2

        @pl.when(index + 1 < blocks)
        def _():
            for item in weights(index + 1):
                item.start()

        for item in weights(index):
            item.wait()
        for place in range(steps):
            rows = pl.ds(place * step, step)
            normed = normed_ref[rows]
            gate_pre = product(normed, gate_buf[slot, 0:width])
            up_pre = product(normed, up_buf[slot, 0:width])
            grad_hidden = product_t(cot_ref[rows], down_buf[slot])
            sigma = jax.nn.sigmoid(gate_pre)
            active = gate_pre * sigma
            right_ref[0, rows] = (
                grad_hidden * up_pre * (sigma * (1.0 + gate_pre * (1.0 - sigma)))
            ).astype(BF16)
            right_ref[1, rows] = (grad_hidden * active).astype(BF16)
            right_ref[2, rows] = (active * up_pre).astype(BF16)

        start, stop = index * 3, index * 3 + 3
        marks = [
            (12 * index, start - RING, start, start),
            (12 * index + 4, stop - RING, start, start),
            (12 * index + 6, stop - RING, stop, start),
            (12 * index + 10, stop - RING, stop, start),
            (12 * index + 12, stop - RING, stop, stop),
        ]
        tick(marks[0], marks[1])
        for place in range(3):
            unit = index * 3 + place
            plan.begin(unit, unit % 2, left_ref.at[place // 2], right_ref.at[place])
        tick(marks[1], marks[2])

        @pl.when(index == 0)
        def _():
            for place in range(steps):
                for item in early_stores(place) + [mixed_store(place), resid_store(place)]:
                    item.wait()
            for place in range(min(2, steps)):
                resid_load(place).start()
            pn_acc[...] = jnp.zeros_like(pn_acc)
            out_acc[0:total_rows] = jnp.zeros((total_rows, width), F32)

        for place in range(steps):
            rows = pl.ds(place * step, step)
            pn_acc[pl.ds(place * step + 8, step)] += product_t(
                right_ref[0, rows], gate_buf[slot, 0:width]
            ) + product_t(right_ref[1, rows], up_buf[slot, 0:width])
            out_acc[rows] += product(right_ref[2, rows], down_buf[slot])
        tick(marks[2], marks[3])
        for place in range(3):
            unit = index * 3 + place
            plan.hold(unit, unit % 2, left_ref.at[place // 2], right_ref.at[place])
        tick(marks[3], marks[4])
        return carry

    lax.fori_loop(0, blocks, block_step, 0)
    mark = (12 * blocks, early - RING, early, early)

    def paced(mark, clock, body):
        def run(index, carry):
            body(index)
            before = mark[0] + clock * index
            tick((before,) + mark[1:], (before + clock,) + mark[1:])
            return carry

        lax.fori_loop(0, steps, run, 0)
        return (mark[0] + clock * steps,) + mark[1:]

    def move(mark, clock, begun=None, held=None):
        begun = mark[2] if begun is None else begun
        held = mark[3] if held is None else held
        new = (mark[0] + clock, max(mark[1], begun - RING), begun, held)
        tick(mark, new)
        return new

    pn_acc[0:8, 0:half] = prior_ref[...]
    pn_acc[0:8, half:width] = jnp.ones((8, half), F32)

    pl.semaphore_wait(free_sem.at[0], 1)

    def hand_over(index, carry):
        rows = span(index)
        normed_ref[rows] = pn_acc[later(index)].astype(BF16)
        pn_swap(index).start()
        mixed_ref[rows] = out_acc[rows, other].astype(BF16)
        out_swap(index).start()
        for item in back_loads(index):
            item.start()
        return carry

    lax.fori_loop(0, steps, hand_over, 0)
    mark = move(mark, STEPS[0])

    def right_of(place, piece):
        tall = pl.ds(0, total_rows)
        if place == 0:
            return gate_buf.at[piece, tall]
        if place == 1:
            return up_buf.at[piece, tall]
        if place == 2:
            return right_ref.at[piece]
        return mixed_ref.at[:, pl.ds(piece * UNIT, UNIT)]

    def first_pass(index):
        start = pl.multiple_of(index * step, step)
        rows = span(index)
        slot = index % 2
        resid_load(index).wait()
        for item in back_loads(index):
            item.wait()
        pn_swap(index).wait_recv()
        out_swap(index).wait_recv()

        @pl.when(index >= 2)
        def _():
            block_store(index - 2).wait()

        block_buf[slot] = (
            resid_buf[slot, :, own] + out_acc[rows, own] + out_recv[rows].astype(F32)
        ).astype(BF16)
        block_store(index).start()
        resid = resid_buf[slot]
        scale = inverse_rms(resid)
        unit = resid * scale
        grad = normed_ref[rows].astype(F32) + pn_recv[rows].astype(F32)
        sums_ref[0:1] += jnp.sum(grad * unit, axis=0, keepdims=True)
        grad = grad * gain_two
        mean = jnp.mean(grad * unit, axis=-1, keepdims=True)
        grad = cot_ref[rows].astype(F32) + scale * (grad - unit * mean)
        full_ref[...] = grad
        out_acc[rows, own] = full_ref[:, own]

        @pl.when(index + 2 < steps)
        def _():
            resid_load(index + 2).start()

        rounded = grad.astype(BF16)
        left_ref[1, :, :, rows] = chunked(rounded)
        token_load(index).wait()
        left_ref[0, :, :, rows] = chunked(normalise(token_buf[slot].astype(F32), gain_one))
        next_tokens(index)
        grad_mixed = product_t(rounded, out_weight_ref[...])
        window = pn_acc[pl.ds(start, step + 8), 0:half] * pn_acc[pl.ds(start, step + 8), half:width]
        views = [window[6 + k : 6 + k + step] for k in range(3)]
        conv_out = taps[0] * views[0] + taps[1] * views[1] + taps[2] * views[2]
        grad_c = (grad_mixed * conv_out).astype(BF16)
        for piece in range(pieces):
            up_buf[piece, rows] = grad_c[:, piece * UNIT : (piece + 1) * UNIT]
        grad_conv = grad_mixed * out_acc[rows, other]
        out_acc[rows, other] = grad_conv
        for k in range(3):
            sums_ref[1 + k : 2 + k, 0:half] += jnp.sum(grad_conv * views[k], axis=0, keepdims=True)

        @pl.when((index == 0) & (seq > 0))
        def _():
            halo().start()

    mark = paced(mark, STEPS[1], first_pass)
    start_tokens()
    pl.semaphore_signal(
        free_sem.at[1], inc=1, device_id=plan.other_core(), device_id_type=MESH
    )
    for index in range(steps):
        out_swap(index).wait_send()
        pn_swap(index).wait_send()
    mixed_load().start()
    for item in in_weight_loads():
        item.start()
    places = (1, 3, 0, 2)
    work = [(place, piece) for place in places for piece in range(pieces)]

    def produce(mark, count, stop):
        room = (mark[0], max(mark[1], early + stop - RING)) + mark[2:]
        tick(mark, room)
        for hold in (False, True):
            for index in range(count, stop):
                place, piece = work[index]
                unit = early + index
                call = plan.hold if hold else plan.begin
                call(unit, unit % 2, left_ref.at[int(place == 3)], right_of(place, piece))
            if not hold:
                room = move(room, STEPS[2], early + stop)
        return move(room, STEPS[2], None, early + stop)

    mark = produce(mark, 0, pieces)
    mixed_load().wait()
    mark = produce(mark, pieces, 2 * pieces)

    @pl.when(seq < last)
    def _():
        halo().wait_recv()

    @pl.when(seq == last)
    def _():
        out_acc[pl.ds(total_rows, 8), other] = jnp.zeros((8, half), F32)

    def second_pass(index):
        start = pl.multiple_of(index * step, step)
        rows = span(index)
        window = out_acc[pl.ds(start, step + 8), other]
        grad_gated = (
            taps[0] * window[2 : 2 + step]
            + taps[1] * window[1 : 1 + step]
            + taps[2] * window[0:step]
        )
        grad_b = (grad_gated * pn_acc[later(index), half:width]).astype(BF16)
        grad_x = (grad_gated * pn_acc[later(index), 0:half]).astype(BF16)
        for piece in range(pieces):
            columns = slice(piece * UNIT, (piece + 1) * UNIT)
            gate_buf[piece, rows] = grad_b[:, columns]
            right_ref[piece, rows] = grad_x[:, columns]

    mark = paced(mark, STEPS[3], second_pass)
    mark = produce(mark, 2 * pieces, 3 * pieces)
    mark = produce(mark, 3 * pieces, 4 * pieces)
    pl.semaphore_wait(free_sem.at[1], 1)
    for item in in_weight_loads():
        item.wait()

    def third_pass(index):
        rows = span(index)
        total = None
        for place in range(3):
            for piece in range(pieces):
                columns = pl.ds(piece * UNIT, UNIT)
                if place < 2:
                    weight = cot_ref[pl.ds(0, width), pl.ds(place * half + piece * UNIT, UNIT)]
                else:
                    weight = x_weight_ref[:, columns]
                term = product_t(right_of(place, piece)[rows], weight)
                total = term if total is None else total + term
        normed_ref[rows] = total.astype(BF16)
        part_swap(index).start()

    mark = paced(mark, STEPS[4], third_pass)

    def fourth_pass(index):
        rows = span(index)
        slot = index % 2
        part_swap(index).wait_recv()
        token_load(index).wait()
        value = token_buf[slot].astype(F32)
        scale = inverse_rms(value)
        unit = value * scale
        grad = normed_ref[rows].astype(F32) + pn_recv[rows].astype(F32)
        sums_ref[4:5] += jnp.sum(grad * unit, axis=0, keepdims=True)
        grad = grad * gain_one
        mean = jnp.mean(grad * unit, axis=-1, keepdims=True)
        full_ref[...] = scale * (grad - unit * mean)
        out_acc[rows, own] += full_ref[:, own]
        token_store(index).start()
        next_tokens(index)

    mark = paced(mark, STEPS[5], fourth_pass)
    small_send[0] = jnp.zeros_like(small_ref)
    small_send[0, 0:3] = sums_ref[1:4, 0:half]
    small_send[0, 3:4] = sums_ref[4:5, own]
    small_send[0, 4:5] = sums_ref[0:1, own]
    small(0).start()
    mark = move(mark, STEPS[6])
    for bit in range(plan.bits):
        small(bit).wait_recv()
        total = small_send[bit] + small_recv[bit]
        if bit + 1 < plan.bits:
            small_send[bit + 1] = total
            small(bit + 1).start()
            mark = move(mark, STEPS[6])
        else:
            small_ref[...] = total
    rest = 0
    while limit(plan.bits, mark[0] + 3 * rest, 0, units) < units:
        rest += 1

    def drain(index, carry):
        clock = mark[0] + 3 * index
        tick((clock,) + mark[1:], (clock + 3,) + mark[1:])
        return carry

    lax.fori_loop(0, rest, drain, 0)
    for unit in range(units - RING, units):
        plan.copy(plan.order(unit % 2), unit, 0).wait_send()
    for unit in range(units):
        grads_store(unit).wait()
    for bit in range(plan.bits):
        small(bit).wait_send()

    cot_swap().wait_send()

    @pl.when(seq < last)
    def _():
        edge_copy().wait_send()

    @pl.when(seq > 0)
    def _():
        halo().wait_send()

    for index in range(steps):
        part_swap(index).wait_send()
        token_store(index).wait()
    for index in range(max(0, steps - 2), steps):
        block_store(index).wait()


def main(plan, smalls, operands, hidden):
    total_rows, width = operands[0].shape
    half = width // 2
    assert half == 2 * UNIT
    step = min(256, total_rows)
    steps = total_rows // step
    tall = max(total_rows, width)
    units = (3 * hidden + 4 * half) // UNIT
    shape = jax.ShapeDtypeStruct
    dma = pltpu.SemaphoreType.DMA
    vmem = pltpu.VMEM
    assert total_rows >= width and steps <= 4
    return pl.pallas_call(
        functools.partial(main_kernel, plan),
        name="main",
        out_shape=(
            shape((8, half), F32),
            shape((units, plan.rows, UNIT), F32),
            shape((total_rows, half), BF16),
            shape((total_rows, half), F32),
            shape((total_rows, width), F32),
            shape((total_rows, half), F32),
            shape((total_rows, half), F32),
            shape((total_rows, half), F32),
            shape((total_rows, half), BF16),
        ),
        in_specs=[whole()] * 3 + [anywhere()] * 7,
        out_specs=[whole()] + [anywhere()] * 8,
        scratch_shapes=[
            vmem((16, width), BF16),
            vmem((8, half), F32),
            vmem((units, plan.rows, UNIT), F32),
            vmem((total_rows, width), BF16),
            vmem((total_rows, width), BF16),
            vmem((2, plan.shards, plan.rows, total_rows), BF16),
            vmem((2, tall, UNIT), BF16),
            vmem((2, tall, UNIT), BF16),
            vmem((2, UNIT, width), BF16),
            vmem((3, total_rows, UNIT), BF16),
            vmem((total_rows + 8, width), F32),
            vmem((total_rows + 8, width), F32),
            vmem((total_rows, half), BF16),
            vmem((total_rows, width), BF16),
            vmem((total_rows, half), BF16),
            vmem((half, width), BF16),
            vmem((width, half), BF16),
            vmem((2, step, width), F32),
            vmem((2, step, width), BF16),
            vmem((step, width), F32),
            vmem((2, step, half), BF16),
            vmem((8, width), F32),
            vmem((plan.bits, 8, half), F32),
            vmem((plan.bits, 8, half), F32),
            dma((3, 2)),
            dma((8, steps)),
            dma((3,)),
            dma((2,)),
            dma((2,)),
            dma((2,)),
            dma((steps,)),
            dma((steps,)),
            dma((steps,)),
            dma((steps,)),
            dma((steps,)),
            dma((steps,)),
            dma((steps,)),
            dma((1,)),
            dma((1,)),
            dma((plan.bits,)),
            dma((plan.bits,)),
            pltpu.SemaphoreType.REGULAR((2,)),
            dma((units,)),
            dma((7,)),
            dma((2,)),
            dma((1,)),
            dma((1,)),
            dma((steps,)),
            dma((steps,)),
        ]
        + plan.scratch(units),
        compiler_params=pltpu.CompilerParams(
            collective_id=0, has_side_effects=True, vmem_limit_bytes=VMEM_BYTES
        ),
    )(*smalls, *operands)


def finish_kernel(
    grads_in,
    block_in,
    tokens_in,
    small_ref,
    gate_hbm,
    up_hbm,
    down_hbm,
    in_hbm,
    out_hbm,
    block_hbm,
    tokens_hbm,
    conv_ref,
    one_ref,
    two_ref,
    grads_buf,
    block_buf,
    tokens_buf,
    load_sem,
    store_sem,
):
    hidden, half = gate_hbm.shape[1], out_hbm.shape[1]
    blocks, pieces = hidden // UNIT, half // UNIT
    early = 3 * blocks
    total_rows = block_buf.shape[0]
    step = min(256, total_rows)
    moves = []

    def move(source, buf, target):
        index = len(moves)
        moves.append(
            (
                pltpu.make_async_copy(source, buf, load_sem.at[index]),
                pltpu.make_async_copy(buf, target, store_sem.at[index]),
            )
        )
        moves[-1][0].start()

    for index in range(total_rows // step):
        part = pl.ds(index * step, step)
        move(tokens_in.at[part], tokens_buf.at[part], tokens_hbm.at[part])
        move(block_in.at[part], block_buf.at[part], block_hbm.at[part])
    for block in range(blocks):
        columns = pl.ds(block * UNIT, UNIT)
        for place, target in enumerate((gate_hbm, up_hbm, down_hbm)):
            unit = 3 * block + place
            move(grads_in.at[unit], grads_buf.at[unit], target.at[:, columns])
    for index, place in enumerate((1, 3, 0, 2)):
        for piece in range(pieces):
            unit = early + index * pieces + piece
            columns = pl.ds(piece * UNIT, UNIT)
            target = out_hbm if place == 3 else in_hbm.at[place]
            move(grads_in.at[unit], grads_buf.at[unit], target.at[:, columns])
    conv_ref[...] = small_ref[0:3]
    one_ref[...] = small_ref[3:4]
    two_ref[...] = small_ref[4:5]
    for load, store in moves:
        load.wait()
        store.start()
    for load, store in moves:
        store.wait()


def finish(rows, hidden, grads, small, block_out, tokens_grad):
    total_rows, half = block_out.shape
    shape = jax.ShapeDtypeStruct
    moves = 2 * (total_rows // min(256, total_rows)) + grads.shape[0]
    return pl.pallas_call(
        finish_kernel,
        name="finish",
        out_shape=(
            shape((rows, hidden), F32),
            shape((rows, hidden), F32),
            shape((rows, hidden), F32),
            shape((3, rows, half), F32),
            shape((rows, half), F32),
            shape((total_rows, half), BF16),
            shape((total_rows, half), F32),
            shape((3, half), F32),
            shape((1, half), F32),
            shape((1, half), F32),
        ),
        in_specs=[anywhere()] * 3 + [whole()],
        out_specs=[anywhere()] * 7 + [whole()] * 3,
        scratch_shapes=[
            pltpu.VMEM(grads.shape, F32),
            pltpu.VMEM((total_rows, half), BF16),
            pltpu.VMEM((total_rows, half), F32),
            pltpu.SemaphoreType.DMA((moves,)),
            pltpu.SemaphoreType.DMA((moves,)),
        ],
        compiler_params=pltpu.CompilerParams(vmem_limit_bytes=VMEM_BYTES),
    )(grads, block_out, tokens_grad, small)


def local(
    seq_size,
    shards,
    tokens,
    norm1_gain,
    in_weight,
    conv_weight,
    out_weight,
    norm2_gain,
    gate_weight,
    up_weight,
    down_weight,
    out_cotangent,
):
    seqs, length, width = tokens.shape
    assert seqs == 1
    half = in_weight.shape[2]
    total_rows = seqs * length
    chunk_rows = width // shards
    plan = Halving(seq_size, shards, chunk_rows)
    gains = (norm1_gain.reshape(1, width), norm2_gain.reshape(1, width))
    tokens = tokens.reshape(total_rows, width)
    hidden = gate_weight.shape[1]
    small, grads, block_out, tokens_grad = main(
        plan,
        (*gains, conv_weight),
        (
            tokens,
            out_cotangent.reshape(total_rows, half),
            gate_weight,
            up_weight,
            down_weight,
            out_weight,
            in_weight,
        ),
        hidden,
    )[:4]
    (
        gate_grad,
        up_grad,
        down_grad,
        in_grad,
        out_grad,
        block_out,
        tokens_grad,
        conv_grad,
        norm1_grad,
        norm2_grad,
    ) = finish(chunk_rows, hidden, grads, small, block_out, tokens_grad)
    norm1_grad, norm2_grad = norm1_grad[0], norm2_grad[0]
    down_grad, out_grad = down_grad.T, out_grad.T
    block_out = block_out.reshape(seqs, length, half)
    tokens_grad = tokens_grad.reshape(seqs, length, half)
    return (
        block_out,
        tokens_grad,
        norm1_grad,
        in_grad,
        conv_grad,
        out_grad,
        norm2_grad,
        gate_grad,
        up_grad,
        down_grad,
    )


def solution(mesh):
    seq_size = mesh.shape["seq"]
    shards = mesh.shape["dp"] * seq_size
    return jax.shard_map(
        functools.partial(local, seq_size, shards),
        mesh=mesh,
        in_specs=(
            P("dp", "seq", None),
            P(),
            P(None, None, "tensor"),
            P(None, "tensor"),
            P("tensor", None),
            P(),
            P(None, "tensor"),
            P(None, "tensor"),
            P("tensor", None),
            P("dp", "seq", "tensor"),
        ),
        out_specs=(
            P("dp", "seq", "tensor"),
            P("dp", "seq", "tensor"),
            P("tensor"),
            P(None, ("dp", "seq"), "tensor"),
            P(None, "tensor"),
            P("tensor", ("dp", "seq")),
            P("tensor"),
            P(("dp", "seq"), "tensor"),
            P(("dp", "seq"), "tensor"),
            P("tensor", ("dp", "seq")),
        ),
        check_vma=False,
    )
```

```python
import functools

import jax
import jax.numpy as jnp
from jax import lax
from jax.experimental import pallas as pl
from jax.experimental.pallas import tpu as pltpu
from jax.sharding import PartitionSpec as P

EPSILON = 1e-05
MESH = pl.DeviceIdType.MESH
UNIT = 256
RING = 8
PACE = (5, 24)
LATE_FIRST = 1
LAGS = (-6, 6, 26, 45, 155)
STEPS = (7, 6, 2, 1, 1, 4, 7)
VMEM_BYTES = 67043328
F32 = jnp.float32
BF16 = jnp.bfloat16


def inverse_rms(values):
    return lax.rsqrt(jnp.mean(values * values, axis=-1, keepdims=True) + EPSILON)


def product(left, right):
    return jnp.dot(left, right, preferred_element_type=F32)


def product_t(left, right):
    return lax.dot_general(left, right, (((1,), (1,)), ((), ())), preferred_element_type=F32)


class Halving:
    def __init__(self, seq_size, shards, rows):
        self.seq_size = seq_size
        self.bits = shards.bit_length() - 1
        self.shards = shards
        self.rows = rows

    def stage_rows(self, stage):
        return self.rows << (self.bits - 1 - stage)

    def enter(self):
        self.me = lax.axis_index("dp") * self.seq_size + lax.axis_index("seq")
        self.core = lax.axis_index("tensor")

    def place(self, flat):
        return (flat // self.seq_size, flat % self.seq_size, self.core)

    def flipped(self, weight):
        return self.me + (1 - 2 * ((self.me // weight) % 2)) * weight

    def other_core(self):
        return (self.me // self.seq_size, self.me % self.seq_size, 1 - self.core)

    def along_seq(self, steps):
        seq = (self.me + steps) % self.seq_size
        return (self.me // self.seq_size, seq, self.core)

    def greet(self, steps):
        barrier = pltpu.get_barrier_semaphore()
        partners = [self.other_core()]
        partners += [self.place(self.flipped(1 << bit)) for bit in range(self.bits)]
        partners.extend(self.along_seq(count) for count in steps)
        for partner in partners:
            pl.semaphore_signal(barrier, inc=1, device_id=partner, device_id_type=MESH)
        pl.semaphore_wait(barrier, len(partners))

    def order(self, parity):
        top = self.shards // 2
        high = (self.me // top) % 2
        low = self.me % 2
        first = (top + parity * (1 - top), high + parity * (low - high))
        third = (1 + parity * (top - 1), low + parity * (high - low))
        middle = [(2, (self.me // 2) % 2)]
        rest = [(1 << bit, (self.me // (1 << bit)) % 2) for bit in range(2, self.bits - 1)]
        return [first] + middle + [third] + rest

    def chunks(self, order, keep):
        weight, bit = order[0]
        base = (bit if keep else 1 - bit) * weight
        found = []
        for code in range(self.shards // 2):
            chunk = base
            for place in range(1, self.bits):
                if (code >> (self.bits - 1 - place)) & 1:
                    chunk = chunk + order[place][0]
            found.append(chunk)
        return found

    def offset(self, order, source, stage):
        total = 0
        for place in range(source + 1, min(stage, self.bits - 1) + 1):
            bit = order[place][1]
            if place == stage:
                bit = 1 - bit
            total = total + bit * (1 << (self.bits - 1 - place))
        return total * self.rows

    def scratch(self, units):
        half = self.stage_rows(0)
        ring = min(RING, units)
        return (
            [pltpu.VMEM((ring, half, UNIT), BF16), pltpu.VMEM((units, half, UNIT), BF16)]
            + [pltpu.VMEM((units, self.stage_rows(s), UNIT), BF16) for s in range(self.bits)]
            + [
                pltpu.SemaphoreType.DMA((2, self.bits, units)),
                pltpu.SemaphoreType.DMA((2, self.bits, units)),
            ]
        )

    def bind(self, refs):
        self.first, self.keep = refs[0], refs[1]
        self.recv = refs[2 : 2 + self.bits]
        self.send_sem, self.recv_sem = refs[2 + self.bits :]

    def copies(self, order, unit, stage):
        weight, bit = order[stage]
        rows = self.stage_rows(stage)
        starts = [0]
        if stage + 1 < self.bits:
            rows = rows // 2
            following = order[stage + 1][1]
            starts = [(1 - following) * rows, following * rows]
        base = 0 if stage == 0 else self.offset(order, 0, stage)
        found = []
        for part, start in enumerate(starts):
            source = pl.ds(pl.multiple_of(base + start, self.rows), rows)
            target = pl.ds(pl.multiple_of(start, self.rows), rows)
            buffer = self.keep.at[unit] if stage else self.first.at[unit % RING]
            found.append(
                pltpu.make_async_remote_copy(
                    src_ref=buffer.at[source],
                    dst_ref=self.recv[stage].at[unit, target],
                    send_sem=self.send_sem.at[part, stage, unit],
                    recv_sem=self.recv_sem.at[part, stage, unit],
                    device_id=self.place(self.me + (1 - 2 * bit) * weight),
                    device_id_type=MESH,
                )
            )
        return found

    def arrived(self, order, unit, stage):
        self.copies(order, unit, stage - 1)[0].wait_recv()
        if stage >= 2:
            self.copies(order, unit, stage - 2)[1].wait_recv()

    def sent(self, order, unit, stage):
        for item in self.copies(order, unit, stage):
            item.wait_send()

    def gather(self, left, order, keep):
        return jnp.concatenate([left[chunk] for chunk in self.chunks(order, keep)], axis=0)

    def begin(self, unit, parity, left, right):
        order = self.order(parity)

        @pl.when(unit >= RING)
        def _():
            self.sent(order, unit - RING, 0)

        value = product(self.gather(left, order, False), right[...]).astype(BF16)
        self.first[unit % RING] = value

    def launch(self, unit, parity):
        for item in self.copies(self.order(parity), unit, 0):
            item.start()

    def hold(self, unit, parity, left, right):
        order = self.order(parity)
        self.keep[unit] = product(self.gather(left, order, True), right[...]).astype(BF16)

    def collect(self, order, unit, stage, rows):
        start = pl.multiple_of(self.offset(order, 0, stage), self.rows)
        total = self.keep[unit, pl.ds(start, rows)].astype(F32)
        for source in range(min(stage, self.bits)):
            start = pl.multiple_of(self.offset(order, source, stage), self.rows)
            total = total + self.recv[source][unit, pl.ds(start, rows)].astype(F32)
        return total

    def advance(self, unit, parity, stage):
        order = self.order(parity)
        self.arrived(order, unit, stage)
        rows = self.stage_rows(stage)
        total = self.collect(order, unit, stage, rows)
        start = pl.multiple_of(self.offset(order, 0, stage), self.rows)
        self.keep[unit, pl.ds(start, rows)] = total.astype(BF16)
        for item in self.copies(order, unit, stage):
            item.start()

    def finish(self, unit, parity):
        order = self.order(parity)
        self.arrived(order, unit, self.bits)
        total = self.collect(order, unit, self.bits, self.rows)
        for stage in range(1, self.bits):
            self.sent(order, unit, stage)
        return total


def whole():
    return pl.BlockSpec(memory_space=pltpu.VMEM)


def anywhere():
    return pl.BlockSpec(memory_space=pl.ANY)


def main_kernel(
    plan,
    gain_one_ref,
    gain_two_ref,
    tap_ref,
    token_hbm,
    cot_hbm,
    gate_hbm,
    up_hbm,
    down_hbm,
    out_weight_hbm,
    in_weight_hbm,
    small_ref,
    grads_hbm,
    block_hbm,
    tokens_hbm,
    resid_hbm,
    b_hbm,
    c_hbm,
    x_hbm,
    mixed_hbm,
    edge_ref,
    prior_ref,
    grads_ref,
    normed_ref,
    cot_ref,
    left_ref,
    gate_buf,
    up_buf,
    down_buf,
    right_ref,
    pn_acc,
    out_acc,
    mixed_ref,
    pn_recv,
    out_recv,
    out_weight_ref,
    x_weight_ref,
    resid_buf,
    token_buf,
    full_ref,
    block_buf,
    sums_ref,
    small_send,
    small_recv,
    weight_sem,
    load_sem,
    late_sem,
    resid_sem,
    token_sem,
    block_sem,
    store_sem,
    pn_send_sem,
    pn_recv_sem,
    out_send_sem,
    out_recv_sem,
    part_send_sem,
    part_recv_sem,
    halo_send,
    halo_recv,
    small_send_sem,
    small_recv_sem,
    free_sem,
    grads_sem,
    front_sem,
    cot_sem,
    edge_send,
    edge_recv,
    first_send_sem,
    first_recv_sem,
    *refs,
):
    total_rows, width = normed_ref.shape
    blocks = gate_hbm.shape[1] // UNIT
    half = width // 2
    step = min(256, total_rows)
    steps = total_rows // step
    pieces = half // UNIT
    early = 3 * blocks
    units = early + 4 * pieces
    plan.bind(refs)
    plan.enter()
    seq = lax.axis_index("seq")
    last = plan.seq_size - 1
    own = pl.ds(pl.multiple_of(plan.core * half, half), half)
    other = pl.ds(pl.multiple_of((1 - plan.core) * half, half), half)

    def span(index):
        return pl.ds(pl.multiple_of(index * step, step), step)

    def later(index):
        return pl.ds(pl.multiple_of(index * step + 8, 8), step)

    def local_copy(source, target, sem):
        return pltpu.make_async_copy(source, target, sem)

    def core_copy(source, target, send, recv):
        return pltpu.make_async_remote_copy(
            src_ref=source,
            dst_ref=target,
            send_sem=send,
            recv_sem=recv,
            device_id=plan.other_core(),
            device_id_type=MESH,
        )

    def weights(index):
        slot = index % 2
        columns = pl.ds(pl.multiple_of(index * UNIT, UNIT), UNIT)
        tall = pl.ds(0, width)
        return [
            local_copy(gate_hbm.at[:, columns], gate_buf.at[slot, tall], weight_sem.at[0, slot]),
            local_copy(up_hbm.at[:, columns], up_buf.at[slot, tall], weight_sem.at[1, slot]),
            local_copy(down_hbm.at[columns], down_buf.at[slot], weight_sem.at[2, slot]),
        ]

    def front_loads(late):
        tall = pl.ds(0, width)
        if late:
            pairs = [(out_weight_hbm, out_weight_ref), (cot_hbm, cot_ref.at[:, own])]
            return [
                local_copy(source, target, front_sem.at[place])
                for place, (source, target) in enumerate(pairs)
            ]
        pairs = [(in_weight_hbm.at[2], x_weight_ref)]
        for piece in range(pieces):
            columns = pl.ds(piece * UNIT, UNIT)
            pairs.append((in_weight_hbm.at[0, :, columns], gate_buf.at[piece, tall]))
            pairs.append((in_weight_hbm.at[1, :, columns], up_buf.at[piece, tall]))
        return [
            local_copy(source, target, front_sem.at[2 + place])
            for place, (source, target) in enumerate(pairs)
        ]

    def c_place(index):
        columns = pl.ds(pl.multiple_of((index % 2) * half, half), half)
        return resid_buf.at[index // 2, :, columns]

    def early_stores(index):
        rows = span(index)
        low, high = pl.ds(0, half), pl.ds(half, half)
        return [
            local_copy(pn_acc.at[later(index), low], b_hbm.at[rows], load_sem.at[0, index]),
            local_copy(pn_acc.at[later(index), high], x_hbm.at[rows], load_sem.at[1, index]),
            local_copy(c_place(index), c_hbm.at[rows], load_sem.at[5, index]),
        ]

    def mixed_store(index):
        rows = span(index)
        return local_copy(mixed_ref.at[rows], mixed_hbm.at[rows], load_sem.at[6, index])

    def resid_store(index):
        rows = span(index)
        return local_copy(out_acc.at[rows], resid_hbm.at[rows], load_sem.at[7, index])

    def cot_swap():
        return core_copy(cot_hbm, cot_ref.at[:, own], cot_sem.at[0], cot_sem.at[1])

    def first_swap(index):
        rows = span(index)
        return core_copy(
            normed_ref.at[rows],
            pn_recv.at[rows],
            first_send_sem.at[index],
            first_recv_sem.at[index],
        )

    def edge_copy():
        return pltpu.make_async_remote_copy(
            src_ref=token_hbm.at[pl.ds(total_rows - edge_ref.shape[0], edge_ref.shape[0])],
            dst_ref=edge_ref,
            send_sem=edge_send.at[0],
            recv_sem=edge_recv.at[0],
            device_id=plan.along_seq(1),
            device_id_type=MESH,
        )

    def back_loads(index):
        rows = span(index)
        low, high = pl.ds(0, half), pl.ds(half, half)
        return [
            local_copy(b_hbm.at[rows], pn_acc.at[later(index), low], load_sem.at[2, index]),
            local_copy(x_hbm.at[rows], pn_acc.at[later(index), high], load_sem.at[3, index]),
            local_copy(c_hbm.at[rows], out_acc.at[rows, other], load_sem.at[4, index]),
        ]

    def resid_load(index):
        slot = index % 2
        return local_copy(resid_hbm.at[span(index)], resid_buf.at[slot], resid_sem.at[slot])

    def token_load(index):
        slot = index % 2
        return local_copy(token_hbm.at[span(index)], token_buf.at[slot], token_sem.at[slot])

    def block_store(index):
        slot = index % 2
        return local_copy(block_buf.at[slot], block_hbm.at[span(index)], block_sem.at[slot])

    def token_store(index):
        rows = span(index)
        return local_copy(out_acc.at[rows, own], tokens_hbm.at[rows], store_sem.at[index])

    def grads_store(unit):
        return local_copy(grads_ref.at[unit], grads_hbm.at[unit], grads_sem.at[unit])

    def in_weight_loads():
        tall = pl.ds(0, width)
        return [
            local_copy(
                in_weight_hbm.at[place],
                cot_ref.at[tall, pl.ds(place * half, half)],
                late_sem.at[place],
            )
            for place in range(2)
        ]

    def mixed_load():
        return local_copy(mixed_hbm, mixed_ref, late_sem.at[2])

    def pn_swap(index):
        rows = span(index)
        return core_copy(
            normed_ref.at[rows], pn_recv.at[rows], pn_send_sem.at[index], pn_recv_sem.at[index]
        )

    def out_swap(index):
        rows = span(index)
        return core_copy(
            mixed_ref.at[rows], out_recv.at[rows], out_send_sem.at[index], out_recv_sem.at[index]
        )

    def part_swap(index):
        rows = span(index)
        return core_copy(
            normed_ref.at[rows],
            pn_recv.at[rows],
            part_send_sem.at[index],
            part_recv_sem.at[index],
        )

    def halo():
        return pltpu.make_async_remote_copy(
            src_ref=out_acc.at[pl.ds(0, 8), other],
            dst_ref=out_acc.at[pl.ds(total_rows, 8), other],
            send_sem=halo_send.at[0],
            recv_sem=halo_recv.at[0],
            device_id=plan.along_seq(-1),
            device_id_type=MESH,
        )

    def small(bit):
        return pltpu.make_async_remote_copy(
            src_ref=small_send.at[bit],
            dst_ref=small_recv.at[bit],
            send_sem=small_send_sem.at[bit],
            recv_sem=small_recv_sem.at[bit],
            device_id=plan.place(plan.flipped(1 << bit)),
            device_id_type=MESH,
        )

    def limit(stage, clock, floor, cap):
        lag = LAGS[min(stage, len(LAGS) - 1)] + 12 * max(0, stage - len(LAGS) + 1)
        if stage:
            floor = 0
        count = (clock - lag) * PACE[0] // PACE[1]
        if all(isinstance(value, int) for value in (clock, floor, cap)):
            return max(floor, min(count, cap), 0)
        return jnp.maximum(jnp.maximum(jnp.minimum(count, cap), floor), 0)

    def tick(before, after):
        for stage in [0] + sorted(range(1, plan.bits + 1), reverse=bool(LATE_FIRST)):
            low = limit(stage, before[0], before[1], before[2 + (stage > 0)])
            high = limit(stage, after[0], after[1], after[2 + (stage > 0)])
            if isinstance(low, int) and isinstance(high, int) and low >= high:
                continue

            def advance(unit, carry, stage=stage):
                if stage == 0:
                    plan.launch(unit, unit % 2)
                elif stage < plan.bits:
                    plan.advance(unit, unit % 2, stage)
                else:
                    grads_ref[unit] = plan.finish(unit, unit % 2)
                    grads_store(unit).start()
                return carry

            lax.fori_loop(low, high, advance, 0)

    def normalise(value, gain):
        return (value * inverse_rms(value) * gain).astype(BF16)

    def chunked(value):
        return value.T.reshape(plan.shards, plan.rows, step)

    gain_one, gain_two = gain_one_ref[...], gain_two_ref[...]
    taps = [tap_ref[k : k + 1] for k in range(3)]

    def start_tokens():
        for index in range(min(2, steps)):
            token_load(index).start()

    def next_tokens(index):
        @pl.when(index + 2 < steps)
        def _():
            token_load(index + 2).start()

    start_tokens()
    for item in front_loads(False) + front_loads(True):
        item.start()
    sums_ref[...] = jnp.zeros_like(sums_ref)
    plan.greet((-1, 1))

    @pl.when(seq < last)
    def _():
        edge_copy().start()

    cot_swap().start()
    for item in front_loads(False):
        item.wait()

    def project(index, carry):
        rows = span(index)
        slot = index % 2
        token_load(index).wait()
        value = token_buf[slot].astype(F32)
        out_acc[rows] = value
        normed = normalise(value, gain_one)
        next_tokens(index)
        for piece in range(pieces):
            columns = pl.ds(piece * UNIT, UNIT)
            pn_acc[later(index), columns] = product(normed, gate_buf[piece, 0:width])
            pn_acc[later(index), pl.ds(half + piece * UNIT, UNIT)] = product(
                normed, x_weight_ref[:, columns]
            )
            place = pl.ds(pl.multiple_of((index % 2) * half + piece * UNIT, UNIT), UNIT)
            resid_buf[index // 2, :, place] = product(normed, up_buf[piece, 0:width])
        for item in early_stores(index):
            item.start()
        return carry

    lax.fori_loop(0, steps, project, 0)
    start_tokens()

    @pl.when(seq > 0)
    def _():
        edge_copy().wait_recv()

    @pl.when(seq == 0)
    def _():
        edge_ref[...] = jnp.zeros_like(edge_ref)

    normed = normalise(edge_ref[...].astype(F32), gain_one)
    edge = edge_ref.shape[0]
    for piece in range(pieces):
        columns = pl.ds(piece * UNIT, UNIT)
        gated = product(normed, gate_buf[piece, 0:width]) * product(
            normed, x_weight_ref[:, columns]
        )
        prior_ref[:, columns] = gated[edge - 8 : edge]
    for item in weights(0):
        item.start()
    pn_acc[0:8, 0:half] = prior_ref[...]
    pn_acc[0:8, half:width] = jnp.ones((8, half), F32)

    def convolve(index, carry):
        start = pl.multiple_of(index * step, step)
        rows = span(index)
        window = pn_acc[pl.ds(start, step + 8), 0:half] * pn_acc[pl.ds(start, step + 8), half:width]
        views = [window[6 + k : 6 + k + step] for k in range(3)]
        conv_out = taps[0] * views[0] + taps[1] * views[1] + taps[2] * views[2]
        mixed = (c_place(index)[...] * conv_out).astype(BF16)
        mixed_ref[rows] = mixed
        part = product(mixed, out_weight_ref[...])
        normed_ref[rows] = part.astype(BF16)
        first_swap(index).start()
        out_acc[rows] += part
        mixed_store(index).start()
        left_ref[1, :, :, rows] = chunked(cot_ref[rows])
        return carry

    for item in front_loads(True):
        item.wait()
    cot_swap().wait_recv()
    lax.fori_loop(0, steps, convolve, 0)

    def settle(index, carry):
        rows = span(index)
        first_swap(index).wait_recv()
        first_swap(index).wait_send()
        resid = out_acc[rows] + pn_recv[rows].astype(F32)
        out_acc[rows] = resid
        normed = normalise(resid, gain_two)
        normed_ref[rows] = normed
        resid_store(index).start()
        left_ref[0, :, :, rows] = chunked(normed)
        return carry

    lax.fori_loop(0, steps, settle, 0)
    pl.semaphore_signal(
        free_sem.at[0], inc=1, device_id=plan.other_core(), device_id_type=MESH
    )

    def block_step(index, carry):
        slot = index % 2

        @pl.when(index + 1 < blocks)
        def _():
            for item in weights(index + 1):
                item.start()

        for item in weights(index):
            item.wait()
        for place in range(steps):
            rows = pl.ds(place * step, step)
            normed = normed_ref[rows]
            gate_pre = product(normed, gate_buf[slot, 0:width])
            up_pre = product(normed, up_buf[slot, 0:width])
            grad_hidden = product_t(cot_ref[rows], down_buf[slot])
            sigma = jax.nn.sigmoid(gate_pre)
            active = gate_pre * sigma
            right_ref[0, rows] = (
                grad_hidden * up_pre * (sigma * (1.0 + gate_pre * (1.0 - sigma)))
            ).astype(BF16)
            right_ref[1, rows] = (grad_hidden * active).astype(BF16)
            right_ref[2, rows] = (active * up_pre).astype(BF16)

        start, stop = index * 3, index * 3 + 3
        marks = [
            (12 * index, start - RING, start, start),
            (12 * index + 4, stop - RING, start, start),
            (12 * index + 6, stop - RING, stop, start),
            (12 * index + 10, stop - RING, stop, start),
            (12 * index + 12, stop - RING, stop, stop),
        ]
        tick(marks[0], marks[1])
        for place in range(3):
            unit = index * 3 + place
            plan.begin(unit, unit % 2, left_ref.at[place // 2], right_ref.at[place])
        tick(marks[1], marks[2])

        @pl.when(index == 0)
        def _():
            for place in range(steps):
                for item in early_stores(place) + [mixed_store(place), resid_store(place)]:
                    item.wait()
            for place in range(min(2, steps)):
                resid_load(place).start()
            pn_acc[...] = jnp.zeros_like(pn_acc)
            out_acc[0:total_rows] = jnp.zeros((total_rows, width), F32)

        for place in range(steps):
            rows = pl.ds(place * step, step)
            pn_acc[pl.ds(place * step + 8, step)] += product_t(
                right_ref[0, rows], gate_buf[slot, 0:width]
            ) + product_t(right_ref[1, rows], up_buf[slot, 0:width])
            out_acc[rows] += product(right_ref[2, rows], down_buf[slot])
        tick(marks[2], marks[3])
        for place in range(3):
            unit = index * 3 + place
            plan.hold(unit, unit % 2, left_ref.at[place // 2], right_ref.at[place])
        tick(marks[3], marks[4])
        return carry

    lax.fori_loop(0, blocks, block_step, 0)
    mark = (12 * blocks, early - RING, early, early)

    def paced(mark, clock, body):
        def run(index, carry):
            body(index)
            before = mark[0] + clock * index
            tick((before,) + mark[1:], (before + clock,) + mark[1:])
            return carry

        lax.fori_loop(0, steps, run, 0)
        return (mark[0] + clock * steps,) + mark[1:]

    def move(mark, clock, begun=None, held=None):
        begun = mark[2] if begun is None else begun
        held = mark[3] if held is None else held
        new = (mark[0] + clock, max(mark[1], begun - RING), begun, held)
        tick(mark, new)
        return new

    pn_acc[0:8, 0:half] = prior_ref[...]
    pn_acc[0:8, half:width] = jnp.ones((8, half), F32)

    pl.semaphore_wait(free_sem.at[0], 1)

    def hand_over(index, carry):
        rows = span(index)
        normed_ref[rows] = pn_acc[later(index)].astype(BF16)
        pn_swap(index).start()
        mixed_ref[rows] = out_acc[rows, other].astype(BF16)
        out_swap(index).start()
        for item in back_loads(index):
            item.start()
        return carry

    lax.fori_loop(0, steps, hand_over, 0)
    mark = move(mark, STEPS[0])

    def right_of(place, piece):
        tall = pl.ds(0, total_rows)
        if place == 0:
            return gate_buf.at[piece, tall]
        if place == 1:
            return up_buf.at[piece, tall]
        if place == 2:
            return right_ref.at[piece]
        return mixed_ref.at[:, pl.ds(piece * UNIT, UNIT)]

    def first_pass(index):
        start = pl.multiple_of(index * step, step)
        rows = span(index)
        slot = index % 2
        resid_load(index).wait()
        for item in back_loads(index):
            item.wait()
        pn_swap(index).wait_recv()
        out_swap(index).wait_recv()

        @pl.when(index >= 2)
        def _():
            block_store(index - 2).wait()

        block_buf[slot] = (
            resid_buf[slot, :, own] + out_acc[rows, own] + out_recv[rows].astype(F32)
        ).astype(BF16)
        block_store(index).start()
        resid = resid_buf[slot]
        scale = inverse_rms(resid)
        unit = resid * scale
        grad = normed_ref[rows].astype(F32) + pn_recv[rows].astype(F32)
        sums_ref[0:1] += jnp.sum(grad * unit, axis=0, keepdims=True)
        grad = grad * gain_two
        mean = jnp.mean(grad * unit, axis=-1, keepdims=True)
        grad = cot_ref[rows].astype(F32) + scale * (grad - unit * mean)
        full_ref[...] = grad
        out_acc[rows, own] = full_ref[:, own]

        @pl.when(index + 2 < steps)
        def _():
            resid_load(index + 2).start()

        rounded = grad.astype(BF16)
        left_ref[1, :, :, rows] = chunked(rounded)
        token_load(index).wait()
        left_ref[0, :, :, rows] = chunked(normalise(token_buf[slot].astype(F32), gain_one))
        next_tokens(index)
        grad_mixed = product_t(rounded, out_weight_ref[...])
        window = pn_acc[pl.ds(start, step + 8), 0:half] * pn_acc[pl.ds(start, step + 8), half:width]
        views = [window[6 + k : 6 + k + step] for k in range(3)]
        conv_out = taps[0] * views[0] + taps[1] * views[1] + taps[2] * views[2]
        grad_c = (grad_mixed * conv_out).astype(BF16)
        for piece in range(pieces):
            up_buf[piece, rows] = grad_c[:, piece * UNIT : (piece + 1) * UNIT]
        grad_conv = grad_mixed * out_acc[rows, other]
        out_acc[rows, other] = grad_conv
        for k in range(3):
            sums_ref[1 + k : 2 + k, 0:half] += jnp.sum(grad_conv * views[k], axis=0, keepdims=True)

        @pl.when((index == 0) & (seq > 0))
        def _():
            halo().start()

    mark = paced(mark, STEPS[1], first_pass)
    start_tokens()
    pl.semaphore_signal(
        free_sem.at[1], inc=1, device_id=plan.other_core(), device_id_type=MESH
    )
    for index in range(steps):
        out_swap(index).wait_send()
        pn_swap(index).wait_send()
    mixed_load().start()
    for item in in_weight_loads():
        item.start()
    places = (1, 3, 0, 2)
    work = [(place, piece) for place in places for piece in range(pieces)]

    def produce(mark, count, stop):
        room = (mark[0], max(mark[1], early + stop - RING)) + mark[2:]
        tick(mark, room)
        for hold in (False, True):
            for index in range(count, stop):
                place, piece = work[index]
                unit = early + index
                call = plan.hold if hold else plan.begin
                call(unit, unit % 2, left_ref.at[int(place == 3)], right_of(place, piece))
            if not hold:
                room = move(room, STEPS[2], early + stop)
        return move(room, STEPS[2], None, early + stop)

    mark = produce(mark, 0, pieces)
    mixed_load().wait()
    mark = produce(mark, pieces, 2 * pieces)

    @pl.when(seq < last)
    def _():
        halo().wait_recv()

    @pl.when(seq == last)
    def _():
        out_acc[pl.ds(total_rows, 8), other] = jnp.zeros((8, half), F32)

    def second_pass(index):
        start = pl.multiple_of(index * step, step)
        rows = span(index)
        window = out_acc[pl.ds(start, step + 8), other]
        grad_gated = (
            taps[0] * window[2 : 2 + step]
            + taps[1] * window[1 : 1 + step]
            + taps[2] * window[0:step]
        )
        grad_b = (grad_gated * pn_acc[later(index), half:width]).astype(BF16)
        grad_x = (grad_gated * pn_acc[later(index), 0:half]).astype(BF16)
        for piece in range(pieces):
            columns = slice(piece * UNIT, (piece + 1) * UNIT)
            gate_buf[piece, rows] = grad_b[:, columns]
            right_ref[piece, rows] = grad_x[:, columns]

    mark = paced(mark, STEPS[3], second_pass)
    mark = produce(mark, 2 * pieces, 3 * pieces)
    mark = produce(mark, 3 * pieces, 4 * pieces)
    pl.semaphore_wait(free_sem.at[1], 1)
    for item in in_weight_loads():
        item.wait()

    def third_pass(index):
        rows = span(index)
        total = None
        for place in range(3):
            for piece in range(pieces):
                columns = pl.ds(piece * UNIT, UNIT)
                if place < 2:
                    weight = cot_ref[pl.ds(0, width), pl.ds(place * half + piece * UNIT, UNIT)]
                else:
                    weight = x_weight_ref[:, columns]
                term = product_t(right_of(place, piece)[rows], weight)
                total = term if total is None else total + term
        normed_ref[rows] = total.astype(BF16)
        part_swap(index).start()

    mark = paced(mark, STEPS[4], third_pass)

    def fourth_pass(index):
        rows = span(index)
        slot = index % 2
        part_swap(index).wait_recv()
        token_load(index).wait()
        value = token_buf[slot].astype(F32)
        scale = inverse_rms(value)
        unit = value * scale
        grad = normed_ref[rows].astype(F32) + pn_recv[rows].astype(F32)
        sums_ref[4:5] += jnp.sum(grad * unit, axis=0, keepdims=True)
        grad = grad * gain_one
        mean = jnp.mean(grad * unit, axis=-1, keepdims=True)
        full_ref[...] = scale * (grad - unit * mean)
        out_acc[rows, own] += full_ref[:, own]
        token_store(index).start()
        next_tokens(index)

    mark = paced(mark, STEPS[5], fourth_pass)
    small_send[0] = jnp.zeros_like(small_ref)
    small_send[0, 0:3] = sums_ref[1:4, 0:half]
    small_send[0, 3:4] = sums_ref[4:5, own]
    small_send[0, 4:5] = sums_ref[0:1, own]
    small(0).start()
    mark = move(mark, STEPS[6])
    for bit in range(plan.bits):
        small(bit).wait_recv()
        total = small_send[bit] + small_recv[bit]
        if bit + 1 < plan.bits:
            small_send[bit + 1] = total
            small(bit + 1).start()
            mark = move(mark, STEPS[6])
        else:
            small_ref[...] = total
    rest = 0
    while limit(plan.bits, mark[0] + 3 * rest, 0, units) < units:
        rest += 1

    def drain(index, carry):
        clock = mark[0] + 3 * index
        tick((clock,) + mark[1:], (clock + 3,) + mark[1:])
        return carry

    lax.fori_loop(0, rest, drain, 0)
    for unit in range(units - RING, units):
        plan.sent(plan.order(unit % 2), unit, 0)
    for unit in range(units):
        grads_store(unit).wait()
    for bit in range(plan.bits):
        small(bit).wait_send()

    cot_swap().wait_send()

    @pl.when(seq < last)
    def _():
        edge_copy().wait_send()

    @pl.when(seq > 0)
    def _():
        halo().wait_send()

    for index in range(steps):
        part_swap(index).wait_send()
        token_store(index).wait()
    for index in range(max(0, steps - 2), steps):
        block_store(index).wait()


def main(plan, smalls, operands, hidden):
    total_rows, width = operands[0].shape
    half = width // 2
    assert half == 2 * UNIT
    step = min(256, total_rows)
    steps = total_rows // step
    tall = max(total_rows, width)
    units = (3 * hidden + 4 * half) // UNIT
    shape = jax.ShapeDtypeStruct
    dma = pltpu.SemaphoreType.DMA
    vmem = pltpu.VMEM
    assert total_rows >= width and steps <= 4
    return pl.pallas_call(
        functools.partial(main_kernel, plan),
        name="main",
        out_shape=(
            shape((8, half), F32),
            shape((units, plan.rows, UNIT), F32),
            shape((total_rows, half), BF16),
            shape((total_rows, half), F32),
            shape((total_rows, width), F32),
            shape((total_rows, half), F32),
            shape((total_rows, half), F32),
            shape((total_rows, half), F32),
            shape((total_rows, half), BF16),
        ),
        in_specs=[whole()] * 3 + [anywhere()] * 7,
        out_specs=[whole()] + [anywhere()] * 8,
        scratch_shapes=[
            vmem((16, width), BF16),
            vmem((8, half), F32),
            vmem((units, plan.rows, UNIT), F32),
            vmem((total_rows, width), BF16),
            vmem((total_rows, width), BF16),
            vmem((2, plan.shards, plan.rows, total_rows), BF16),
            vmem((2, tall, UNIT), BF16),
            vmem((2, tall, UNIT), BF16),
            vmem((2, UNIT, width), BF16),
            vmem((3, total_rows, UNIT), BF16),
            vmem((total_rows + 8, width), F32),
            vmem((total_rows + 8, width), F32),
            vmem((total_rows, half), BF16),
            vmem((total_rows, width), BF16),
            vmem((total_rows, half), BF16),
            vmem((half, width), BF16),
            vmem((width, half), BF16),
            vmem((2, step, width), F32),
            vmem((2, step, width), BF16),
            vmem((step, width), F32),
            vmem((2, step, half), BF16),
            vmem((8, width), F32),
            vmem((plan.bits, 8, half), F32),
            vmem((plan.bits, 8, half), F32),
            dma((3, 2)),
            dma((8, steps)),
            dma((3,)),
            dma((2,)),
            dma((2,)),
            dma((2,)),
            dma((steps,)),
            dma((steps,)),
            dma((steps,)),
            dma((steps,)),
            dma((steps,)),
            dma((steps,)),
            dma((steps,)),
            dma((1,)),
            dma((1,)),
            dma((plan.bits,)),
            dma((plan.bits,)),
            pltpu.SemaphoreType.REGULAR((2,)),
            dma((units,)),
            dma((7,)),
            dma((2,)),
            dma((1,)),
            dma((1,)),
            dma((steps,)),
            dma((steps,)),
        ]
        + plan.scratch(units),
        compiler_params=pltpu.CompilerParams(
            collective_id=0, has_side_effects=True, vmem_limit_bytes=VMEM_BYTES
        ),
    )(*smalls, *operands)


def finish_kernel(
    grads_in,
    block_in,
    tokens_in,
    small_ref,
    gate_hbm,
    up_hbm,
    down_hbm,
    in_hbm,
    out_hbm,
    block_hbm,
    tokens_hbm,
    conv_ref,
    one_ref,
    two_ref,
    grads_buf,
    block_buf,
    tokens_buf,
    load_sem,
    store_sem,
):
    hidden, half = gate_hbm.shape[1], out_hbm.shape[1]
    blocks, pieces = hidden // UNIT, half // UNIT
    early = 3 * blocks
    total_rows = block_buf.shape[0]
    step = min(256, total_rows)
    moves = []

    def move(source, buf, target):
        index = len(moves)
        moves.append(
            (
                pltpu.make_async_copy(source, buf, load_sem.at[index]),
                pltpu.make_async_copy(buf, target, store_sem.at[index]),
            )
        )
        moves[-1][0].start()

    for index in range(total_rows // step):
        part = pl.ds(index * step, step)
        move(tokens_in.at[part], tokens_buf.at[part], tokens_hbm.at[part])
        move(block_in.at[part], block_buf.at[part], block_hbm.at[part])
    for block in range(blocks):
        columns = pl.ds(block * UNIT, UNIT)
        for place, target in enumerate((gate_hbm, up_hbm, down_hbm)):
            unit = 3 * block + place
            move(grads_in.at[unit], grads_buf.at[unit], target.at[:, columns])
    for index, place in enumerate((1, 3, 0, 2)):
        for piece in range(pieces):
            unit = early + index * pieces + piece
            columns = pl.ds(piece * UNIT, UNIT)
            target = out_hbm if place == 3 else in_hbm.at[place]
            move(grads_in.at[unit], grads_buf.at[unit], target.at[:, columns])
    conv_ref[...] = small_ref[0:3]
    one_ref[...] = small_ref[3:4]
    two_ref[...] = small_ref[4:5]
    for load, store in moves:
        load.wait()
        store.start()
    for load, store in moves:
        store.wait()


def finish(rows, hidden, grads, small, block_out, tokens_grad):
    total_rows, half = block_out.shape
    shape = jax.ShapeDtypeStruct
    moves = 2 * (total_rows // min(256, total_rows)) + grads.shape[0]
    return pl.pallas_call(
        finish_kernel,
        name="finish",
        out_shape=(
            shape((rows, hidden), F32),
            shape((rows, hidden), F32),
            shape((rows, hidden), F32),
            shape((3, rows, half), F32),
            shape((rows, half), F32),
            shape((total_rows, half), BF16),
            shape((total_rows, half), F32),
            shape((3, half), F32),
            shape((1, half), F32),
            shape((1, half), F32),
        ),
        in_specs=[anywhere()] * 3 + [whole()],
        out_specs=[anywhere()] * 7 + [whole()] * 3,
        scratch_shapes=[
            pltpu.VMEM(grads.shape, F32),
            pltpu.VMEM((total_rows, half), BF16),
            pltpu.VMEM((total_rows, half), F32),
            pltpu.SemaphoreType.DMA((moves,)),
            pltpu.SemaphoreType.DMA((moves,)),
        ],
        compiler_params=pltpu.CompilerParams(vmem_limit_bytes=VMEM_BYTES),
    )(grads, block_out, tokens_grad, small)


def local(
    seq_size,
    shards,
    tokens,
    norm1_gain,
    in_weight,
    conv_weight,
    out_weight,
    norm2_gain,
    gate_weight,
    up_weight,
    down_weight,
    out_cotangent,
):
    seqs, length, width = tokens.shape
    assert seqs == 1
    half = in_weight.shape[2]
    total_rows = seqs * length
    chunk_rows = width // shards
    plan = Halving(seq_size, shards, chunk_rows)
    gains = (norm1_gain.reshape(1, width), norm2_gain.reshape(1, width))
    tokens = tokens.reshape(total_rows, width)
    hidden = gate_weight.shape[1]
    small, grads, block_out, tokens_grad = main(
        plan,
        (*gains, conv_weight),
        (
            tokens,
            out_cotangent.reshape(total_rows, half),
            gate_weight,
            up_weight,
            down_weight,
            out_weight,
            in_weight,
        ),
        hidden,
    )[:4]
    (
        gate_grad,
        up_grad,
        down_grad,
        in_grad,
        out_grad,
        block_out,
        tokens_grad,
        conv_grad,
        norm1_grad,
        norm2_grad,
    ) = finish(chunk_rows, hidden, grads, small, block_out, tokens_grad)
    norm1_grad, norm2_grad = norm1_grad[0], norm2_grad[0]
    down_grad, out_grad = down_grad.T, out_grad.T
    block_out = block_out.reshape(seqs, length, half)
    tokens_grad = tokens_grad.reshape(seqs, length, half)
    return (
        block_out,
        tokens_grad,
        norm1_grad,
        in_grad,
        conv_grad,
        out_grad,
        norm2_grad,
        gate_grad,
        up_grad,
        down_grad,
    )


def solution(mesh):
    seq_size = mesh.shape["seq"]
    shards = mesh.shape["dp"] * seq_size
    return jax.shard_map(
        functools.partial(local, seq_size, shards),
        mesh=mesh,
        in_specs=(
            P("dp", "seq", None),
            P(),
            P(None, None, "tensor"),
            P(None, "tensor"),
            P("tensor", None),
            P(),
            P(None, "tensor"),
            P(None, "tensor"),
            P("tensor", None),
            P("dp", "seq", "tensor"),
        ),
        out_specs=(
            P("dp", "seq", "tensor"),
            P("dp", "seq", "tensor"),
            P("tensor"),
            P(None, ("dp", "seq"), "tensor"),
            P(None, "tensor"),
            P("tensor", ("dp", "seq")),
            P("tensor"),
            P(("dp", "seq"), "tensor"),
            P(("dp", "seq"), "tensor"),
            P("tensor", ("dp", "seq")),
        ),
        check_vma=False,
    )
```

```python
import functools

import jax
import jax.numpy as jnp
from jax import lax
from jax.experimental import pallas as pl
from jax.experimental.pallas import tpu as pltpu
from jax.sharding import PartitionSpec as P

EPSILON = 1e-05
MESH = pl.DeviceIdType.MESH
UNIT = 256
RING = 8
PACE = (5, 24)
LATE_FIRST = 1
LAGS = (-7, 5, 25, 46, 140)
STEPS = (6, 5, 2, 1, 5, 6, 10)
VMEM_BYTES = 67043328
F32 = jnp.float32
BF16 = jnp.bfloat16


def inverse_rms(values):
    return lax.rsqrt(jnp.mean(values * values, axis=-1, keepdims=True) + EPSILON)


def product(left, right):
    return jnp.dot(left, right, preferred_element_type=F32)


def product_t(left, right):
    return lax.dot_general(left, right, (((1,), (1,)), ((), ())), preferred_element_type=F32)


class Halving:
    def __init__(self, seq_size, shards, rows):
        self.seq_size = seq_size
        self.bits = shards.bit_length() - 1
        self.shards = shards
        self.rows = rows

    def stage_rows(self, stage):
        return self.rows << (self.bits - 1 - stage)

    def enter(self):
        self.me = lax.axis_index("dp") * self.seq_size + lax.axis_index("seq")
        self.core = lax.axis_index("tensor")

    def place(self, flat):
        return (flat // self.seq_size, flat % self.seq_size, self.core)

    def flipped(self, weight):
        return self.me + (1 - 2 * ((self.me // weight) % 2)) * weight

    def other_core(self):
        return (self.me // self.seq_size, self.me % self.seq_size, 1 - self.core)

    def along_seq(self, steps):
        seq = (self.me + steps) % self.seq_size
        return (self.me // self.seq_size, seq, self.core)

    def greet(self, steps):
        barrier = pltpu.get_barrier_semaphore()
        partners = [self.other_core()]
        partners += [self.place(self.flipped(1 << bit)) for bit in range(self.bits)]
        partners.extend(self.along_seq(count) for count in steps)
        for partner in partners:
            pl.semaphore_signal(barrier, inc=1, device_id=partner, device_id_type=MESH)
        pl.semaphore_wait(barrier, len(partners))

    def order(self, parity):
        top = self.shards // 2
        high = (self.me // top) % 2
        low = self.me % 2
        first = (top + parity * (1 - top), high + parity * (low - high))
        third = (1 + parity * (top - 1), low + parity * (high - low))
        middle = [(2, (self.me // 2) % 2)]
        rest = [(1 << bit, (self.me // (1 << bit)) % 2) for bit in range(2, self.bits - 1)]
        return [first] + middle + [third] + rest

    def chunks(self, order, keep):
        weight, bit = order[0]
        base = (bit if keep else 1 - bit) * weight
        found = []
        for code in range(self.shards // 2):
            chunk = base
            for place in range(1, self.bits):
                if (code >> (self.bits - 1 - place)) & 1:
                    chunk = chunk + order[place][0]
            found.append(chunk)
        return found

    def offset(self, order, source, stage):
        total = 0
        for place in range(source + 1, min(stage, self.bits - 1) + 1):
            bit = order[place][1]
            if place == stage:
                bit = 1 - bit
            total = total + bit * (1 << (self.bits - 1 - place))
        return total * self.rows

    def scratch(self, units):
        half = self.stage_rows(0)
        ring = min(RING, units)
        return (
            [pltpu.VMEM((ring, half, UNIT), BF16), pltpu.VMEM((units, half, UNIT), BF16)]
            + [pltpu.VMEM((units, self.stage_rows(s), UNIT), BF16) for s in range(self.bits)]
            + [
                pltpu.SemaphoreType.DMA((2, self.bits, units)),
                pltpu.SemaphoreType.DMA((2, self.bits, units)),
            ]
        )

    def bind(self, refs):
        self.first, self.keep = refs[0], refs[1]
        self.recv = refs[2 : 2 + self.bits]
        self.send_sem, self.recv_sem = refs[2 + self.bits :]

    def copies(self, order, unit, stage):
        weight, bit = order[stage]
        rows = self.stage_rows(stage)
        starts = [0]
        if stage + 1 < self.bits:
            rows = rows // 2
            following = order[stage + 1][1]
            starts = [(1 - following) * rows, following * rows]
        base = 0 if stage == 0 else self.offset(order, 0, stage)
        found = []
        for part, start in enumerate(starts):
            source = pl.ds(pl.multiple_of(base + start, self.rows), rows)
            target = pl.ds(pl.multiple_of(start, self.rows), rows)
            buffer = self.keep.at[unit] if stage else self.first.at[unit % RING]
            found.append(
                pltpu.make_async_remote_copy(
                    src_ref=buffer.at[source],
                    dst_ref=self.recv[stage].at[unit, target],
                    send_sem=self.send_sem.at[part, stage, unit],
                    recv_sem=self.recv_sem.at[part, stage, unit],
                    device_id=self.place(self.me + (1 - 2 * bit) * weight),
                    device_id_type=MESH,
                )
            )
        return found

    def arrived(self, order, unit, stage):
        self.copies(order, unit, stage - 1)[0].wait_recv()
        if stage >= 2:
            self.copies(order, unit, stage - 2)[1].wait_recv()

    def sent(self, order, unit, stage):
        for item in self.copies(order, unit, stage):
            item.wait_send()

    def gather(self, left, order, keep):
        return jnp.concatenate([left[chunk] for chunk in self.chunks(order, keep)], axis=0)

    def begin(self, unit, parity, left, right):
        order = self.order(parity)

        @pl.when(unit >= RING)
        def _():
            self.sent(order, unit - RING, 0)

        value = product(self.gather(left, order, False), right[...]).astype(BF16)
        self.first[unit % RING] = value

    def launch(self, unit, parity):
        for item in self.copies(self.order(parity), unit, 0):
            item.start()

    def hold(self, unit, parity, left, right):
        order = self.order(parity)
        self.keep[unit] = product(self.gather(left, order, True), right[...]).astype(BF16)

    def collect(self, order, unit, stage, rows):
        start = pl.multiple_of(self.offset(order, 0, stage), self.rows)
        total = self.keep[unit, pl.ds(start, rows)].astype(F32)
        for source in range(min(stage, self.bits)):
            start = pl.multiple_of(self.offset(order, source, stage), self.rows)
            total = total + self.recv[source][unit, pl.ds(start, rows)].astype(F32)
        return total

    def advance(self, unit, parity, stage):
        order = self.order(parity)
        self.arrived(order, unit, stage)
        rows = self.stage_rows(stage)
        total = self.collect(order, unit, stage, rows)
        start = pl.multiple_of(self.offset(order, 0, stage), self.rows)
        self.keep[unit, pl.ds(start, rows)] = total.astype(BF16)
        for item in self.copies(order, unit, stage):
            item.start()

    def finish(self, unit, parity):
        order = self.order(parity)
        self.arrived(order, unit, self.bits)
        total = self.collect(order, unit, self.bits, self.rows)
        for stage in range(1, self.bits):
            self.sent(order, unit, stage)
        return total


def whole():
    return pl.BlockSpec(memory_space=pltpu.VMEM)


def anywhere():
    return pl.BlockSpec(memory_space=pl.ANY)


def main_kernel(
    plan,
    gain_one_ref,
    gain_two_ref,
    tap_ref,
    token_hbm,
    cot_hbm,
    gate_hbm,
    up_hbm,
    down_hbm,
    out_weight_hbm,
    in_weight_hbm,
    small_ref,
    grads_hbm,
    block_hbm,
    tokens_hbm,
    resid_hbm,
    b_hbm,
    c_hbm,
    x_hbm,
    mixed_hbm,
    edge_ref,
    prior_ref,
    grads_ref,
    normed_ref,
    cot_ref,
    left_ref,
    gate_buf,
    up_buf,
    down_buf,
    right_ref,
    pn_acc,
    out_acc,
    mixed_ref,
    pn_recv,
    out_recv,
    out_weight_ref,
    x_weight_ref,
    resid_buf,
    token_buf,
    full_ref,
    block_buf,
    sums_ref,
    small_send,
    small_recv,
    weight_sem,
    load_sem,
    late_sem,
    resid_sem,
    token_sem,
    block_sem,
    store_sem,
    pn_send_sem,
    pn_recv_sem,
    out_send_sem,
    out_recv_sem,
    part_send_sem,
    part_recv_sem,
    halo_send,
    halo_recv,
    small_send_sem,
    small_recv_sem,
    free_sem,
    grads_sem,
    front_sem,
    cot_sem,
    edge_send,
    edge_recv,
    first_send_sem,
    first_recv_sem,
    *refs,
):
    total_rows, width = normed_ref.shape
    blocks = gate_hbm.shape[1] // UNIT
    half = width // 2
    step = min(256, total_rows)
    steps = total_rows // step
    pieces = half // UNIT
    early = 3 * blocks
    units = early + 4 * pieces
    plan.bind(refs)
    plan.enter()
    seq = lax.axis_index("seq")
    last = plan.seq_size - 1
    own = pl.ds(pl.multiple_of(plan.core * half, half), half)
    other = pl.ds(pl.multiple_of((1 - plan.core) * half, half), half)

    def span(index):
        return pl.ds(pl.multiple_of(index * step, step), step)

    def later(index):
        return pl.ds(pl.multiple_of(index * step + 8, 8), step)

    def local_copy(source, target, sem):
        return pltpu.make_async_copy(source, target, sem)

    def core_copy(source, target, send, recv):
        return pltpu.make_async_remote_copy(
            src_ref=source,
            dst_ref=target,
            send_sem=send,
            recv_sem=recv,
            device_id=plan.other_core(),
            device_id_type=MESH,
        )

    def weights(index):
        slot = index % 2
        columns = pl.ds(pl.multiple_of(index * UNIT, UNIT), UNIT)
        tall = pl.ds(0, width)
        return [
            local_copy(gate_hbm.at[:, columns], gate_buf.at[slot, tall], weight_sem.at[0, slot]),
            local_copy(up_hbm.at[:, columns], up_buf.at[slot, tall], weight_sem.at[1, slot]),
            local_copy(down_hbm.at[columns], down_buf.at[slot], weight_sem.at[2, slot]),
        ]

    def front_loads(late):
        tall = pl.ds(0, width)
        if late:
            pairs = [(out_weight_hbm, out_weight_ref), (cot_hbm, cot_ref.at[:, own])]
            return [
                local_copy(source, target, front_sem.at[place])
                for place, (source, target) in enumerate(pairs)
            ]
        pairs = [(in_weight_hbm.at[2], x_weight_ref)]
        for piece in range(pieces):
            columns = pl.ds(piece * UNIT, UNIT)
            pairs.append((in_weight_hbm.at[0, :, columns], gate_buf.at[piece, tall]))
            pairs.append((in_weight_hbm.at[1, :, columns], up_buf.at[piece, tall]))
        return [
            local_copy(source, target, front_sem.at[2 + place])
            for place, (source, target) in enumerate(pairs)
        ]

    def c_place(index):
        columns = pl.ds(pl.multiple_of((index % 2) * half, half), half)
        return resid_buf.at[index // 2, :, columns]

    def early_stores(index):
        rows = span(index)
        low, high = pl.ds(0, half), pl.ds(half, half)
        return [
            local_copy(pn_acc.at[later(index), low], b_hbm.at[rows], load_sem.at[0, index]),
            local_copy(pn_acc.at[later(index), high], x_hbm.at[rows], load_sem.at[1, index]),
            local_copy(c_place(index), c_hbm.at[rows], load_sem.at[5, index]),
        ]

    def mixed_store(index):
        rows = span(index)
        return local_copy(mixed_ref.at[rows], mixed_hbm.at[rows], load_sem.at[6, index])

    def resid_store(index):
        rows = span(index)
        return local_copy(out_acc.at[rows], resid_hbm.at[rows], load_sem.at[7, index])

    def cot_swap():
        return core_copy(cot_hbm, cot_ref.at[:, own], cot_sem.at[0], cot_sem.at[1])

    def first_swap(index):
        rows = span(index)
        return core_copy(
            normed_ref.at[rows],
            pn_recv.at[rows],
            first_send_sem.at[index],
            first_recv_sem.at[index],
        )

    def edge_copy():
        return pltpu.make_async_remote_copy(
            src_ref=token_hbm.at[pl.ds(total_rows - edge_ref.shape[0], edge_ref.shape[0])],
            dst_ref=edge_ref,
            send_sem=edge_send.at[0],
            recv_sem=edge_recv.at[0],
            device_id=plan.along_seq(1),
            device_id_type=MESH,
        )

    def back_loads(index):
        rows = span(index)
        low, high = pl.ds(0, half), pl.ds(half, half)
        return [
            local_copy(b_hbm.at[rows], pn_acc.at[later(index), low], load_sem.at[2, index]),
            local_copy(x_hbm.at[rows], pn_acc.at[later(index), high], load_sem.at[3, index]),
            local_copy(c_hbm.at[rows], out_acc.at[rows, other], load_sem.at[4, index]),
        ]

    def resid_load(index):
        slot = index % 2
        return local_copy(resid_hbm.at[span(index)], resid_buf.at[slot], resid_sem.at[slot])

    def token_load(index):
        slot = index % 2
        return local_copy(token_hbm.at[span(index)], token_buf.at[slot], token_sem.at[slot])

    def block_store(index):
        slot = index % 2
        return local_copy(block_buf.at[slot], block_hbm.at[span(index)], block_sem.at[slot])

    def token_store(index):
        rows = span(index)
        return local_copy(out_acc.at[rows, own], tokens_hbm.at[rows], store_sem.at[index])

    def grads_store(unit):
        return local_copy(grads_ref.at[unit], grads_hbm.at[unit], grads_sem.at[unit])

    def in_weight_loads():
        tall = pl.ds(0, width)
        return [
            local_copy(
                in_weight_hbm.at[place],
                cot_ref.at[tall, pl.ds(place * half, half)],
                late_sem.at[place],
            )
            for place in range(2)
        ]

    def mixed_load():
        return local_copy(mixed_hbm, mixed_ref, late_sem.at[2])

    def pn_swap(index):
        rows = span(index)
        return core_copy(
            normed_ref.at[rows], pn_recv.at[rows], pn_send_sem.at[index], pn_recv_sem.at[index]
        )

    def out_swap(index):
        rows = span(index)
        return core_copy(
            mixed_ref.at[rows], out_recv.at[rows], out_send_sem.at[index], out_recv_sem.at[index]
        )

    def part_swap(index):
        rows = span(index)
        return core_copy(
            normed_ref.at[rows],
            pn_recv.at[rows],
            part_send_sem.at[index],
            part_recv_sem.at[index],
        )

    def halo():
        return pltpu.make_async_remote_copy(
            src_ref=out_acc.at[pl.ds(0, 8), other],
            dst_ref=out_acc.at[pl.ds(total_rows, 8), other],
            send_sem=halo_send.at[0],
            recv_sem=halo_recv.at[0],
            device_id=plan.along_seq(-1),
            device_id_type=MESH,
        )

    def small(bit):
        return pltpu.make_async_remote_copy(
            src_ref=small_send.at[bit],
            dst_ref=small_recv.at[bit],
            send_sem=small_send_sem.at[bit],
            recv_sem=small_recv_sem.at[bit],
            device_id=plan.place(plan.flipped(1 << bit)),
            device_id_type=MESH,
        )

    def limit(stage, clock, floor, cap):
        lag = LAGS[min(stage, len(LAGS) - 1)] + 12 * max(0, stage - len(LAGS) + 1)
        if stage:
            floor = 0
        count = (clock - lag) * PACE[0] // PACE[1]
        if all(isinstance(value, int) for value in (clock, floor, cap)):
            return max(floor, min(count, cap), 0)
        return jnp.maximum(jnp.maximum(jnp.minimum(count, cap), floor), 0)

    def tick(before, after):
        for stage in [0] + sorted(range(1, plan.bits + 1), reverse=bool(LATE_FIRST)):
            low = limit(stage, before[0], before[1], before[2 + (stage > 0)])
            high = limit(stage, after[0], after[1], after[2 + (stage > 0)])
            if isinstance(low, int) and isinstance(high, int) and low >= high:
                continue

            def advance(unit, carry, stage=stage):
                if stage == 0:
                    plan.launch(unit, unit % 2)
                elif stage < plan.bits:
                    plan.advance(unit, unit % 2, stage)
                else:
                    grads_ref[unit] = plan.finish(unit, unit % 2)
                    grads_store(unit).start()
                return carry

            lax.fori_loop(low, high, advance, 0)

    def normalise(value, gain):
        return (value * inverse_rms(value) * gain).astype(BF16)

    def chunked(value):
        return value.T.reshape(plan.shards, plan.rows, step)

    gain_one, gain_two = gain_one_ref[...], gain_two_ref[...]
    taps = [tap_ref[k : k + 1] for k in range(3)]

    def start_tokens():
        for index in range(min(2, steps)):
            token_load(index).start()

    def next_tokens(index):
        @pl.when(index + 2 < steps)
        def _():
            token_load(index + 2).start()

    start_tokens()
    for item in front_loads(False) + front_loads(True):
        item.start()
    sums_ref[...] = jnp.zeros_like(sums_ref)
    plan.greet((-1, 1))

    @pl.when(seq < last)
    def _():
        edge_copy().start()

    cot_swap().start()
    for item in front_loads(False):
        item.wait()

    def project(index, carry):
        rows = span(index)
        slot = index % 2
        token_load(index).wait()
        value = token_buf[slot].astype(F32)
        out_acc[rows] = value
        normed = normalise(value, gain_one)
        next_tokens(index)
        for piece in range(pieces):
            columns = pl.ds(piece * UNIT, UNIT)
            pn_acc[later(index), columns] = product(normed, gate_buf[piece, 0:width])
            pn_acc[later(index), pl.ds(half + piece * UNIT, UNIT)] = product(
                normed, x_weight_ref[:, columns]
            )
            place = pl.ds(pl.multiple_of((index % 2) * half + piece * UNIT, UNIT), UNIT)
            resid_buf[index // 2, :, place] = product(normed, up_buf[piece, 0:width])
        for item in early_stores(index):
            item.start()
        return carry

    lax.fori_loop(0, steps, project, 0)
    start_tokens()

    @pl.when(seq > 0)
    def _():
        edge_copy().wait_recv()

    @pl.when(seq == 0)
    def _():
        edge_ref[...] = jnp.zeros_like(edge_ref)

    normed = normalise(edge_ref[...].astype(F32), gain_one)
    edge = edge_ref.shape[0]
    for piece in range(pieces):
        columns = pl.ds(piece * UNIT, UNIT)
        gated = product(normed, gate_buf[piece, 0:width]) * product(
            normed, x_weight_ref[:, columns]
        )
        prior_ref[:, columns] = gated[edge - 8 : edge]
    for item in weights(0):
        item.start()
    pn_acc[0:8, 0:half] = prior_ref[...]
    pn_acc[0:8, half:width] = jnp.ones((8, half), F32)

    def convolve(index, carry):
        start = pl.multiple_of(index * step, step)
        rows = span(index)
        window = pn_acc[pl.ds(start, step + 8), 0:half] * pn_acc[pl.ds(start, step + 8), half:width]
        views = [window[6 + k : 6 + k + step] for k in range(3)]
        conv_out = taps[0] * views[0] + taps[1] * views[1] + taps[2] * views[2]
        mixed = (c_place(index)[...] * conv_out).astype(BF16)
        mixed_ref[rows] = mixed
        part = product(mixed, out_weight_ref[...])
        normed_ref[rows] = part.astype(BF16)
        first_swap(index).start()
        out_acc[rows] += part
        mixed_store(index).start()
        left_ref[1, :, :, rows] = chunked(cot_ref[rows])
        return carry

    for item in front_loads(True):
        item.wait()
    cot_swap().wait_recv()
    lax.fori_loop(0, steps, convolve, 0)

    def settle(index, carry):
        rows = span(index)
        first_swap(index).wait_recv()
        first_swap(index).wait_send()
        resid = out_acc[rows] + pn_recv[rows].astype(F32)
        out_acc[rows] = resid
        normed = normalise(resid, gain_two)
        normed_ref[rows] = normed
        resid_store(index).start()
        left_ref[0, :, :, rows] = chunked(normed)
        return carry

    lax.fori_loop(0, steps, settle, 0)
    pl.semaphore_signal(
        free_sem.at[0], inc=1, device_id=plan.other_core(), device_id_type=MESH
    )

    def block_step(index, carry):
        slot = index % 2

        @pl.when(index + 1 < blocks)
        def _():
            for item in weights(index + 1):
                item.start()

        for item in weights(index):
            item.wait()
        for place in range(steps):
            rows = pl.ds(place * step, step)
            normed = normed_ref[rows]
            gate_pre = product(normed, gate_buf[slot, 0:width])
            up_pre = product(normed, up_buf[slot, 0:width])
            grad_hidden = product_t(cot_ref[rows], down_buf[slot])
            sigma = jax.nn.sigmoid(gate_pre)
            active = gate_pre * sigma
            right_ref[0, rows] = (
                grad_hidden * up_pre * (sigma * (1.0 + gate_pre * (1.0 - sigma)))
            ).astype(BF16)
            right_ref[1, rows] = (grad_hidden * active).astype(BF16)
            right_ref[2, rows] = (active * up_pre).astype(BF16)

        start, stop = index * 3, index * 3 + 3
        marks = [
            (12 * index, start - RING, start, start),
            (12 * index + 4, stop - RING, start, start),
            (12 * index + 6, stop - RING, stop, start),
            (12 * index + 10, stop - RING, stop, start),
            (12 * index + 12, stop - RING, stop, stop),
        ]
        tick(marks[0], marks[1])
        for place in range(3):
            unit = index * 3 + place
            plan.begin(unit, unit % 2, left_ref.at[place // 2], right_ref.at[place])
        tick(marks[1], marks[2])

        @pl.when(index == 0)
        def _():
            for place in range(steps):
                for item in early_stores(place) + [mixed_store(place), resid_store(place)]:
                    item.wait()
            for place in range(min(2, steps)):
                resid_load(place).start()
            pn_acc[...] = jnp.zeros_like(pn_acc)
            out_acc[0:total_rows] = jnp.zeros((total_rows, width), F32)

        for place in range(steps):
            rows = pl.ds(place * step, step)
            pn_acc[pl.ds(place * step + 8, step)] += product_t(
                right_ref[0, rows], gate_buf[slot, 0:width]
            ) + product_t(right_ref[1, rows], up_buf[slot, 0:width])
            out_acc[rows] += product(right_ref[2, rows], down_buf[slot])
        tick(marks[2], marks[3])
        for place in range(3):
            unit = index * 3 + place
            plan.hold(unit, unit % 2, left_ref.at[place // 2], right_ref.at[place])
        tick(marks[3], marks[4])
        return carry

    lax.fori_loop(0, blocks, block_step, 0)
    mark = (12 * blocks, early - RING, early, early)

    def paced(mark, clock, body):
        def run(index, carry):
            body(index)
            before = mark[0] + clock * index
            tick((before,) + mark[1:], (before + clock,) + mark[1:])
            return carry

        lax.fori_loop(0, steps, run, 0)
        return (mark[0] + clock * steps,) + mark[1:]

    def move(mark, clock, begun=None, held=None):
        begun = mark[2] if begun is None else begun
        held = mark[3] if held is None else held
        new = (mark[0] + clock, max(mark[1], begun - RING), begun, held)
        tick(mark, new)
        return new

    pn_acc[0:8, 0:half] = prior_ref[...]
    pn_acc[0:8, half:width] = jnp.ones((8, half), F32)

    pl.semaphore_wait(free_sem.at[0], 1)

    def hand_over(index, carry):
        rows = span(index)
        normed_ref[rows] = pn_acc[later(index)].astype(BF16)
        pn_swap(index).start()
        mixed_ref[rows] = out_acc[rows, other].astype(BF16)
        out_swap(index).start()
        for item in back_loads(index):
            item.start()
        return carry

    lax.fori_loop(0, steps, hand_over, 0)
    mark = move(mark, STEPS[0])

    def right_of(place, piece):
        tall = pl.ds(0, total_rows)
        if place == 0:
            return gate_buf.at[piece, tall]
        if place == 1:
            return up_buf.at[piece, tall]
        if place == 2:
            return right_ref.at[piece]
        return mixed_ref.at[:, pl.ds(piece * UNIT, UNIT)]

    def first_pass(index):
        start = pl.multiple_of(index * step, step)
        rows = span(index)
        slot = index % 2
        resid_load(index).wait()
        for item in back_loads(index):
            item.wait()
        pn_swap(index).wait_recv()
        out_swap(index).wait_recv()

        @pl.when(index >= 2)
        def _():
            block_store(index - 2).wait()

        block_buf[slot] = (
            resid_buf[slot, :, own] + out_acc[rows, own] + out_recv[rows].astype(F32)
        ).astype(BF16)
        block_store(index).start()
        resid = resid_buf[slot]
        scale = inverse_rms(resid)
        unit = resid * scale
        grad = normed_ref[rows].astype(F32) + pn_recv[rows].astype(F32)
        sums_ref[0:1] += jnp.sum(grad * unit, axis=0, keepdims=True)
        grad = grad * gain_two
        mean = jnp.mean(grad * unit, axis=-1, keepdims=True)
        grad = cot_ref[rows].astype(F32) + scale * (grad - unit * mean)
        full_ref[...] = grad
        out_acc[rows, own] = full_ref[:, own]

        @pl.when(index + 2 < steps)
        def _():
            resid_load(index + 2).start()

        rounded = grad.astype(BF16)
        left_ref[1, :, :, rows] = chunked(rounded)
        token_load(index).wait()
        left_ref[0, :, :, rows] = chunked(normalise(token_buf[slot].astype(F32), gain_one))
        next_tokens(index)
        grad_mixed = product_t(rounded, out_weight_ref[...])
        window = pn_acc[pl.ds(start, step + 8), 0:half] * pn_acc[pl.ds(start, step + 8), half:width]
        views = [window[6 + k : 6 + k + step] for k in range(3)]
        conv_out = taps[0] * views[0] + taps[1] * views[1] + taps[2] * views[2]
        grad_c = (grad_mixed * conv_out).astype(BF16)
        for piece in range(pieces):
            up_buf[piece, rows] = grad_c[:, piece * UNIT : (piece + 1) * UNIT]
        grad_conv = grad_mixed * out_acc[rows, other]
        out_acc[rows, other] = grad_conv
        for k in range(3):
            sums_ref[1 + k : 2 + k, 0:half] += jnp.sum(grad_conv * views[k], axis=0, keepdims=True)

        @pl.when((index == 0) & (seq > 0))
        def _():
            halo().start()

    mark = paced(mark, STEPS[1], first_pass)
    start_tokens()
    pl.semaphore_signal(
        free_sem.at[1], inc=1, device_id=plan.other_core(), device_id_type=MESH
    )
    for index in range(steps):
        out_swap(index).wait_send()
        pn_swap(index).wait_send()
    mixed_load().start()
    for item in in_weight_loads():
        item.start()
    places = (1, 3, 0, 2)
    work = [(place, piece) for place in places for piece in range(pieces)]

    def produce(mark, count, stop):
        room = (mark[0], max(mark[1], early + stop - RING)) + mark[2:]
        tick(mark, room)
        for hold in (False, True):
            for index in range(count, stop):
                place, piece = work[index]
                unit = early + index
                call = plan.hold if hold else plan.begin
                call(unit, unit % 2, left_ref.at[int(place == 3)], right_of(place, piece))
            if not hold:
                room = move(room, STEPS[2], early + stop)
        return move(room, STEPS[2], None, early + stop)

    mark = produce(mark, 0, pieces)
    mixed_load().wait()
    mark = produce(mark, pieces, 2 * pieces)

    @pl.when(seq < last)
    def _():
        halo().wait_recv()

    @pl.when(seq == last)
    def _():
        out_acc[pl.ds(total_rows, 8), other] = jnp.zeros((8, half), F32)

    def second_pass(index):
        start = pl.multiple_of(index * step, step)
        rows = span(index)
        window = out_acc[pl.ds(start, step + 8), other]
        grad_gated = (
            taps[0] * window[2 : 2 + step]
            + taps[1] * window[1 : 1 + step]
            + taps[2] * window[0:step]
        )
        grad_b = (grad_gated * pn_acc[later(index), half:width]).astype(BF16)
        grad_x = (grad_gated * pn_acc[later(index), 0:half]).astype(BF16)
        for piece in range(pieces):
            columns = slice(piece * UNIT, (piece + 1) * UNIT)
            gate_buf[piece, rows] = grad_b[:, columns]
            right_ref[piece, rows] = grad_x[:, columns]

    mark = paced(mark, STEPS[3], second_pass)
    mark = produce(mark, 2 * pieces, 3 * pieces)
    mark = produce(mark, 3 * pieces, 4 * pieces)
    pl.semaphore_wait(free_sem.at[1], 1)
    for item in in_weight_loads():
        item.wait()

    def third_pass(index):
        rows = span(index)
        total = None
        for place in range(3):
            for piece in range(pieces):
                columns = pl.ds(piece * UNIT, UNIT)
                if place < 2:
                    weight = cot_ref[pl.ds(0, width), pl.ds(place * half + piece * UNIT, UNIT)]
                else:
                    weight = x_weight_ref[:, columns]
                term = product_t(right_of(place, piece)[rows], weight)
                total = term if total is None else total + term
        normed_ref[rows] = total.astype(BF16)
        part_swap(index).start()

    mark = paced(mark, STEPS[4], third_pass)

    def fourth_pass(index):
        rows = span(index)
        slot = index % 2
        part_swap(index).wait_recv()
        token_load(index).wait()
        value = token_buf[slot].astype(F32)
        scale = inverse_rms(value)
        unit = value * scale
        grad = normed_ref[rows].astype(F32) + pn_recv[rows].astype(F32)
        sums_ref[4:5] += jnp.sum(grad * unit, axis=0, keepdims=True)
        grad = grad * gain_one
        mean = jnp.mean(grad * unit, axis=-1, keepdims=True)
        full_ref[...] = scale * (grad - unit * mean)
        out_acc[rows, own] += full_ref[:, own]
        token_store(index).start()
        next_tokens(index)

    mark = paced(mark, STEPS[5], fourth_pass)
    small_send[0] = jnp.zeros_like(small_ref)
    small_send[0, 0:3] = sums_ref[1:4, 0:half]
    small_send[0, 3:4] = sums_ref[4:5, own]
    small_send[0, 4:5] = sums_ref[0:1, own]
    small(0).start()
    mark = move(mark, STEPS[6])
    for bit in range(plan.bits):
        small(bit).wait_recv()
        total = small_send[bit] + small_recv[bit]
        if bit + 1 < plan.bits:
            small_send[bit + 1] = total
            small(bit + 1).start()
            mark = move(mark, STEPS[6])
        else:
            small_ref[...] = total
    rest = 0
    while limit(plan.bits, mark[0] + 3 * rest, 0, units) < units:
        rest += 1

    def drain(index, carry):
        clock = mark[0] + 3 * index
        tick((clock,) + mark[1:], (clock + 3,) + mark[1:])
        return carry

    lax.fori_loop(0, rest, drain, 0)
    for unit in range(units - RING, units):
        plan.sent(plan.order(unit % 2), unit, 0)
    for unit in range(units):
        grads_store(unit).wait()
    for bit in range(plan.bits):
        small(bit).wait_send()

    cot_swap().wait_send()

    @pl.when(seq < last)
    def _():
        edge_copy().wait_send()

    @pl.when(seq > 0)
    def _():
        halo().wait_send()

    for index in range(steps):
        part_swap(index).wait_send()
        token_store(index).wait()
    for index in range(max(0, steps - 2), steps):
        block_store(index).wait()


def main(plan, smalls, operands, hidden):
    total_rows, width = operands[0].shape
    half = width // 2
    assert half == 2 * UNIT
    step = min(256, total_rows)
    steps = total_rows // step
    tall = max(total_rows, width)
    units = (3 * hidden + 4 * half) // UNIT
    shape = jax.ShapeDtypeStruct
    dma = pltpu.SemaphoreType.DMA
    vmem = pltpu.VMEM
    assert total_rows >= width and steps <= 4
    return pl.pallas_call(
        functools.partial(main_kernel, plan),
        name="main",
        out_shape=(
            shape((8, half), F32),
            shape((units, plan.rows, UNIT), F32),
            shape((total_rows, half), BF16),
            shape((total_rows, half), F32),
            shape((total_rows, width), F32),
            shape((total_rows, half), F32),
            shape((total_rows, half), F32),
            shape((total_rows, half), F32),
            shape((total_rows, half), BF16),
        ),
        in_specs=[whole()] * 3 + [anywhere()] * 7,
        out_specs=[whole()] + [anywhere()] * 8,
        scratch_shapes=[
            vmem((16, width), BF16),
            vmem((8, half), F32),
            vmem((units, plan.rows, UNIT), F32),
            vmem((total_rows, width), BF16),
            vmem((total_rows, width), BF16),
            vmem((2, plan.shards, plan.rows, total_rows), BF16),
            vmem((2, tall, UNIT), BF16),
            vmem((2, tall, UNIT), BF16),
            vmem((2, UNIT, width), BF16),
            vmem((3, total_rows, UNIT), BF16),
            vmem((total_rows + 8, width), F32),
            vmem((total_rows + 8, width), F32),
            vmem((total_rows, half), BF16),
            vmem((total_rows, width), BF16),
            vmem((total_rows, half), BF16),
            vmem((half, width), BF16),
            vmem((width, half), BF16),
            vmem((2, step, width), F32),
            vmem((2, step, width), BF16),
            vmem((step, width), F32),
            vmem((2, step, half), BF16),
            vmem((8, width), F32),
            vmem((plan.bits, 8, half), F32),
            vmem((plan.bits, 8, half), F32),
            dma((3, 2)),
            dma((8, steps)),
            dma((3,)),
            dma((2,)),
            dma((2,)),
            dma((2,)),
            dma((steps,)),
            dma((steps,)),
            dma((steps,)),
            dma((steps,)),
            dma((steps,)),
            dma((steps,)),
            dma((steps,)),
            dma((1,)),
            dma((1,)),
            dma((plan.bits,)),
            dma((plan.bits,)),
            pltpu.SemaphoreType.REGULAR((2,)),
            dma((units,)),
            dma((7,)),
            dma((2,)),
            dma((1,)),
            dma((1,)),
            dma((steps,)),
            dma((steps,)),
        ]
        + plan.scratch(units),
        compiler_params=pltpu.CompilerParams(
            collective_id=0, has_side_effects=True, vmem_limit_bytes=VMEM_BYTES
        ),
    )(*smalls, *operands)


def finish_kernel(
    grads_in,
    block_in,
    tokens_in,
    small_ref,
    gate_hbm,
    up_hbm,
    down_hbm,
    in_hbm,
    out_hbm,
    block_hbm,
    tokens_hbm,
    conv_ref,
    one_ref,
    two_ref,
    grads_buf,
    block_buf,
    tokens_buf,
    load_sem,
    store_sem,
):
    hidden, half = gate_hbm.shape[1], out_hbm.shape[1]
    blocks, pieces = hidden // UNIT, half // UNIT
    early = 3 * blocks
    total_rows = block_buf.shape[0]
    step = min(256, total_rows)
    moves = []

    def move(source, buf, target):
        index = len(moves)
        moves.append(
            (
                pltpu.make_async_copy(source, buf, load_sem.at[index]),
                pltpu.make_async_copy(buf, target, store_sem.at[index]),
            )
        )
        moves[-1][0].start()

    for index in range(total_rows // step):
        part = pl.ds(index * step, step)
        move(tokens_in.at[part], tokens_buf.at[part], tokens_hbm.at[part])
        move(block_in.at[part], block_buf.at[part], block_hbm.at[part])
    for block in range(blocks):
        columns = pl.ds(block * UNIT, UNIT)
        for place, target in enumerate((gate_hbm, up_hbm, down_hbm)):
            unit = 3 * block + place
            move(grads_in.at[unit], grads_buf.at[unit], target.at[:, columns])
    for index, place in enumerate((1, 3, 0, 2)):
        for piece in range(pieces):
            unit = early + index * pieces + piece
            columns = pl.ds(piece * UNIT, UNIT)
            target = out_hbm if place == 3 else in_hbm.at[place]
            move(grads_in.at[unit], grads_buf.at[unit], target.at[:, columns])
    conv_ref[...] = small_ref[0:3]
    one_ref[...] = small_ref[3:4]
    two_ref[...] = small_ref[4:5]
    for load, store in moves:
        load.wait()
        store.start()
    for load, store in moves:
        store.wait()


def finish(rows, hidden, grads, small, block_out, tokens_grad):
    total_rows, half = block_out.shape
    shape = jax.ShapeDtypeStruct
    moves = 2 * (total_rows // min(256, total_rows)) + grads.shape[0]
    return pl.pallas_call(
        finish_kernel,
        name="finish",
        out_shape=(
            shape((rows, hidden), F32),
            shape((rows, hidden), F32),
            shape((rows, hidden), F32),
            shape((3, rows, half), F32),
            shape((rows, half), F32),
            shape((total_rows, half), BF16),
            shape((total_rows, half), F32),
            shape((3, half), F32),
            shape((1, half), F32),
            shape((1, half), F32),
        ),
        in_specs=[anywhere()] * 3 + [whole()],
        out_specs=[anywhere()] * 7 + [whole()] * 3,
        scratch_shapes=[
            pltpu.VMEM(grads.shape, F32),
            pltpu.VMEM((total_rows, half), BF16),
            pltpu.VMEM((total_rows, half), F32),
            pltpu.SemaphoreType.DMA((moves,)),
            pltpu.SemaphoreType.DMA((moves,)),
        ],
        compiler_params=pltpu.CompilerParams(vmem_limit_bytes=VMEM_BYTES),
    )(grads, block_out, tokens_grad, small)


def local(
    seq_size,
    shards,
    tokens,
    norm1_gain,
    in_weight,
    conv_weight,
    out_weight,
    norm2_gain,
    gate_weight,
    up_weight,
    down_weight,
    out_cotangent,
):
    seqs, length, width = tokens.shape
    assert seqs == 1
    half = in_weight.shape[2]
    total_rows = seqs * length
    chunk_rows = width // shards
    plan = Halving(seq_size, shards, chunk_rows)
    gains = (norm1_gain.reshape(1, width), norm2_gain.reshape(1, width))
    tokens = tokens.reshape(total_rows, width)
    hidden = gate_weight.shape[1]
    small, grads, block_out, tokens_grad = main(
        plan,
        (*gains, conv_weight),
        (
            tokens,
            out_cotangent.reshape(total_rows, half),
            gate_weight,
            up_weight,
            down_weight,
            out_weight,
            in_weight,
        ),
        hidden,
    )[:4]
    (
        gate_grad,
        up_grad,
        down_grad,
        in_grad,
        out_grad,
        block_out,
        tokens_grad,
        conv_grad,
        norm1_grad,
        norm2_grad,
    ) = finish(chunk_rows, hidden, grads, small, block_out, tokens_grad)
    norm1_grad, norm2_grad = norm1_grad[0], norm2_grad[0]
    down_grad, out_grad = down_grad.T, out_grad.T
    block_out = block_out.reshape(seqs, length, half)
    tokens_grad = tokens_grad.reshape(seqs, length, half)
    return (
        block_out,
        tokens_grad,
        norm1_grad,
        in_grad,
        conv_grad,
        out_grad,
        norm2_grad,
        gate_grad,
        up_grad,
        down_grad,
    )


def solution(mesh):
    seq_size = mesh.shape["seq"]
    shards = mesh.shape["dp"] * seq_size
    return jax.shard_map(
        functools.partial(local, seq_size, shards),
        mesh=mesh,
        in_specs=(
            P("dp", "seq", None),
            P(),
            P(None, None, "tensor"),
            P(None, "tensor"),
            P("tensor", None),
            P(),
            P(None, "tensor"),
            P(None, "tensor"),
            P("tensor", None),
            P("dp", "seq", "tensor"),
        ),
        out_specs=(
            P("dp", "seq", "tensor"),
            P("dp", "seq", "tensor"),
            P("tensor"),
            P(None, ("dp", "seq"), "tensor"),
            P(None, "tensor"),
            P("tensor", ("dp", "seq")),
            P("tensor"),
            P(("dp", "seq"), "tensor"),
            P(("dp", "seq"), "tensor"),
            P("tensor", ("dp", "seq")),
        ),
        check_vma=False,
    )
```
